16 devices in a mesh: data: 4 (over z, y), dap: 4 (over x, core).
Axes of the slice: x: 2, y: 2, z: 2, core: 2. Of those that a mesh axis runs over, the one named last changes fastest.
Arguments:
- msa_act: bfloat16 [512, 64, 384], P(('data', 'dap')), parts along dimension 0
- pair_act: bfloat16 [256, 64, 128], P(('data', 'dap')), parts along dimension 0
- msa_mask: int32 [512, 64], P('data'), parts along dimension 0
- res_mask: int32 [256], P('data'), parts along dimension 0
- w_row_bias: bfloat16 [2, 128, 16], replicated
- w_row_in: bfloat16 [2, 384, 4, 16, 24], replicated
- w_row_out: bfloat16 [2, 16, 24, 384], replicated
- w_col_in: bfloat16 [2, 384, 4, 16, 24], replicated
- w_col_out: bfloat16 [2, 16, 24, 384], replicated
- w_opm_in: bfloat16 [2, 384, 2, 32], replicated
- w_opm_out: bfloat16 [2, 32, 32, 128], replicated
- w_ts_bias: bfloat16 [2, 128, 4], replicated
- w_ts_in: bfloat16 [2, 128, 4, 4, 32], replicated
- w_ts_out: bfloat16 [2, 4, 32, 128], replicated
- w_te_bias: bfloat16 [2, 128, 4], replicated
- w_te_in: bfloat16 [2, 128, 4, 4, 32], replicated
- w_te_out: bfloat16 [2, 4, 32, 128], replicated
Outputs:
- output 1: bfloat16 [512, 64, 384], P(('data', 'dap')), parts along dimension 0
- output 2: bfloat16 [256, 64, 128], P(('data', 'dap')), parts along dimension 0
There are 4 independent parts. The reference program is written for one: setup_inputs(seed, part) draws one part's arguments, and reference() takes and returns one part's arrays. A program takes and returns all parts, laid end to end along the dimension named above; an argument that names none is the same for every part.
All inputs are finite; a program needn't handle non-finite values.
Results may differ from the reference program's by a relative error of at most 0.0182426.
Values are sent between devices in bfloat16 or wider.
A program may use at most 1 GiB of HBM per device.

```python
import jax
import jax.numpy as jnp
from jax import lax

NR = 64
NS = 128
C_M = 384
C_Z = 128
HEADS_MSA = 16
HEAD_MSA = 24
HEADS_TRI = 4
HEAD_TRI = 32
OPM_DIM = 32


def draw_normal(key, shape, scale):
    return (jax.random.normal(key, shape, jnp.float32) * scale).astype(jnp.bfloat16)


def setup_inputs(seed: int = 0, part: int = 0) -> dict:
    base_key = jax.random.key(seed)
    part_keys = jax.random.split(jax.random.fold_in(base_key, part), 4)
    w_keys = jax.random.split(jax.random.fold_in(base_key, 1000), 13)
    width_msa = HEADS_MSA * HEAD_MSA
    width_tri = HEADS_TRI * HEAD_TRI
    return {
        'msa_act': draw_normal(part_keys[0], (NS, NR, C_M), 1.0),
        'pair_act': draw_normal(part_keys[1], (NR, NR, C_Z), 1.0),
        'msa_mask': (jax.random.randint(part_keys[2], (NS, NR), 0, 4) > 0).astype(jnp.int32),
        'res_mask': (jax.random.randint(part_keys[3], (NR,), 0, 4) > 0).astype(jnp.int32),
        'w_row_bias': draw_normal(w_keys[0], (2, C_Z, HEADS_MSA), 1.5 * C_Z ** -0.5),
        'w_row_in': draw_normal(w_keys[1], (2, C_M, 4, HEADS_MSA, HEAD_MSA), 1.25 * C_M ** -0.5),
        'w_row_out': draw_normal(w_keys[2], (2, HEADS_MSA, HEAD_MSA, C_M), 0.5 * width_msa ** -0.5),
        'w_col_in': draw_normal(w_keys[3], (2, C_M, 4, HEADS_MSA, HEAD_MSA), 1.25 * C_M ** -0.5),
        'w_col_out': draw_normal(w_keys[4], (2, HEADS_MSA, HEAD_MSA, C_M), 0.5 * width_msa ** -0.5),
        'w_opm_in': draw_normal(w_keys[5], (2, C_M, 2, OPM_DIM), C_M ** -0.5),
        'w_opm_out': draw_normal(w_keys[6], (2, OPM_DIM, OPM_DIM, C_Z), 0.25 * NS ** 0.5 / OPM_DIM),
        'w_ts_bias': draw_normal(w_keys[7], (2, C_Z, HEADS_TRI), 1.5 * C_Z ** -0.5),
        'w_ts_in': draw_normal(w_keys[8], (2, C_Z, 4, HEADS_TRI, HEAD_TRI), 1.25 * C_Z ** -0.5),
        'w_ts_out': draw_normal(w_keys[9], (2, HEADS_TRI, HEAD_TRI, C_Z), 0.5 * width_tri ** -0.5),
        'w_te_bias': draw_normal(w_keys[10], (2, C_Z, HEADS_TRI), 1.5 * C_Z ** -0.5),
        'w_te_in': draw_normal(w_keys[11], (2, C_Z, 4, HEADS_TRI, HEAD_TRI), 1.25 * C_Z ** -0.5),
        'w_te_out': draw_normal(w_keys[12], (2, HEADS_TRI, HEAD_TRI, C_Z), 0.5 * width_tri ** -0.5),
    }


def layer_norm(values):
    flat = values.astype(jnp.float32)
    row_mean = jnp.mean(flat, axis=-1, keepdims=True)
    centered = flat - row_mean
    row_var = jnp.mean(centered * centered, axis=-1, keepdims=True)
    return (centered * lax.rsqrt(row_var + 1e-5)).astype(jnp.bfloat16)


def add_residual(current, update):
    return (current.astype(jnp.float32) + update).astype(jnp.bfloat16)


def pair_bias(pair_ln, w_bias):
    num_res = pair_ln.shape[0]
    flat = jnp.dot(pair_ln.reshape(num_res * num_res, -1), w_bias, preferred_element_type=jnp.float32)
    return jnp.transpose(flat.astype(jnp.bfloat16).reshape(num_res, num_res, -1), (2, 0, 1))


def attend_one(x_ln, w_in, w_out, bias_hqk, key_mask):
    length = x_ln.shape[0]
    heads = w_in.shape[2]
    head_dim = w_in.shape[3]
    projected = jnp.dot(x_ln, w_in.reshape(w_in.shape[0], -1), preferred_element_type=jnp.float32)
    projected = projected.astype(jnp.bfloat16).astype(jnp.float32).reshape(length, 4, heads, head_dim)
    logits = jnp.einsum('qhd,khd->hqk', projected[:, 0], projected[:, 1]) * head_dim ** -0.5
    if bias_hqk is not None:
        logits = logits + bias_hqk.astype(jnp.float32)
    logits = jnp.where(key_mask[None, None, :] > 0, logits, -1e9)
    attn_probs = jax.nn.softmax(logits, axis=-1).astype(jnp.bfloat16).astype(jnp.float32)
    attended = jnp.einsum('hqk,khd->qhd', attn_probs, projected[:, 2])
    gated = (attended * jax.nn.sigmoid(projected[:, 3])).astype(jnp.bfloat16)
    return jnp.dot(gated.reshape(length, heads * head_dim), w_out.reshape(heads * head_dim, -1), preferred_element_type=jnp.float32)


def row_attention(msa_act, bias_hqk, msa_mask, w_in, w_out):
    def one_seq(inputs):
        seq_act, seq_mask = inputs
        return add_residual(seq_act, attend_one(layer_norm(seq_act), w_in, w_out, bias_hqk, seq_mask))
    return lax.map(one_seq, (msa_act, msa_mask))


def column_attention(msa_act, msa_mask, w_in, w_out):
    def one_col(inputs):
        col_act, col_mask = inputs
        return add_residual(col_act, attend_one(layer_norm(col_act), w_in, w_out, None, col_mask))
    result = lax.map(one_col, (jnp.swapaxes(msa_act, 0, 1), msa_mask.T))
    return jnp.swapaxes(result, 0, 1)


def outer_mean(msa_act, pair_act, msa_mask, w_in, w_out):
    num_seq, num_res, width = msa_act.shape
    mask_f32 = msa_mask.astype(jnp.float32)
    projected = jnp.dot(layer_norm(msa_act).reshape(num_seq * num_res, width), w_in.reshape(width, -1), preferred_element_type=jnp.float32)
    projected = projected.reshape(num_seq, num_res, 2, -1) * mask_f32[:, :, None, None]
    projected = projected.astype(jnp.bfloat16).astype(jnp.float32)
    left = jnp.swapaxes(projected[:, :, 0], 0, 1)
    right = projected[:, :, 1]
    pair_norm = jnp.dot(mask_f32.T, mask_f32)
    w_flat = w_out.reshape(-1, w_out.shape[-1])
    def one_row(inputs):
        left_row, norm_row = inputs
        outer = jnp.einsum('sp,sjq->jpq', left_row, right).astype(jnp.bfloat16)
        update = jnp.dot(outer.reshape(num_res, -1), w_flat, preferred_element_type=jnp.float32)
        return update / (1e-3 + norm_row[:, None])
    return add_residual(pair_act, lax.map(one_row, (left, pair_norm)))


def triangle_start(pair_act, res_mask, w_bias, w_in, w_out):
    pair_ln = layer_norm(pair_act)
    bias_hqk = pair_bias(pair_ln, w_bias)
    def one_row(row_ln):
        return attend_one(row_ln, w_in, w_out, bias_hqk, res_mask)
    return add_residual(pair_act, lax.map(one_row, pair_ln))


def triangle_end(pair_act, res_mask, w_bias, w_in, w_out):
    flipped = triangle_start(jnp.swapaxes(pair_act, 0, 1), res_mask, w_bias, w_in, w_out)
    return jnp.swapaxes(flipped, 0, 1)


def reference(msa_act, pair_act, msa_mask, res_mask, w_row_bias, w_row_in, w_row_out, w_col_in, w_col_out, w_opm_in, w_opm_out, w_ts_bias, w_ts_in, w_ts_out, w_te_bias, w_te_in, w_te_out):
    bias_first = pair_bias(layer_norm(pair_act), w_row_bias[0])
    msa_act = row_attention(msa_act, bias_first, msa_mask, w_row_in[0], w_row_out[0])
    msa_act = column_attention(msa_act, msa_mask, w_col_in[0], w_col_out[0])
    pair_act = outer_mean(msa_act, pair_act, msa_mask, w_opm_in[0], w_opm_out[0])
    pair_act = triangle_start(pair_act, res_mask, w_ts_bias[0], w_ts_in[0], w_ts_out[0])
    pair_act = triangle_end(pair_act, res_mask, w_te_bias[0], w_te_in[0], w_te_out[0])
    bias_second = pair_bias(layer_norm(pair_act), w_row_bias[1])
    msa_act = column_attention(msa_act, msa_mask, w_col_in[1], w_col_out[1])
    pair_act = outer_mean(msa_act, pair_act, msa_mask, w_opm_in[1], w_opm_out[1])
    msa_act = row_attention(msa_act, bias_second, msa_mask, w_row_in[1], w_row_out[1])
    pair_act = triangle_end(pair_act, res_mask, w_te_bias[1], w_te_in[1], w_te_out[1])
    pair_act = triangle_start(pair_act, res_mask, w_ts_bias[1], w_ts_in[1], w_ts_out[1])
    return msa_act, pair_act
```

```python
import functools

import jax
import jax.numpy as jnp
from jax import lax
from jax.experimental import pallas as pl
from jax.experimental.pallas import tpu as pltpu
from jax.sharding import PartitionSpec as P

LOG2E = 1.4426950408889634
NEG = -1e9 * LOG2E
F32 = jnp.float32
BF16 = jnp.bfloat16
NT = (((1,), (1,)), ((), ()))


def layer_norm(values):
    flat = values.astype(F32)
    row_mean = jnp.mean(flat, axis=-1, keepdims=True)
    centered = flat - row_mean
    row_var = jnp.mean(centered * centered, axis=-1, keepdims=True)
    return (centered * lax.rsqrt(row_var + 1e-5)).astype(BF16)


def half_masks(rows, split):
    index = lax.broadcasted_iota(jnp.int32, (rows, 128), 0)
    upper = (index < split).astype(F32).astype(BF16)
    lower = (index >= split).astype(F32).astype(BF16)
    return upper, lower


def attend(x, w_ref, wo_ref, pt_ref, gt_ref, heads, dim, keep, bias_ref):
    width = heads * dim
    rows = 2 * dim
    x_ln = layer_norm(x)
    for part in range(4):
        sl = pl.ds(part * width, width)
        pt_ref[sl, :] = lax.dot_general(w_ref[sl, :], x_ln, NT, preferred_element_type=F32).astype(BF16)
    up, low = half_masks(rows, dim)
    scale = dim ** -0.5 * LOG2E
    if bias_ref is not None:
        left = lax.broadcasted_iota(jnp.int32, (64, 128), 1) < 64
        left_b = left.astype(F32).astype(BF16)
        right_b = (1.0 - left.astype(F32)).astype(BF16)
    for blk in range(2):
        ln = pl.ds(blk * 128, 128)
        for hp in range(heads // 2):
            r = rows * hp
            q = pt_ref[pl.ds(r, rows), ln]
            k = pt_ref[pl.ds(width + r, rows), ln]
            v = pt_ref[pl.ds(2 * width + r, rows), ln]
            g = pt_ref[pl.ds(3 * width + r, rows), ln]
            rhs = jnp.concatenate([q * up, q * low], axis=1)
            logits2 = jnp.dot(k.T, rhs, preferred_element_type=F32)
            probs = []
            for half in range(2):
                lg = logits2[:, 128 * half:128 * half + 128]
                if bias_ref is not None:
                    lg = jnp.where(left, lg[0:64], lg[64:128]) * scale + bias_ref[2 * hp + half]
                else:
                    lg = lg * scale
                lg = jnp.where(keep[blk], lg, NEG)
                e = jnp.exp2(lg - jnp.max(lg, axis=0, keepdims=True))
                p = (e * (1.0 / jnp.sum(e, axis=0, keepdims=True))).astype(BF16)
                if bias_ref is not None:
                    probs += [p * left_b, p * right_b]
                else:
                    probs += [p]
            att = jnp.dot(jnp.concatenate([v * up, v * low], axis=1), jnp.concatenate(probs, axis=0),
                          preferred_element_type=F32)
            gt_ref[pl.ds(r, rows), ln] = (att * jax.nn.sigmoid(g.astype(F32))).astype(BF16)
    update = jnp.dot(gt_ref[...].T, wo_ref[...], preferred_element_type=F32)
    return (x + update).astype(BF16)


def pick_column(table, col):
    lane = lax.broadcasted_iota(jnp.int32, table.shape, 1)
    return jnp.sum(jnp.where(lane == col, table, 0.0), axis=1, keepdims=True)


def row_kernel(heads, dim, per_row, x_ref, keys_ref, bias_ref, w_ref, wo_ref, out_ref, pt_ref, gt_ref):
    step = pl.program_id(0)
    x = x_ref[...].astype(F32).reshape(256, x_ref.shape[-1])
    left = lax.broadcasted_iota(jnp.int32, (64, 128), 1) < 64
    keep = []
    for blk in range(2):
        if per_row:
            keys = keys_ref[...]
            first = pick_column(keys, step * 4 + 2 * blk)
            second = pick_column(keys, step * 4 + 2 * blk + 1)
            keep.append(jnp.where(left, first, second) > 0.5)
        else:
            keep.append(jnp.broadcast_to(keys_ref[...], (64, 128)) > 0.5)
    out = attend(x, w_ref, wo_ref, pt_ref, gt_ref, heads, dim, keep, bias_ref)
    out_ref[...] = out.reshape(out_ref.shape)


def row_attention(x, keys, bias_t, w, wo, heads, dim, per_row):
    groups, length, width = x.shape
    inner = heads * dim
    bias_t = bias_t.astype(F32) * LOG2E
    bias_t = jnp.concatenate([bias_t, bias_t], axis=2)
    return pl.pallas_call(
        functools.partial(row_kernel, heads, dim, per_row),
        grid=(groups // 4,),
        in_specs=[
            pl.BlockSpec((4, length, width), lambda i: (i, 0, 0)),
            pl.BlockSpec(keys.shape, lambda i: (0, 0)),
            pl.BlockSpec(bias_t.shape, lambda i: (0, 0, 0)),
            pl.BlockSpec(w.shape, lambda i: (0, 0)),
            pl.BlockSpec(wo.shape, lambda i: (0, 0)),
        ],
        out_specs=pl.BlockSpec((4, length, width), lambda i: (i, 0, 0)),
        out_shape=jax.ShapeDtypeStruct(x.shape, BF16),
        scratch_shapes=[pltpu.VMEM((4 * inner, 256), BF16), pltpu.VMEM((inner, 256), BF16)],
        cost_estimate=pl.CostEstimate(flops=groups * length * width * inner * 10, bytes_accessed=x.size * 4, transcendentals=0),
        name="row_att" if per_row else "tri_att",
    )(x, keys, bias_t, w, wo)


def col_kernel(x_ref, keys_ref, lanes_ref, w1_ref, wo1_ref, wp1_ref, w2_ref, wo2_ref, wp2_ref,
               out_ref, ac1_ref, ac2_ref, pt_ref, gt_ref):
    step = pl.program_id(0)
    x = x_ref[...].astype(F32).reshape(256, 384)
    keep = [jnp.broadcast_to(pick_column(keys_ref[...], step * 2 + blk), (128, 128)) > 0.5 for blk in range(2)]
    lane_mask = jnp.concatenate([lanes_ref[0], lanes_ref[1]], axis=1)
    for w_ref, wo_ref, wp_ref, ac_ref in ((w1_ref, wo1_ref, wp1_ref, ac1_ref), (w2_ref, wo2_ref, wp2_ref, ac2_ref)):
        out = attend(x, w_ref, wo_ref, pt_ref, gt_ref, 16, 24, keep, None)
        x = out.astype(F32)
        ac = lax.dot_general(wp_ref[...], layer_norm(x), NT, preferred_element_type=F32)
        ac_ref[0] = (ac * lane_mask).astype(BF16)
    out_ref[...] = out.reshape(out_ref.shape)


def column_pair(x, keys, lanes, weights):
    whole = lambda a: pl.BlockSpec(a.shape, lambda i: (0,) * a.ndim)
    return pl.pallas_call(
        col_kernel,
        grid=(8,),
        in_specs=[
            pl.BlockSpec((2, 128, 384), lambda i: (i, 0, 0)),
            whole(keys),
            pl.BlockSpec((2, 1, 128), lambda i: (i, 0, 0)),
        ] + [whole(a) for a in weights],
        out_specs=[
            pl.BlockSpec((2, 128, 384), lambda i: (i, 0, 0)),
            pl.BlockSpec((1, 64, 256), lambda i: (i, 0, 0)),
            pl.BlockSpec((1, 64, 256), lambda i: (i, 0, 0)),
        ],
        out_shape=[
            jax.ShapeDtypeStruct(x.shape, BF16),
            jax.ShapeDtypeStruct((8, 64, 256), BF16),
            jax.ShapeDtypeStruct((8, 64, 256), BF16),
        ],
        scratch_shapes=[pltpu.VMEM((1536, 256), BF16), pltpu.VMEM((384, 256), BF16)],
        cost_estimate=pl.CostEstimate(flops=2048 * 384 * 384 * 20, bytes_accessed=x.size * 4, transcendentals=0),
        name="col_att",
    )(x, keys, lanes, *weights)


def opm_kernel(own_ref, full_ref, z_ref, norm_ref, w_ref, out_ref, full32_ref, o_ref):
    full32_ref[...] = full_ref[...].astype(F32)
    own = own_ref[...]
    zeros = jnp.zeros((64, 128), BF16)

    def one(q, carry):
        c_q = full32_ref[pl.ds(q, 64, stride=32), :].astype(BF16)
        rhs = jnp.concatenate([jnp.concatenate([c_q, zeros], axis=1), jnp.concatenate([zeros, c_q], axis=1)], axis=0)
        o = lax.dot_general(own, rhs, NT, preferred_element_type=F32).astype(BF16)
        for pair in range(8):
            o_ref[pair, pl.ds(pl.multiple_of(q * 32, 32), 32), :] = o[32 * pair:32 * pair + 32]
        return carry

    lax.fori_loop(0, 32, one, 0, unroll=4)
    w = w_ref[...]
    for pair in range(8):
        update = jnp.dot(w, o_ref[pair], preferred_element_type=F32).T
        z = z_ref[pl.ds(2 * pair, 2)].astype(F32).reshape(128, 128)
        norm = norm_ref[...]
        norm = jnp.concatenate([pick_column(norm, 2 * pair), pick_column(norm, 2 * pair + 1)], axis=0)
        out_ref[pl.ds(2 * pair, 2)] = (z + update / (1e-3 + norm)).astype(BF16).reshape(2, 64, 128)


def opm(own, full, z, norm, w):
    return pl.pallas_call(
        opm_kernel,
        out_shape=jax.ShapeDtypeStruct(z.shape, BF16),
        scratch_shapes=[pltpu.VMEM((2048, 128), F32), pltpu.VMEM((8, 1024, 128), BF16)],
        cost_estimate=pl.CostEstimate(flops=10 ** 9, bytes_accessed=2 ** 20, transcendentals=0),
        name="opm",
    )(own, full, z, norm, w)


def solution(mesh):
    def local_step(m, z, mask, res_mask, w_row_bias, w_row_in, w_row_out, w_col_in, w_col_out, w_opm_in, w_opm_out, w_ts_bias, w_ts_in, w_ts_out, w_te_bias, w_te_in, w_te_out):
        dev = lax.axis_index('dap')
        flat_in = lambda w: jnp.transpose(w, (0, 2, 3, 4, 1)).reshape(2, -1, w.shape[1])
        flat_out = lambda w: w.reshape(2, -1, w.shape[-1])
        w_row_in, w_col_in, w_ts_in, w_te_in = map(flat_in, (w_row_in, w_col_in, w_ts_in, w_te_in))
        w_row_out, w_col_out, w_ts_out, w_te_out = map(flat_out, (w_row_out, w_col_out, w_ts_out, w_te_out))
        w_opm_in = jnp.transpose(w_opm_in, (0, 2, 3, 1)).reshape(2, 64, 384)
        w_opm_1 = jnp.transpose(w_opm_out[0], (2, 1, 0)).reshape(128, 1024)
        w_opm_2 = jnp.transpose(w_opm_out[1], (2, 0, 1)).reshape(128, 1024)

        mask_f = mask.astype(F32)
        row_keys = lax.dynamic_slice_in_dim(mask_f, dev * 32, 32, 0).T
        col_keys = lax.dynamic_slice_in_dim(mask_f, dev * 16, 16, 1)
        lanes = col_keys.T.reshape(16, 1, 128)
        tri_keys = res_mask.astype(F32).reshape(64, 1)
        norm = jnp.dot(mask_f.T, col_keys)

        def bias(z_blk, w, form, axis):
            part = jnp.einsum(form, layer_norm(z_blk), w, preferred_element_type=F32).astype(BF16)
            return lax.all_gather(part, 'dap', axis=axis, tiled=True)

        def gather_full(half):
            full = lax.all_gather(half.reshape(8, 32, 2, 128).transpose(0, 2, 1, 3).reshape(512, 128), 'dap', axis=0, tiled=True)
            return full

        row_bias = bias(z, w_row_bias[0], 'ijc,ch->hji', 2)
        m = row_attention(m, row_keys, row_bias, w_row_in[0], w_row_out[0], 16, 24, True)
        m = lax.all_to_all(m, 'dap', 1, 0, tiled=True)
        m = jnp.transpose(m, (1, 0, 2))
        m, ac1, ac2 = column_pair(m, col_keys, lanes, (w_col_in[0], w_col_out[0], w_opm_in[0], w_col_in[1], w_col_out[1], w_opm_in[1]))
        z = opm(ac1[:, :32].reshape(256, 256), gather_full(ac1[:, 32:]), z, norm, w_opm_1)
        ts_bias = bias(z, w_ts_bias[0], 'ijc,ch->hji', 2)
        z = row_attention(z, tri_keys, ts_bias, w_ts_in[0], w_ts_out[0], 4, 32, False)
        z = jnp.transpose(lax.all_to_all(z, 'dap', 1, 0, tiled=True), (1, 0, 2))
        te_bias = bias(z, w_te_bias[0], 'ijc,ch->hji', 2)
        z = row_attention(z, tri_keys, te_bias, w_te_in[0], w_te_out[0], 4, 32, False)

        row_bias = bias(z, w_row_bias[1], 'jic,ch->hji', 1)
        z = opm(ac2[:, 32:].reshape(256, 256), gather_full(ac2[:, :32]), z, norm, w_opm_2)
        m = lax.all_to_all(jnp.transpose(m, (1, 0, 2)), 'dap', 0, 1, tiled=True)
        m = row_attention(m, row_keys, row_bias, w_row_in[1], w_row_out[1], 16, 24, True)
        te_bias = bias(z, w_te_bias[1], 'ijc,ch->hji', 2)
        z = row_attention(z, tri_keys, te_bias, w_te_in[1], w_te_out[1], 4, 32, False)
        z = lax.all_to_all(jnp.transpose(z, (1, 0, 2)), 'dap', 0, 1, tiled=True)
        ts_bias = bias(z, w_ts_bias[1], 'ijc,ch->hji', 2)
        z = row_attention(z, tri_keys, ts_bias, w_ts_in[1], w_ts_out[1], 4, 32, False)
        return m, z

    in_specs = (P(('data', 'dap')), P(('data', 'dap')), P('data'), P('data')) + (P(),) * 13
    out_specs = (P(('data', 'dap')), P(('data', 'dap')))
    return jax.shard_map(local_step, mesh=mesh, in_specs=in_specs, out_specs=out_specs, check_vma=False)
```

```python
import functools

import jax
import jax.numpy as jnp
from jax import lax
from jax.experimental import pallas as pl
from jax.experimental.pallas import tpu as pltpu
from jax.sharding import PartitionSpec as P

LOG2E = 1.4426950408889634
NEG = -1e9 * LOG2E
F32 = jnp.float32
BF16 = jnp.bfloat16
LAG = 3
NT = (((1,), (1,)), ((), ()))


def layer_norm(values):
    flat = values.astype(F32)
    row_mean = jnp.mean(flat, axis=-1, keepdims=True)
    centered = flat - row_mean
    row_var = jnp.mean(centered * centered, axis=-1, keepdims=True)
    return (centered * lax.rsqrt(row_var + 1e-5)).astype(BF16)


def half_masks(rows, split):
    index = lax.broadcasted_iota(jnp.int32, (rows, 128), 0)
    upper = (index < split).astype(F32).astype(BF16)
    lower = (index >= split).astype(F32).astype(BF16)
    return upper, lower


def attend(x, w_ref, wo_ref, pt_ref, gt_ref, kt_ref, lg_ref, pr_ref, heads, dim, keep, bias_ref):
    width = heads * dim
    rows = 2 * dim
    pairs = heads // 2
    x_ln = layer_norm(x)
    for part in range(4):
        sl = pl.ds(part * width, width)
        pt_ref[sl, :] = lax.dot_general(w_ref[sl, :], x_ln, NT, preferred_element_type=F32).astype(BF16)
    up, low = half_masks(rows, dim)
    scale = dim ** -0.5 * LOG2E
    if bias_ref is not None:
        left = lax.broadcasted_iota(jnp.int32, (64, 128), 1) < 64
        left_b = left.astype(F32).astype(BF16)
        right_b = (1.0 - left.astype(F32)).astype(BF16)

    def place(unit):
        return pl.ds(unit // pairs * 128, 128), rows * (unit % pairs)

    def turn_keys(unit):
        ln, r = place(unit)
        kt_ref[unit % 8] = pt_ref[pl.ds(width + r, rows), ln].T

    def make_logits(unit):
        ln, r = place(unit)
        q = pt_ref[pl.ds(r, rows), ln]
        rhs = jnp.concatenate([q * up, q * low], axis=1)
        logits2 = jnp.dot(kt_ref[unit % 8], rhs, preferred_element_type=F32)
        for half in range(2):
            lg = logits2[:, 128 * half:128 * half + 128]
            if bias_ref is not None:
                lg = jnp.where(left, lg[0:64], lg[64:128])
            lg_ref[unit % 8, half] = lg

    def soften(unit):
        blk, hp = unit // pairs, unit % pairs
        for half in range(2):
            lg = lg_ref[unit % 8, half] * scale
            if bias_ref is not None:
                lg = lg + bias_ref[2 * hp + half]
            lg = jnp.where(keep[blk], lg, NEG)
            e = jnp.exp2(lg - jnp.max(lg, axis=0, keepdims=True))
            p = (e * (1.0 / jnp.sum(e, axis=0, keepdims=True))).astype(BF16)
            if bias_ref is not None:
                pr_ref[unit % 8, pl.ds(128 * half, 64)] = p * left_b
                pr_ref[unit % 8, pl.ds(128 * half + 64, 64)] = p * right_b
            else:
                pr_ref[unit % 8, pl.ds(128 * half, 128)] = p

    def mix(unit):
        ln, r = place(unit)
        v = pt_ref[pl.ds(2 * width + r, rows), ln]
        g = pt_ref[pl.ds(3 * width + r, rows), ln]
        att = jnp.dot(jnp.concatenate([v * up, v * low], axis=1), pr_ref[unit % 8], preferred_element_type=F32)
        gt_ref[pl.ds(r, rows), ln] = (att * jax.nn.sigmoid(g.astype(F32))).astype(BF16)

    stages = ((turn_keys, 0), (make_logits, LAG), (soften, 2 * LAG), (mix, 3 * LAG))
    for tick in range(2 * pairs + 3 * LAG):
        for stage, lag in stages:
            if 0 <= tick - lag < 2 * pairs:
                stage(tick - lag)
    update = jnp.dot(gt_ref[...].T, wo_ref[...], preferred_element_type=F32)
    return (x + update).astype(BF16)


def attend_scratch(heads, dim, keys):
    return [
        pltpu.VMEM((4 * heads * dim, 256), BF16),
        pltpu.VMEM((heads * dim, 256), BF16),
        pltpu.VMEM((8, 128, 2 * dim), BF16),
        pltpu.VMEM((8, 2, keys, 128), F32),
        pltpu.VMEM((8, 256, 128), BF16),
    ]


def pick_column(table, col):
    lane = lax.broadcasted_iota(jnp.int32, table.shape, 1)
    return jnp.sum(jnp.where(lane == col, table, 0.0), axis=1, keepdims=True)


def row_kernel(heads, dim, per_row, x_ref, keys_ref, bias_ref, w_ref, wo_ref, out_ref, *scratch):
    step = pl.program_id(0)
    x = x_ref[...].astype(F32).reshape(256, x_ref.shape[-1])
    left = lax.broadcasted_iota(jnp.int32, (64, 128), 1) < 64
    keep = []
    for blk in range(2):
        if per_row:
            keys = keys_ref[...]
            first = pick_column(keys, step * 4 + 2 * blk)
            second = pick_column(keys, step * 4 + 2 * blk + 1)
            keep.append(jnp.where(left, first, second) > 0.5)
        else:
            keep.append(jnp.broadcast_to(keys_ref[...], (64, 128)) > 0.5)
    out = attend(x, w_ref, wo_ref, *scratch, heads, dim, keep, bias_ref)
    out_ref[...] = out.reshape(out_ref.shape)


def row_attention(x, keys, bias_t, w, wo, heads, dim, per_row):
    groups, length, width = x.shape
    bias_t = bias_t.astype(F32) * LOG2E
    bias_t = jnp.concatenate([bias_t, bias_t], axis=2)
    return pl.pallas_call(
        functools.partial(row_kernel, heads, dim, per_row),
        grid=(groups // 4,),
        in_specs=[
            pl.BlockSpec((4, length, width), lambda i: (i, 0, 0)),
            pl.BlockSpec(keys.shape, lambda i: (0, 0)),
            pl.BlockSpec(bias_t.shape, lambda i: (0, 0, 0)),
            pl.BlockSpec(w.shape, lambda i: (0, 0)),
            pl.BlockSpec(wo.shape, lambda i: (0, 0)),
        ],
        out_specs=pl.BlockSpec((4, length, width), lambda i: (i, 0, 0)),
        out_shape=jax.ShapeDtypeStruct(x.shape, BF16),
        scratch_shapes=attend_scratch(heads, dim, 64),
        cost_estimate=pl.CostEstimate(flops=groups * length * width * heads * dim * 10, bytes_accessed=x.size * 4, transcendentals=0),
        name="row_att" if per_row else "tri_att",
    )(x, keys, bias_t, w, wo)


def col_kernel(x_ref, keys_ref, lanes_ref, w1_ref, wo1_ref, wp1_ref, w2_ref, wo2_ref, wp2_ref,
               out_ref, ac1_ref, ac2_ref, *scratch):
    step = pl.program_id(0)
    x = x_ref[...].astype(F32).reshape(256, 384)
    keep = [jnp.broadcast_to(pick_column(keys_ref[...], step * 2 + blk), (128, 128)) > 0.5 for blk in range(2)]
    lane_mask = jnp.concatenate([lanes_ref[0], lanes_ref[1]], axis=1)
    for w_ref, wo_ref, wp_ref, ac_ref in ((w1_ref, wo1_ref, wp1_ref, ac1_ref), (w2_ref, wo2_ref, wp2_ref, ac2_ref)):
        out = attend(x, w_ref, wo_ref, *scratch, 16, 24, keep, None)
        x = out.astype(F32)
        ac = lax.dot_general(wp_ref[...], layer_norm(x), NT, preferred_element_type=F32)
        ac_ref[0] = (ac * lane_mask).astype(BF16)
    out_ref[...] = out.reshape(out_ref.shape)


def column_pair(x, keys, lanes, weights):
    whole = lambda a: pl.BlockSpec(a.shape, lambda i: (0,) * a.ndim)
    return pl.pallas_call(
        col_kernel,
        grid=(8,),
        in_specs=[
            pl.BlockSpec((2, 128, 384), lambda i: (i, 0, 0)),
            whole(keys),
            pl.BlockSpec((2, 1, 128), lambda i: (i, 0, 0)),
        ] + [whole(a) for a in weights],
        out_specs=[
            pl.BlockSpec((2, 128, 384), lambda i: (i, 0, 0)),
            pl.BlockSpec((1, 64, 256), lambda i: (i, 0, 0)),
            pl.BlockSpec((1, 64, 256), lambda i: (i, 0, 0)),
        ],
        out_shape=[
            jax.ShapeDtypeStruct(x.shape, BF16),
            jax.ShapeDtypeStruct((8, 64, 256), BF16),
            jax.ShapeDtypeStruct((8, 64, 256), BF16),
        ],
        scratch_shapes=attend_scratch(16, 24, 128),
        cost_estimate=pl.CostEstimate(flops=2048 * 384 * 384 * 20, bytes_accessed=x.size * 4, transcendentals=0),
        name="col_att",
    )(x, keys, lanes, *weights)


def opm_kernel(own_ref, full_ref, z_ref, norm_ref, w_ref, out_ref, full32_ref, o_ref):
    full32_ref[...] = full_ref[...].astype(F32)
    own = own_ref[...]
    zeros = jnp.zeros((64, 128), BF16)

    def one(q, carry):
        c_q = full32_ref[pl.ds(q, 64, stride=32), :].astype(BF16)
        rhs = jnp.concatenate([jnp.concatenate([c_q, zeros], axis=1), jnp.concatenate([zeros, c_q], axis=1)], axis=0)
        o = lax.dot_general(own, rhs, NT, preferred_element_type=F32).astype(BF16)
        for pair in range(8):
            o_ref[pair, pl.ds(pl.multiple_of(q * 32, 32), 32), :] = o[32 * pair:32 * pair + 32]
        return carry

    lax.fori_loop(0, 32, one, 0, unroll=4)
    w = w_ref[...]
    for pair in range(8):
        update = jnp.dot(w, o_ref[pair], preferred_element_type=F32).T
        z = z_ref[pl.ds(2 * pair, 2)].astype(F32).reshape(128, 128)
        norm = norm_ref[...]
        norm = jnp.concatenate([pick_column(norm, 2 * pair), pick_column(norm, 2 * pair + 1)], axis=0)
        out_ref[pl.ds(2 * pair, 2)] = (z + update / (1e-3 + norm)).astype(BF16).reshape(2, 64, 128)


def opm(own, full, z, norm, w):
    return pl.pallas_call(
        opm_kernel,
        out_shape=jax.ShapeDtypeStruct(z.shape, BF16),
        scratch_shapes=[pltpu.VMEM((2048, 128), F32), pltpu.VMEM((8, 1024, 128), BF16)],
        cost_estimate=pl.CostEstimate(flops=10 ** 9, bytes_accessed=2 ** 20, transcendentals=0),
        name="opm",
    )(own, full, z, norm, w)


def solution(mesh):
    def local_step(m, z, mask, res_mask, w_row_bias, w_row_in, w_row_out, w_col_in, w_col_out, w_opm_in, w_opm_out, w_ts_bias, w_ts_in, w_ts_out, w_te_bias, w_te_in, w_te_out):
        dev = lax.axis_index('dap')
        flat_in = lambda w: jnp.transpose(w, (0, 2, 3, 4, 1)).reshape(2, -1, w.shape[1])
        flat_out = lambda w: w.reshape(2, -1, w.shape[-1])
        w_row_in, w_col_in, w_ts_in, w_te_in = map(flat_in, (w_row_in, w_col_in, w_ts_in, w_te_in))
        w_row_out, w_col_out, w_ts_out, w_te_out = map(flat_out, (w_row_out, w_col_out, w_ts_out, w_te_out))
        w_opm_in = jnp.transpose(w_opm_in, (0, 2, 3, 1)).reshape(2, 64, 384)
        w_opm_1 = jnp.transpose(w_opm_out[0], (2, 1, 0)).reshape(128, 1024)
        w_opm_2 = jnp.transpose(w_opm_out[1], (2, 0, 1)).reshape(128, 1024)

        mask_f = mask.astype(F32)
        row_keys = lax.dynamic_slice_in_dim(mask_f, dev * 32, 32, 0).T
        col_keys = lax.dynamic_slice_in_dim(mask_f, dev * 16, 16, 1)
        lanes = col_keys.T.reshape(16, 1, 128)
        tri_keys = res_mask.astype(F32).reshape(64, 1)
        norm = jnp.dot(mask_f.T, col_keys)

        def bias(z_blk, w, form, axis):
            part = jnp.einsum(form, layer_norm(z_blk), w, preferred_element_type=F32).astype(BF16)
            return lax.all_gather(part, 'dap', axis=axis, tiled=True)

        def gather_full(half):
            full = lax.all_gather(half.reshape(8, 32, 2, 128).transpose(0, 2, 1, 3).reshape(512, 128), 'dap', axis=0, tiled=True)
            return full

        row_bias = bias(z, w_row_bias[0], 'ijc,ch->hji', 2)
        m = row_attention(m, row_keys, row_bias, w_row_in[0], w_row_out[0], 16, 24, True)
        m = lax.all_to_all(m, 'dap', 1, 0, tiled=True)
        m = jnp.transpose(m, (1, 0, 2))
        m, ac1, ac2 = column_pair(m, col_keys, lanes, (w_col_in[0], w_col_out[0], w_opm_in[0], w_col_in[1], w_col_out[1], w_opm_in[1]))
        z = opm(ac1[:, :32].reshape(256, 256), gather_full(ac1[:, 32:]), z, norm, w_opm_1)
        ts_bias = bias(z, w_ts_bias[0], 'ijc,ch->hji', 2)
        z = row_attention(z, tri_keys, ts_bias, w_ts_in[0], w_ts_out[0], 4, 32, False)
        z = jnp.transpose(lax.all_to_all(z, 'dap', 1, 0, tiled=True), (1, 0, 2))
        te_bias = bias(z, w_te_bias[0], 'ijc,ch->hji', 2)
        z = row_attention(z, tri_keys, te_bias, w_te_in[0], w_te_out[0], 4, 32, False)

        row_bias = bias(z, w_row_bias[1], 'jic,ch->hji', 1)
        z = opm(ac2[:, 32:].reshape(256, 256), gather_full(ac2[:, :32]), z, norm, w_opm_2)
        m = lax.all_to_all(jnp.transpose(m, (1, 0, 2)), 'dap', 0, 1, tiled=True)
        m = row_attention(m, row_keys, row_bias, w_row_in[1], w_row_out[1], 16, 24, True)
        te_bias = bias(z, w_te_bias[1], 'ijc,ch->hji', 2)
        z = row_attention(z, tri_keys, te_bias, w_te_in[1], w_te_out[1], 4, 32, False)
        z = lax.all_to_all(jnp.transpose(z, (1, 0, 2)), 'dap', 0, 1, tiled=True)
        ts_bias = bias(z, w_ts_bias[1], 'ijc,ch->hji', 2)
        z = row_attention(z, tri_keys, ts_bias, w_ts_in[1], w_ts_out[1], 4, 32, False)
        return m, z

    in_specs = (P(('data', 'dap')), P(('data', 'dap')), P('data'), P('data')) + (P(),) * 13
    out_specs = (P(('data', 'dap')), P(('data', 'dap')))
    return jax.shard_map(local_step, mesh=mesh, in_specs=in_specs, out_specs=out_specs, check_vma=False)
```

```python
import functools

import jax
import jax.numpy as jnp
from jax import lax
from jax.experimental import pallas as pl
from jax.experimental.pallas import tpu as pltpu
from jax.sharding import PartitionSpec as P

LOG2E = 1.4426950408889634
NEG = -1e9 * LOG2E
F32 = jnp.float32
BF16 = jnp.bfloat16
LAG = 2
SLOTS = 4
NT = (((1,), (1,)), ((), ()))


def layer_norm(values):
    flat = values.astype(F32)
    row_mean = jnp.mean(flat, axis=-1, keepdims=True)
    centered = flat - row_mean
    row_var = jnp.mean(centered * centered, axis=-1, keepdims=True)
    return (centered * lax.rsqrt(row_var + 1e-5)).astype(BF16)


def half_masks(rows, split):
    index = lax.broadcasted_iota(jnp.int32, (rows, 128), 0)
    upper = (index < split).astype(F32).astype(BF16)
    lower = (index >= split).astype(F32).astype(BF16)
    return upper, lower


def attend_units(pt_ref, gt_ref, kt_ref, lg_ref, pr_ref, heads, dim, keep, bias_ref, work):
    width = heads * dim
    rows = 2 * dim
    pairs = heads // 2
    units = 2 * pairs
    up, low = half_masks(rows, dim)
    scale = dim ** -0.5 * LOG2E
    if bias_ref is not None:
        left = lax.broadcasted_iota(jnp.int32, (64, 128), 1) < 64
        left_b = left.astype(F32).astype(BF16)
        right_b = (1.0 - left.astype(F32)).astype(BF16)

    def place(unit):
        return pl.ds(unit // pairs * 128, 128), rows * (unit % pairs)

    def turn_keys(unit):
        ln, r = place(unit)
        kt_ref[unit % SLOTS] = pt_ref[pl.ds(width + r, rows), ln].T

    def make_logits(unit):
        ln, r = place(unit)
        q = pt_ref[pl.ds(r, rows), ln]
        rhs = jnp.concatenate([q * up, q * low], axis=1)
        logits2 = jnp.dot(kt_ref[unit % SLOTS], rhs, preferred_element_type=F32)
        for half in range(2):
            lg = logits2[:, 128 * half:128 * half + 128]
            if bias_ref is not None:
                lg = jnp.where(left, lg[0:64], lg[64:128])
            lg_ref[unit % SLOTS, half] = lg

    def soften(unit):
        blk, hp = unit // pairs, unit % pairs
        for half in range(2):
            lg = lg_ref[unit % SLOTS, half] * scale
            if bias_ref is not None:
                lg = lg + bias_ref[2 * hp + half]
            lg = jnp.where(keep[blk], lg, NEG)
            e = jnp.exp2(lg - jnp.max(lg, axis=0, keepdims=True))
            p = (e * (1.0 / jnp.sum(e, axis=0, keepdims=True))).astype(BF16)
            pr_ref[unit % SLOTS, half] = p

    def mix(unit):
        ln, r = place(unit)
        v = pt_ref[pl.ds(2 * width + r, rows), ln]
        g = pt_ref[pl.ds(3 * width + r, rows), ln]
        probs = []
        for half in range(2):
            p = pr_ref[unit % SLOTS, half]
            probs += [p] if bias_ref is None else [p * left_b, p * right_b]
        att = jnp.dot(jnp.concatenate([v * up, v * low], axis=1), jnp.concatenate(probs, axis=0), preferred_element_type=F32)
        gt_ref[pl.ds(r, rows), ln] = (att * jax.nn.sigmoid(g.astype(F32))).astype(BF16)

    stages = ((turn_keys, 0), (make_logits, LAG), (soften, 2 * LAG), (mix, 3 * LAG))
    ticks = units + 3 * LAG
    for tick in range(ticks):
        for stage, lag in stages:
            if 0 <= tick - lag < units:
                stage(tick - lag)
        for job in work[len(work) * tick // ticks:len(work) * (tick + 1) // ticks]:
            job()


def attend_step(half, scratch, heads, dim, x_new, w, keep, bias_ref, x_old, wo, finish):
    ln_ref, pt_refs, gt_refs, others = scratch[0], scratch[1:3], scratch[3:5], scratch[5:8]
    width = heads * dim
    chunk = 256 if width > 256 else 128

    def norm():
        ln_ref[...] = layer_norm(x_new())

    def project(part):
        def job():
            sl = pl.ds(part * chunk, chunk)
            pt_refs[half][sl, :] = lax.dot_general(w(sl), ln_ref[...], NT, preferred_element_type=F32).astype(BF16)
        return job

    def leave():
        update = jnp.dot(gt_refs[half][...].T, wo(), preferred_element_type=F32)
        finish((x_old() + update).astype(BF16))

    work = [norm, leave] + [project(part) for part in range(4 * width // chunk)]
    attend_units(pt_refs[1 - half], gt_refs[1 - half], *others, heads, dim, keep, bias_ref, work)


def attend_scratch(heads, dim, keys, channels):
    inner = heads * dim
    return [
        pltpu.VMEM((256, channels), BF16),
        pltpu.VMEM((4 * inner, 256), BF16),
        pltpu.VMEM((4 * inner, 256), BF16),
        pltpu.VMEM((inner, 256), BF16),
        pltpu.VMEM((inner, 256), BF16),
        pltpu.VMEM((SLOTS, 128, 2 * dim), BF16),
        pltpu.VMEM((SLOTS, 2, keys, 128), F32),
        pltpu.VMEM((SLOTS, 2, keys, 128), BF16),
    ]


def pick_column(table, col):
    lane = lax.broadcasted_iota(jnp.int32, table.shape, 1)
    return jnp.sum(jnp.where(lane == col, table, 0.0), axis=1, keepdims=True)


def row_kernel(heads, dim, per_row, blocks, x_ref, keys_ref, bias_ref, w_ref, wo_ref, out_ref, *scratch):
    channels = x_ref.shape[-1]
    left = lax.broadcasted_iota(jnp.int32, (64, 128), 1) < 64

    def body(turn, carry):
        for half in range(2):
            i = 2 * turn + half
            new = jnp.minimum(i, blocks - 1)
            mid = jnp.clip(i - 1, 0, blocks - 1)
            old = jnp.clip(i - 2, 0, blocks - 1)
            keep = []
            for blk in range(2):
                if per_row:
                    first = pick_column(keys_ref[...], mid * 4 + 2 * blk)
                    second = pick_column(keys_ref[...], mid * 4 + 2 * blk + 1)
                    keep.append(jnp.where(left, first, second) > 0.5)
                else:
                    keep.append(jnp.broadcast_to(keys_ref[...], (64, 128)) > 0.5)
            read = lambda at: x_ref[pl.ds(at * 4, 4)].astype(F32).reshape(256, channels)

            def finish(out):
                out_ref[pl.ds(old * 4, 4)] = out.reshape(4, 64, channels)

            attend_step(half, scratch, heads, dim, lambda: read(new), lambda sl: w_ref[sl, :], keep, bias_ref,
                        lambda: read(old), lambda: wo_ref[...], finish)
        return carry

    lax.fori_loop(0, blocks // 2 + 1, body, 0)


def row_attention(x, keys, bias_t, w, wo, heads, dim, per_row):
    groups, length, width = x.shape
    bias_t = bias_t.astype(F32) * LOG2E
    bias_t = jnp.concatenate([bias_t, bias_t], axis=2)
    return pl.pallas_call(
        functools.partial(row_kernel, heads, dim, per_row, groups // 4),
        out_shape=jax.ShapeDtypeStruct(x.shape, BF16),
        scratch_shapes=attend_scratch(heads, dim, 64, width),
        cost_estimate=pl.CostEstimate(flops=groups * length * width * heads * dim * 10, bytes_accessed=x.size * 4, transcendentals=0),
        name="row_att" if per_row else "tri_att",
    )(x, keys, bias_t, w, wo)


def col_kernel(x_ref, keys_ref, lanes_ref, w_ref, wo_ref, wp_ref, out_ref, ac_ref, m_ref, *scratch):
    m_ref[0] = x_ref[...]

    def body(turn, carry):
        for half in range(2):
            i = 2 * turn + half
            new = jnp.minimum(i, 15)
            mid = jnp.clip(i - 1, 0, 15)
            old = jnp.clip(i - 2, 0, 15)
            keep = [jnp.broadcast_to(pick_column(keys_ref[...], mid % 8 * 2 + blk), (128, 128)) > 0.5 for blk in range(2)]
            read = lambda at: m_ref[at // 8, pl.ds(at % 8 * 2, 2)].astype(F32).reshape(256, 384)

            def finish(out):
                m_ref[old // 8 + 1, pl.ds(old % 8 * 2, 2)] = out.reshape(2, 128, 384)
                ac = lax.dot_general(wp_ref[old // 8], layer_norm(out), NT, preferred_element_type=F32)
                lane_mask = jnp.concatenate([lanes_ref[old % 8 * 2], lanes_ref[old % 8 * 2 + 1]], axis=1)
                ac_ref[old // 8, old % 8] = (ac * lane_mask).astype(BF16)

            attend_step(half, scratch, 16, 24, lambda: read(new), lambda sl: w_ref[new // 8, sl, :], keep, None,
                        lambda: read(old), lambda: wo_ref[old // 8], finish)
        return carry

    lax.fori_loop(0, 9, body, 0)
    out_ref[...] = m_ref[2]


def column_pair(x, keys, lanes, w, wo, wp):
    return pl.pallas_call(
        col_kernel,
        out_shape=[
            jax.ShapeDtypeStruct(x.shape, BF16),
            jax.ShapeDtypeStruct((2, 8, 64, 256), BF16),
        ],
        scratch_shapes=[pltpu.VMEM((3, 16, 128, 384), BF16)] + attend_scratch(16, 24, 128, 384),
        cost_estimate=pl.CostEstimate(flops=2048 * 384 * 384 * 20, bytes_accessed=x.size * 4, transcendentals=0),
        name="col_att",
    )(x, keys, lanes, w, wo, wp)


def opm_kernel(own_ref, full_ref, z_ref, norm_ref, w_ref, out_ref, full32_ref, o_ref):
    full32_ref[...] = full_ref[...].astype(F32)
    own = own_ref[...]
    zeros = jnp.zeros((64, 128), BF16)

    def one(q, carry):
        c_q = full32_ref[pl.ds(q, 64, stride=32), :].astype(BF16)
        rhs = jnp.concatenate([jnp.concatenate([c_q, zeros], axis=1), jnp.concatenate([zeros, c_q], axis=1)], axis=0)
        o = lax.dot_general(own, rhs, NT, preferred_element_type=F32).astype(BF16)
        for pair in range(8):
            o_ref[pair, pl.ds(pl.multiple_of(q * 32, 32), 32), :] = o[32 * pair:32 * pair + 32]
        return carry

    lax.fori_loop(0, 32, one, 0, unroll=4)
    w = w_ref[...]
    for pair in range(8):
        update = jnp.dot(w, o_ref[pair], preferred_element_type=F32).T
        z = z_ref[pl.ds(2 * pair, 2)].astype(F32).reshape(128, 128)
        norm = norm_ref[...]
        norm = jnp.concatenate([pick_column(norm, 2 * pair), pick_column(norm, 2 * pair + 1)], axis=0)
        out_ref[pl.ds(2 * pair, 2)] = (z + update / (1e-3 + norm)).astype(BF16).reshape(2, 64, 128)


def opm(own, full, z, norm, w):
    return pl.pallas_call(
        opm_kernel,
        out_shape=jax.ShapeDtypeStruct(z.shape, BF16),
        scratch_shapes=[pltpu.VMEM((2048, 128), F32), pltpu.VMEM((8, 1024, 128), BF16)],
        cost_estimate=pl.CostEstimate(flops=10 ** 9, bytes_accessed=2 ** 20, transcendentals=0),
        name="opm",
    )(own, full, z, norm, w)


def solution(mesh):
    def local_step(m, z, mask, res_mask, w_row_bias, w_row_in, w_row_out, w_col_in, w_col_out, w_opm_in, w_opm_out, w_ts_bias, w_ts_in, w_ts_out, w_te_bias, w_te_in, w_te_out):
        dev = lax.axis_index('dap')
        flat_in = lambda w: jnp.transpose(w, (0, 2, 3, 4, 1)).reshape(2, -1, w.shape[1])
        flat_out = lambda w: w.reshape(2, -1, w.shape[-1])
        w_row_in, w_col_in, w_ts_in, w_te_in = map(flat_in, (w_row_in, w_col_in, w_ts_in, w_te_in))
        w_row_out, w_col_out, w_ts_out, w_te_out = map(flat_out, (w_row_out, w_col_out, w_ts_out, w_te_out))
        w_opm_in = jnp.transpose(w_opm_in, (0, 2, 3, 1)).reshape(2, 64, 384)
        w_opm_1 = jnp.transpose(w_opm_out[0], (2, 1, 0)).reshape(128, 1024)
        w_opm_2 = jnp.transpose(w_opm_out[1], (2, 0, 1)).reshape(128, 1024)

        mask_f = mask.astype(F32)
        row_keys = lax.dynamic_slice_in_dim(mask_f, dev * 32, 32, 0).T
        col_keys = lax.dynamic_slice_in_dim(mask_f, dev * 16, 16, 1)
        lanes = col_keys.T.reshape(16, 1, 128)
        tri_keys = res_mask.astype(F32).reshape(64, 1)
        norm = jnp.dot(mask_f.T, col_keys)

        def bias(z_blk, w, form, axis):
            part = jnp.einsum(form, layer_norm(z_blk), w, preferred_element_type=F32).astype(BF16)
            return lax.all_gather(part, 'dap', axis=axis, tiled=True)

        def gather_full(half):
            full = lax.all_gather(half.reshape(8, 32, 2, 128).transpose(0, 2, 1, 3).reshape(512, 128), 'dap', axis=0, tiled=True)
            return full

        row_bias = bias(z, w_row_bias[0], 'ijc,ch->hji', 2)
        m = row_attention(m, row_keys, row_bias, w_row_in[0], w_row_out[0], 16, 24, True)
        m = lax.all_to_all(m, 'dap', 1, 0, tiled=True)
        m = jnp.transpose(m, (1, 0, 2))
        m, (ac1, ac2) = column_pair(m, col_keys, lanes, w_col_in, w_col_out, w_opm_in)
        z = opm(ac1[:, :32].reshape(256, 256), gather_full(ac1[:, 32:]), z, norm, w_opm_1)
        ts_bias = bias(z, w_ts_bias[0], 'ijc,ch->hji', 2)
        z = row_attention(z, tri_keys, ts_bias, w_ts_in[0], w_ts_out[0], 4, 32, False)
        z = jnp.transpose(lax.all_to_all(z, 'dap', 1, 0, tiled=True), (1, 0, 2))
        te_bias = bias(z, w_te_bias[0], 'ijc,ch->hji', 2)
        z = row_attention(z, tri_keys, te_bias, w_te_in[0], w_te_out[0], 4, 32, False)

        row_bias = bias(z, w_row_bias[1], 'jic,ch->hji', 1)
        z = opm(ac2[:, 32:].reshape(256, 256), gather_full(ac2[:, :32]), z, norm, w_opm_2)
        m = lax.all_to_all(jnp.transpose(m, (1, 0, 2)), 'dap', 0, 1, tiled=True)
        m = row_attention(m, row_keys, row_bias, w_row_in[1], w_row_out[1], 16, 24, True)
        te_bias = bias(z, w_te_bias[1], 'ijc,ch->hji', 2)
        z = row_attention(z, tri_keys, te_bias, w_te_in[1], w_te_out[1], 4, 32, False)
        z = lax.all_to_all(jnp.transpose(z, (1, 0, 2)), 'dap', 0, 1, tiled=True)
        ts_bias = bias(z, w_ts_bias[1], 'ijc,ch->hji', 2)
        z = row_attention(z, tri_keys, ts_bias, w_ts_in[1], w_ts_out[1], 4, 32, False)
        return m, z

    in_specs = (P(('data', 'dap')), P(('data', 'dap')), P('data'), P('data')) + (P(),) * 13
    out_specs = (P(('data', 'dap')), P(('data', 'dap')))
    return jax.shard_map(local_step, mesh=mesh, in_specs=in_specs, out_specs=out_specs, check_vma=False)
```

```python
import functools

import jax
import jax.numpy as jnp
from jax import lax
from jax.experimental import pallas as pl
from jax.experimental.pallas import tpu as pltpu
from jax.sharding import PartitionSpec as P

LOG2E = 1.4426950408889634
NEG = -1e9 * LOG2E
F32 = jnp.float32
BF16 = jnp.bfloat16
LAG = 2
SLOTS = 4
NT = (((1,), (1,)), ((), ()))
LANES = 128
RES = 64
BLOCK = 256
HELD = 16
WIDE = 384
CELLS = 1024


def layer_norm(values):
    flat = values.astype(F32)
    row_mean = jnp.mean(flat, axis=-1, keepdims=True)
    centered = flat - row_mean
    row_var = jnp.mean(centered * centered, axis=-1, keepdims=True)
    return (centered * lax.rsqrt(row_var + 1e-5)).astype(BF16)


def half_masks(rows, split):
    index = lax.broadcasted_iota(jnp.int32, (rows, LANES), 0)
    upper = (index < split).astype(F32).astype(BF16)
    lower = (index >= split).astype(F32).astype(BF16)
    return upper, lower


def attend_units(pt_ref, gt_ref, kt_ref, lg_ref, pr_ref, heads, dim, keep, bias_ref, work):
    width = heads * dim
    rows = 2 * dim
    pairs = heads // 2
    units = 2 * pairs
    up, low = half_masks(rows, dim)
    scale = dim ** -0.5 * LOG2E
    if bias_ref is not None:
        left = lax.broadcasted_iota(jnp.int32, (RES, LANES), 1) < RES
        left_b = left.astype(F32).astype(BF16)
        right_b = (1.0 - left.astype(F32)).astype(BF16)

    def place(unit):
        return pl.ds(unit // pairs * LANES, LANES), rows * (unit % pairs)

    def turn_keys(unit):
        ln, r = place(unit)
        kt_ref[unit % SLOTS] = pt_ref[pl.ds(width + r, rows), ln].T

    def make_logits(unit):
        ln, r = place(unit)
        q = pt_ref[pl.ds(r, rows), ln]
        rhs = jnp.concatenate([q * up, q * low], axis=1)
        logits2 = jnp.dot(kt_ref[unit % SLOTS], rhs, preferred_element_type=F32)
        for half in range(2):
            lg = logits2[:, LANES * half:LANES * half + LANES]
            if bias_ref is not None:
                lg = jnp.where(left, lg[0:RES], lg[RES:LANES])
            lg_ref[unit % SLOTS, half] = lg

    def soften(unit):
        blk, hp = unit // pairs, unit % pairs
        for half in range(2):
            lg = lg_ref[unit % SLOTS, half] * scale
            if bias_ref is not None:
                lg = lg + bias_ref[2 * hp + half]
            lg = jnp.where(keep[blk], lg, NEG)
            e = jnp.exp2(lg - jnp.max(lg, axis=0, keepdims=True))
            p = (e * (1.0 / jnp.sum(e, axis=0, keepdims=True))).astype(BF16)
            pr_ref[unit % SLOTS, half] = p

    def mix(unit):
        ln, r = place(unit)
        v = pt_ref[pl.ds(2 * width + r, rows), ln]
        g = pt_ref[pl.ds(3 * width + r, rows), ln]
        probs = []
        for half in range(2):
            p = pr_ref[unit % SLOTS, half]
            probs += [p] if bias_ref is None else [p * left_b, p * right_b]
        att = jnp.dot(jnp.concatenate([v * up, v * low], axis=1), jnp.concatenate(probs, axis=0), preferred_element_type=F32)
        gt_ref[pl.ds(r, rows), ln] = (att * jax.nn.sigmoid(g.astype(F32))).astype(BF16)

    stages = ((turn_keys, 0), (make_logits, LAG), (soften, 2 * LAG), (mix, 3 * LAG))
    ticks = units + 3 * LAG
    for tick in range(ticks):
        for stage, lag in stages:
            if 0 <= tick - lag < units:
                stage(tick - lag)
        for job in work[len(work) * tick // ticks:len(work) * (tick + 1) // ticks]:
            job()


def attend_step(half, scratch, heads, dim, x_new, w, keep, bias_ref, x_old, wo, finish):
    ln_ref, pt_refs, gt_refs, others = scratch[0], scratch[1:3], scratch[3:5], scratch[5:8]
    width = heads * dim
    chunk = BLOCK if width > BLOCK else LANES

    def norm():
        ln_ref[...] = layer_norm(x_new())

    def project(part):
        def job():
            sl = pl.ds(part * chunk, chunk)
            pt_refs[half][sl, :] = lax.dot_general(w(sl), ln_ref[...], NT, preferred_element_type=F32).astype(BF16)
        return job

    def leave():
        update = jnp.dot(gt_refs[half][...].T, wo(), preferred_element_type=F32)
        finish((x_old() + update).astype(BF16))

    work = [norm, leave] + [project(part) for part in range(4 * width // chunk)]
    attend_units(pt_refs[1 - half], gt_refs[1 - half], *others, heads, dim, keep, bias_ref, work)


def attend_scratch(heads, dim, keys, channels):
    inner = heads * dim
    return [
        pltpu.VMEM((BLOCK, channels), BF16),
        pltpu.VMEM((4 * inner, BLOCK), BF16),
        pltpu.VMEM((4 * inner, BLOCK), BF16),
        pltpu.VMEM((inner, BLOCK), BF16),
        pltpu.VMEM((inner, BLOCK), BF16),
        pltpu.VMEM((SLOTS, LANES, 2 * dim), BF16),
        pltpu.VMEM((SLOTS, 2, keys, LANES), F32),
        pltpu.VMEM((SLOTS, 2, keys, LANES), BF16),
    ]


def pick_column(table, col):
    lane = lax.broadcasted_iota(jnp.int32, table.shape, 1)
    return jnp.sum(jnp.where(lane == col, table, 0.0), axis=1, keepdims=True)


def row_kernel(heads, dim, per_row, blocks, x_ref, keys_ref, bias_ref, w_ref, wo_ref, out_ref, *scratch):
    channels = x_ref.shape[-1]
    left = lax.broadcasted_iota(jnp.int32, (RES, LANES), 1) < RES

    def body(turn, carry):
        for half in range(2):
            i = 2 * turn + half
            new = jnp.minimum(i, blocks - 1)
            mid = jnp.clip(i - 1, 0, blocks - 1)
            old = jnp.clip(i - 2, 0, blocks - 1)
            keep = []
            for blk in range(2):
                if per_row:
                    first = pick_column(keys_ref[...], mid * 4 + 2 * blk)
                    second = pick_column(keys_ref[...], mid * 4 + 2 * blk + 1)
                    keep.append(jnp.where(left, first, second) > 0.5)
                else:
                    keep.append(jnp.broadcast_to(keys_ref[...], (RES, LANES)) > 0.5)
            read = lambda at: x_ref[pl.ds(at * 4, 4)].astype(F32).reshape(BLOCK, channels)

            def finish(out):
                out_ref[pl.ds(old * 4, 4)] = out.reshape(4, RES, channels)

            attend_step(half, scratch, heads, dim, lambda: read(new), lambda sl: w_ref[sl, :], keep, bias_ref,
                        lambda: read(old), lambda: wo_ref[...], finish)
        return carry

    lax.fori_loop(0, blocks // 2 + 1, body, 0)


def row_attention(x, keys, bias_t, w, wo, heads, dim, per_row):
    groups, length, width = x.shape
    bias_t = bias_t.astype(F32) * LOG2E
    return pl.pallas_call(
        functools.partial(row_kernel, heads, dim, per_row, groups // 4),
        out_shape=jax.ShapeDtypeStruct(x.shape, BF16),
        scratch_shapes=attend_scratch(heads, dim, RES, width),
        cost_estimate=pl.CostEstimate(flops=groups * length * width * heads * dim * 10, bytes_accessed=x.size * 4, transcendentals=0),
        name="row_att" if per_row else "tri_att",
    )(x, keys, bias_t, w, wo)


def col_kernel(x_ref, keys_ref, lanes_ref, w_ref, wo_ref, wp_ref, out_ref, pairs_ref, singles_ref, m_ref, *scratch):
    m_ref[0] = x_ref[...]

    def body(turn, carry):
        for half in range(2):
            i = 2 * turn + half
            new = jnp.minimum(i, 15)
            mid = jnp.clip(i - 1, 0, 15)
            old = jnp.clip(i - 2, 0, 15)
            keep = [jnp.broadcast_to(pick_column(keys_ref[...], mid % 8 * 2 + blk), (LANES, LANES)) > 0.5 for blk in range(2)]
            read = lambda at: m_ref[at // 8, pl.ds(at % 8 * 2, 2)].astype(F32).reshape(BLOCK, WIDE)

            def finish(out):
                m_ref[old // 8 + 1, pl.ds(old % 8 * 2, 2)] = out.reshape(2, LANES, WIDE)
                ac = lax.dot_general(wp_ref[old // 8], layer_norm(out), NT, preferred_element_type=F32)
                lane_mask = jnp.concatenate([lanes_ref[old % 8 * 2], lanes_ref[old % 8 * 2 + 1]], axis=1)
                ac = (ac * lane_mask).astype(BF16)
                own, part = ac[:32], ac[32:]
                pairs_ref[old // 8, 0, old % 8] = own
                pairs_ref[old // 8, 1, old % 8] = part
                for blk in range(2):
                    singles_ref[old // 8, 0, old % 8 * 2 + blk] = own[:, LANES * blk:LANES * blk + LANES]
                    singles_ref[old // 8, 1, old % 8 * 2 + blk] = part[:, LANES * blk:LANES * blk + LANES]

            attend_step(half, scratch, HELD, 24, lambda: read(new), lambda sl: w_ref[new // 8, sl, :], keep, None,
                        lambda: read(old), lambda: wo_ref[old // 8], finish)
        return carry

    lax.fori_loop(0, 9, body, 0)
    out_ref[...] = m_ref[2]


def column_pair(x, keys, lanes, w, wo, wp):
    return pl.pallas_call(
        col_kernel,
        out_shape=[
            jax.ShapeDtypeStruct(x.shape, BF16),
            jax.ShapeDtypeStruct((2, 2, 8, 32, BLOCK), BF16),
            jax.ShapeDtypeStruct((2, 2, HELD, 32, LANES), BF16),
        ],
        scratch_shapes=[pltpu.VMEM((3, HELD, LANES, WIDE), BF16)] + attend_scratch(HELD, 24, LANES, WIDE),
        cost_estimate=pl.CostEstimate(flops=2048 * WIDE * WIDE * 20, bytes_accessed=x.size * 4, transcendentals=0),
        name="col_att",
    )(x, keys, lanes, w, wo, wp)


def greet(me):
    barrier = pltpu.get_barrier_semaphore()
    for o in range(1, 4):
        pl.semaphore_signal(barrier, inc=1, device_id={'dap': lax.rem(me + o, 4)}, device_id_type=pl.DeviceIdType.MESH)
    pl.semaphore_wait(barrier, 3)


def push(me, kind, send_sem, recv_sem, source, target):
    copies = []
    for o in range(1, 4):
        peer = lax.rem(me + o, 4)
        copy = pltpu.make_async_remote_copy(
            src_ref=source(peer), dst_ref=target, send_sem=send_sem.at[3 * kind + o - 1],
            recv_sem=recv_sem.at[3 * kind + o - 1], device_id={'dap': peer}, device_id_type=pl.DeviceIdType.MESH)
        copy.start()
        copies.append(copy)
    return copies


def finish_all(copies):
    for copy in copies:
        copy.wait()


def local_bias_rows(ln_ref, w_ref):
    rows = w_ref.shape[0]
    index = lax.broadcasted_iota(jnp.int32, (rows, LANES), 0) % HELD
    total = jnp.zeros((rows, LANES), F32)
    for b in range(HELD):
        mine = w_ref[...] * (index == b).astype(F32).astype(BF16)
        part = ln_ref[pl.ds(RES * b, RES), :]
        total += lax.dot_general(mine, jnp.concatenate([part, part], axis=0), NT, preferred_element_type=F32)
    return total.astype(BF16)


def local_bias_lanes(me, ln_ref, w_ref):
    lane = lax.broadcasted_iota(jnp.int32, (1, BLOCK), 1) % RES
    total = jnp.zeros((RES, BLOCK), F32)
    for q in range(HELD):
        mine = w_ref[...] * (lane == HELD * me + q).astype(F32).astype(BF16)
        total += jnp.dot(ln_ref[pl.ds(RES * q, RES), :], mine, preferred_element_type=F32)
    return total.astype(BF16)


def triangle(zf_ref, ln_ref, w_ref, wo_ref, keep, bias_ref, pt_refs, gt_refs, others, ready):
    def project(block, part):
        def job():
            pt_refs[block % 2][pl.ds(LANES * part, LANES), :] = lax.dot_general(
                w_ref[pl.ds(LANES * part, LANES), :], ln_ref[pl.ds(BLOCK * block, BLOCK), :], NT,
                preferred_element_type=F32).astype(BF16)
        return job

    def leave(block):
        def job():
            update = jnp.dot(gt_refs[block % 2][...].T, wo_ref[...], preferred_element_type=F32)
            rows = pl.ds(BLOCK * block, BLOCK)
            zf_ref[rows, :] = (zf_ref[rows, :] + update).astype(BF16).astype(F32)
        return job

    for part in range(4):
        project(0, part)()
    ready()
    for block in range(4):
        work = [leave(block - 1)] if block else []
        if block < 3:
            work += [project(block + 1, part) for part in range(4)]
        attend_units(pt_refs[block % 2], gt_refs[block % 2], *others, 4, 32, [keep, keep], bias_ref, work)
    leave(3)()


def pair_kernel(has_next, own_ref, part_ref, z_ref, norm_ref, keys_ref, wm_ref, wba_ref, wa_ref, woa_ref, wbb_ref, wb_ref, wob_ref, *rest):
    if has_next:
        wn_ref, out_ref, next_ref = rest[:3]
        rest = rest[3:]
    else:
        out_ref = rest[0]
        rest = rest[1:]
    (full_ref, full32_ref, o_ref, zf_ref, zt_ref, ln_ref, lanes_ref, bias_ref, rows_ref, all_rows_ref, zs_ref, zr_ref,
     send_sem, recv_sem) = rest[:14]
    nl_ref = rest[14]
    att = rest[15:]
    pt_refs, gt_refs, others = att[0:2], att[2:4], att[4:7]
    me = lax.axis_index('dap')
    mine = pl.ds(pl.multiple_of(HELD * me, HELD), HELD)
    greet(me)
    copies = push(me, 0, send_sem, recv_sem, lambda peer: part_ref, full_ref.at[mine])
    full_ref[mine] = part_ref[...]
    keep = jnp.broadcast_to(keys_ref[...], (RES, LANES)) > 0.5
    left = lax.broadcasted_iota(jnp.int32, (RES, LANES), 1) < RES
    finish_all(copies)

    full32_ref[...] = full_ref[...].astype(F32).reshape(2048, LANES)
    own = own_ref[...].reshape(BLOCK, BLOCK)
    zeros = jnp.zeros((RES, LANES), BF16)

    def one(q, carry):
        c_q = full32_ref[pl.ds(q, RES, stride=32), :].astype(BF16)
        rhs = jnp.concatenate([jnp.concatenate([c_q, zeros], axis=1), jnp.concatenate([zeros, c_q], axis=1)], axis=0)
        o = lax.dot_general(own, rhs, NT, preferred_element_type=F32).astype(BF16)
        for pair in range(8):
            o_ref[pair, pl.ds(pl.multiple_of(q * 32, 32), 32), :] = o[32 * pair:32 * pair + 32]
        return carry

    lax.fori_loop(0, 32, one, 0, unroll=4)
    for pair in range(8):
        update = jnp.dot(wm_ref[...], o_ref[pair], preferred_element_type=F32).T
        z = z_ref[pl.ds(2 * pair, 2)].astype(F32).reshape(LANES, LANES)
        norm = jnp.concatenate([pick_column(norm_ref[...], 2 * pair), pick_column(norm_ref[...], 2 * pair + 1)], axis=0)
        z = (z + update / (1e-3 + norm)).astype(BF16).astype(F32)
        rows = pl.ds(LANES * pair, LANES)
        zf_ref[rows, :] = z
        ln_ref[rows, :] = layer_norm(z)

    lanes_ref[me] = local_bias_lanes(me, ln_ref, wba_ref)
    copies = push(me, 1, send_sem, recv_sem, lambda peer: lanes_ref.at[me], lanes_ref.at[me])

    def lanes_ready():
        finish_all(copies)
        total = (lanes_ref[0].astype(F32) + lanes_ref[1].astype(F32) + lanes_ref[2].astype(F32) + lanes_ref[3].astype(F32)) * LOG2E
        for two in range(2):
            value = total[:, LANES * two:LANES * two + LANES]
            turned = pltpu.roll(value, RES, 1)
            bias_ref[2 * two] = jnp.where(left, value, turned)
            bias_ref[2 * two + 1] = jnp.where(left, turned, value)

    triangle(zf_ref, ln_ref, wa_ref, woa_ref, keep, bias_ref, pt_refs, gt_refs, others, lanes_ready)

    zs_ref[...] = zf_ref[...].astype(BF16).reshape(HELD, RES, LANES)
    for block in range(8):
        rows = pl.ds(LANES * block, LANES)
        ln_ref[rows, :] = layer_norm(zf_ref[rows, :])
    rows_ref[...] = local_bias_rows(ln_ref, wbb_ref).reshape(4, HELD, LANES)
    moved = push(me, 2, send_sem, recv_sem, lambda peer: zs_ref.at[:, pl.ds(pl.multiple_of(HELD * peer, HELD), HELD), :], zr_ref.at[mine])
    copies = push(me, 3, send_sem, recv_sem, lambda peer: rows_ref, all_rows_ref.at[:, mine, :])
    zr_ref[mine] = zs_ref[:, mine, :]
    all_rows_ref[:, mine, :] = rows_ref[...]
    finish_all(moved)
    zt_ref[...] = zr_ref[...].astype(F32).reshape(CELLS, LANES)
    for row in range(HELD):
        value = zt_ref[pl.ds(row, RES, stride=HELD), :]
        zf_ref[pl.ds(RES * row, RES), :] = value
        ln_ref[pl.ds(RES * row, RES), :] = layer_norm(value)

    def rows_ready():
        finish_all(copies)
        bias_ref[...] = all_rows_ref[...].astype(F32) * LOG2E

    triangle(zf_ref, ln_ref, wb_ref, wob_ref, keep, bias_ref, pt_refs, gt_refs, others, rows_ready)
    out_ref[...] = zf_ref[...].astype(BF16).reshape(HELD, RES, LANES)
    if has_next:
        for block in range(8):
            rows = pl.ds(LANES * block, LANES)
            ln_ref[rows, :] = layer_norm(zf_ref[rows, :])
        nl_ref[...] = local_bias_rows(ln_ref, wn_ref).reshape(HELD, HELD, LANES)
        copies = push(me, 4, send_sem, recv_sem, lambda peer: nl_ref, next_ref.at[:, mine, :])
        next_ref[:, mine, :] = nl_ref[...]
        finish_all(copies)


def pair_block(ident, own, part, z, norm, keys, weights, w_next):
    has_next = w_next is not None
    out_shape = [jax.ShapeDtypeStruct(z.shape, BF16)]
    if has_next:
        weights = weights + (w_next,)
        out_shape.append(jax.ShapeDtypeStruct((HELD, RES, LANES), BF16))
    vmem = pl.BlockSpec(memory_space=pltpu.VMEM)
    args = (own, part, z, norm, keys) + weights
    return pl.pallas_call(
        functools.partial(pair_kernel, has_next),
        out_shape=out_shape,
        in_specs=[vmem] * len(args),
        out_specs=[vmem] * len(out_shape),
        scratch_shapes=[
            pltpu.VMEM((RES, 32, LANES), BF16),
            pltpu.VMEM((2048, LANES), F32),
            pltpu.VMEM((8, CELLS, LANES), BF16),
            pltpu.VMEM((CELLS, LANES), F32),
            pltpu.VMEM((CELLS, LANES), F32),
            pltpu.VMEM((CELLS, LANES), BF16),
            pltpu.VMEM((4, RES, BLOCK), BF16),
            pltpu.VMEM((4, RES, LANES), F32),
            pltpu.VMEM((4, HELD, LANES), BF16),
            pltpu.VMEM((4, RES, LANES), BF16),
            pltpu.VMEM((HELD, RES, LANES), BF16),
            pltpu.VMEM((RES, HELD, LANES), BF16),
            pltpu.SemaphoreType.DMA((15,)),
            pltpu.SemaphoreType.DMA((15,)),
            pltpu.VMEM((HELD, HELD, LANES), BF16),
        ] + attend_scratch(4, 32, RES, LANES)[1:],
        compiler_params=pltpu.CompilerParams(collective_id=ident, has_side_effects=True),
        cost_estimate=pl.CostEstimate(flops=10 ** 10, bytes_accessed=2 ** 22, transcendentals=0),
        name="pair_block",
    )(*args)


def solution(mesh):
    def local_step(m, z, mask, res_mask, w_row_bias, w_row_in, w_row_out, w_col_in, w_col_out, w_opm_in, w_opm_out, w_ts_bias, w_ts_in, w_ts_out, w_te_bias, w_te_in, w_te_out):
        dev = lax.axis_index('dap')
        flat_in = lambda w: jnp.transpose(w, (0, 2, 3, 4, 1)).reshape(2, -1, w.shape[1])
        flat_out = lambda w: w.reshape(2, -1, w.shape[-1])
        w_row_in, w_col_in, w_ts_in, w_te_in = map(flat_in, (w_row_in, w_col_in, w_ts_in, w_te_in))
        w_row_out, w_col_out, w_ts_out, w_te_out = map(flat_out, (w_row_out, w_col_out, w_ts_out, w_te_out))
        w_opm_in = jnp.transpose(w_opm_in, (0, 2, 3, 1)).reshape(2, RES, WIDE)
        w_opm_1 = jnp.transpose(w_opm_out[0], (2, 1, 0)).reshape(LANES, CELLS)
        w_opm_2 = jnp.transpose(w_opm_out[1], (2, 0, 1)).reshape(LANES, CELLS)

        mask_f = mask.astype(F32)
        row_keys = lax.dynamic_slice_in_dim(mask_f, dev * 32, 32, 0).T
        col_keys = lax.dynamic_slice_in_dim(mask_f, dev * HELD, HELD, 1)
        lanes = col_keys.T.reshape(HELD, 1, LANES)
        tri_keys = res_mask.astype(F32).reshape(RES, 1)
        norm = jnp.dot(mask_f.T, col_keys)

        def bias(z_blk, w, form, axis):
            part = jnp.einsum(form, layer_norm(z_blk), w, preferred_element_type=F32).astype(BF16)
            return lax.all_gather(part, 'dap', axis=axis, tiled=True)

        def by_key(w):
            return jnp.repeat(w.T, HELD, axis=0)

        def by_query(w):
            return jnp.repeat(w, RES, axis=1)

        row_bias = bias(z, w_row_bias[0], 'ijc,ch->hji', 2)
        row_bias = jnp.concatenate([row_bias, row_bias], axis=2)
        m = row_attention(m, row_keys, row_bias, w_row_in[0], w_row_out[0], HELD, 24, True)
        m = lax.all_to_all(m, 'dap', 1, 0, tiled=True)
        m = jnp.transpose(m, (1, 0, 2))
        m, pairs, singles = column_pair(m, col_keys, lanes, w_col_in, w_col_out, w_opm_in)
        m = lax.all_to_all(jnp.transpose(m, (1, 0, 2)), 'dap', 0, 1, tiled=True)
        z, row_bias = pair_block(
            0, pairs[0, 0], singles[0, 1], z, norm, tri_keys,
            (w_opm_1, by_query(w_ts_bias[0]), w_ts_in[0], w_ts_out[0], by_key(w_te_bias[0]), w_te_in[0], w_te_out[0]),
            by_key(w_row_bias[1]))

        z, = pair_block(
            1, pairs[1, 1], singles[1, 0], z, norm, tri_keys,
            (w_opm_2, by_query(w_te_bias[1]), w_te_in[1], w_te_out[1], by_key(w_ts_bias[1]), w_ts_in[1], w_ts_out[1]),
            None)
        m = row_attention(m, row_keys, row_bias, w_row_in[1], w_row_out[1], HELD, 24, True)
        return m, z

    in_specs = (P(('data', 'dap')), P(('data', 'dap')), P('data'), P('data')) + (P(),) * 13
    out_specs = (P(('data', 'dap')), P(('data', 'dap')))
    return jax.shard_map(local_step, mesh=mesh, in_specs=in_specs, out_specs=out_specs, check_vma=False)
```

```python
import functools

import jax
import jax.numpy as jnp
from jax import lax
from jax.experimental import pallas as pl
from jax.experimental.pallas import tpu as pltpu
from jax.sharding import PartitionSpec as P

LOG2E = 1.4426950408889634
NEG = -1e9 * LOG2E
F32 = jnp.float32
BF16 = jnp.bfloat16
LAG = 2
SLOTS = 4
NT = (((1,), (1,)), ((), ()))
LANES = 128
RES = 64
BLOCK = 256
HELD = 16
WIDE = 384
CELLS = 1024


def layer_norm(values):
    flat = values.astype(F32)
    row_mean = jnp.mean(flat, axis=-1, keepdims=True)
    centered = flat - row_mean
    row_var = jnp.mean(centered * centered, axis=-1, keepdims=True)
    return (centered * lax.rsqrt(row_var + 1e-5)).astype(BF16)


def half_masks(rows, split):
    index = lax.broadcasted_iota(jnp.int32, (rows, LANES), 0)
    upper = (index < split).astype(F32).astype(BF16)
    lower = (index >= split).astype(F32).astype(BF16)
    return upper, lower


def attend_units(pt_ref, gt_ref, kt_ref, lg_ref, pr_ref, heads, dim, keep, bias_ref, work):
    width = heads * dim
    rows = 2 * dim
    pairs = heads // 2
    units = 2 * pairs
    up, low = half_masks(rows, dim)
    scale = dim ** -0.5 * LOG2E
    if bias_ref is not None:
        left = lax.broadcasted_iota(jnp.int32, (RES, LANES), 1) < RES
        left_b = left.astype(F32).astype(BF16)
        right_b = (1.0 - left.astype(F32)).astype(BF16)

    def place(unit):
        return pl.ds(unit // pairs * LANES, LANES), rows * (unit % pairs)

    def turn_keys(unit):
        ln, r = place(unit)
        kt_ref[unit % SLOTS] = pt_ref[pl.ds(width + r, rows), ln].T

    def make_logits(unit):
        ln, r = place(unit)
        q = pt_ref[pl.ds(r, rows), ln]
        rhs = jnp.concatenate([q * up, q * low], axis=1)
        logits2 = jnp.dot(kt_ref[unit % SLOTS], rhs, preferred_element_type=F32)
        for half in range(2):
            lg = logits2[:, LANES * half:LANES * half + LANES]
            if bias_ref is not None:
                lg = jnp.where(left, lg[0:RES], lg[RES:LANES])
            lg_ref[unit % SLOTS, half] = lg

    def soften(unit):
        blk, hp = unit // pairs, unit % pairs
        for half in range(2):
            lg = lg_ref[unit % SLOTS, half] * scale
            if bias_ref is not None:
                lg = lg + bias_ref[2 * hp + half]
            lg = jnp.where(keep[blk], lg, NEG)
            e = jnp.exp2(lg - jnp.max(lg, axis=0, keepdims=True))
            p = (e * (1.0 / jnp.sum(e, axis=0, keepdims=True))).astype(BF16)
            pr_ref[unit % SLOTS, half] = p

    def mix(unit):
        ln, r = place(unit)
        v = pt_ref[pl.ds(2 * width + r, rows), ln]
        g = pt_ref[pl.ds(3 * width + r, rows), ln]
        probs = []
        for half in range(2):
            p = pr_ref[unit % SLOTS, half]
            probs += [p] if bias_ref is None else [p * left_b, p * right_b]
        att = jnp.dot(jnp.concatenate([v * up, v * low], axis=1), jnp.concatenate(probs, axis=0), preferred_element_type=F32)
        gt_ref[pl.ds(r, rows), ln] = (att * jax.nn.sigmoid(g.astype(F32))).astype(BF16)

    stages = ((turn_keys, 0), (make_logits, LAG), (soften, 2 * LAG), (mix, 3 * LAG))
    ticks = units + 3 * LAG
    for tick in range(ticks):
        for stage, lag in stages:
            if 0 <= tick - lag < units:
                stage(tick - lag)
        for job in work[len(work) * tick // ticks:len(work) * (tick + 1) // ticks]:
            job()


def project(ln_ref, pt_ref, w):
    rows = pt_ref.shape[0]
    chunk = BLOCK if rows > CELLS else LANES

    def job(part):
        sl = pl.ds(part * chunk, chunk)
        pt_ref[sl, :] = lax.dot_general(w(sl), ln_ref[...], NT, preferred_element_type=F32).astype(BF16)
    return [functools.partial(job, part) for part in range(rows // chunk)]


def leave(gt_ref, x_old, wo):
    return (x_old + jnp.dot(gt_ref[...].T, wo, preferred_element_type=F32)).astype(BF16)


def attend_blocks(blocks, scratch, read, w_in, w_out, keep, bias_ref, finish, ready, aside):
    ln_ref, pt_refs, gt_refs, others = scratch[0], scratch[1:3], scratch[3:5], scratch[5:8]
    ln_ref[...] = layer_norm(read(0))
    for job in project(ln_ref, pt_refs[0], w_in(0)):
        job()
    ready()

    def body(turn, carry):
        for half in (1, 0):
            i = 2 * turn + 2 - half
            new = jnp.minimum(i, blocks - 1)
            old = jnp.maximum(i - 2, 0)
            aside(i)

            def norm():
                ln_ref[...] = layer_norm(read(new))

            def done():
                finish(old, leave(gt_refs[half], read(old), w_out(old)))

            work = [norm, done] + project(ln_ref, pt_refs[half], w_in(new))
            attend_units(pt_refs[1 - half], gt_refs[1 - half], *others, 16, 24, keep(i - 1), bias_ref, work)
        return carry

    lax.fori_loop(0, blocks // 2, body, 0)
    finish(blocks - 1, leave(gt_refs[1], read(blocks - 1), w_out(blocks - 1)))


def attend_scratch(heads, dim, keys, channels):
    inner = heads * dim
    return [
        pltpu.VMEM((BLOCK, channels), BF16),
        pltpu.VMEM((4 * inner, BLOCK), BF16),
        pltpu.VMEM((4 * inner, BLOCK), BF16),
        pltpu.VMEM((inner, BLOCK), BF16),
        pltpu.VMEM((inner, BLOCK), BF16),
        pltpu.VMEM((SLOTS, LANES, 2 * dim), BF16),
        pltpu.VMEM((SLOTS, 2, keys, LANES), F32),
        pltpu.VMEM((SLOTS, 2, keys, LANES), BF16),
    ]


def pick_column(table, col):
    lane = lax.broadcasted_iota(jnp.int32, table.shape, 1)
    return jnp.sum(jnp.where(lane == col, table, 0.0), axis=1, keepdims=True)


def row_keep(mask_ref, seq):
    left = lax.broadcasted_iota(jnp.int32, (RES, LANES), 1) < RES
    table = mask_ref[...].astype(F32)
    column = [pick_column(table, seq + n) for n in range(4)]
    return [jnp.where(left, column[2 * blk], column[2 * blk + 1]) > 0.5 for blk in range(2)]


def row_first_kernel(x_ref, z_ref, mask_ref, wb_ref, w_ref, wo_ref, out_ref, mo_ref, lnz_ref, nl_ref, rows_ref, bias_ref,
                     send_sem, recv_sem, *scratch):
    me = lax.axis_index('dap')
    mine = pl.ds(pl.multiple_of(HELD * me, HELD), HELD)
    for part in range(4):
        lnz_ref[pl.ds(BLOCK * part, BLOCK), :] = layer_norm(z_ref[pl.ds(4 * part, 4)].reshape(BLOCK, LANES))
    nl_ref[...] = local_bias_rows(lnz_ref, wb_ref[...]).reshape(HELD, HELD, LANES)
    greet(me)
    copies = push(me, 8, send_sem, recv_sem, lambda peer: nl_ref, rows_ref.at[:, mine, :])
    rows_ref[:, mine, :] = nl_ref[...]

    def ready():
        finish_all(copies)
        bias_by_query(rows_ref, bias_ref)

    def emit(block):
        seqs = pl.ds(4 * block, 4)
        target = pl.ds(32 * me + 4 * block, 4)
        push(me, block, send_sem, recv_sem,
             lambda peer: mo_ref.at[seqs, pl.ds(pl.multiple_of(HELD * peer, HELD), HELD), :], out_ref.at[target])
        out_ref[target] = mo_ref[seqs, mine, :]

    def aside(i):
        @pl.when(i >= 3)
        def _():
            emit(i - 3)

    def finish(block, out):
        mo_ref[pl.ds(4 * block, 4)] = out.reshape(4, RES, WIDE)

    attend_blocks(8, scratch, lambda at: x_ref[pl.ds(at * 4, 4)].astype(F32).reshape(BLOCK, WIDE),
                  lambda at: lambda sl: w_ref[sl, :], lambda at: wo_ref[...],
                  lambda at: row_keep(mask_ref, 32 * me + 4 * at), bias_ref, finish, ready, aside)
    emit(6)
    emit(7)

    def drain(block, carry):
        seqs = pl.ds(4 * block, 4)
        for o in range(1, 4):
            peer = lax.rem(me + o, 4)
            pltpu.make_async_remote_copy(
                src_ref=mo_ref.at[seqs, pl.ds(pl.multiple_of(HELD * peer, HELD), HELD), :],
                dst_ref=out_ref.at[pl.ds(32 * me + 4 * block, 4)], send_sem=send_sem.at[3 * block + o - 1],
                recv_sem=recv_sem.at[3 * block + o - 1], device_id={'dap': peer},
                device_id_type=pl.DeviceIdType.MESH).wait()
        return carry

    lax.fori_loop(0, 8, drain, 0)


def bias_by_query(rows_ref, bias_ref):
    for head in range(rows_ref.shape[0]):
        turned = (rows_ref[head].astype(F32) * LOG2E).T[:RES]
        bias_ref[head] = jnp.concatenate([turned, turned], axis=1)


VMEM = pl.BlockSpec(memory_space=pltpu.VMEM)


def of_layer(array, layer):
    rank = array.ndim - 1
    return pl.BlockSpec((None,) + array.shape[1:], lambda i: (layer,) + (0,) * rank)


def whole(array):
    return pl.BlockSpec(array.shape, lambda i: (0,) * array.ndim)


def row_first(x, z, mask, wb, w, wo):
    return pl.pallas_call(
        row_first_kernel,
        grid=(1,),
        in_specs=[whole(x), whole(z), whole(mask)] + [of_layer(a, 0) for a in (wb, w, wo)],
        out_specs=VMEM,
        out_shape=jax.ShapeDtypeStruct((LANES, HELD, WIDE), BF16),
        scratch_shapes=[
            pltpu.VMEM((32, RES, WIDE), BF16),
            pltpu.VMEM((CELLS, LANES), BF16),
            pltpu.VMEM((HELD, HELD, LANES), BF16),
            pltpu.VMEM((HELD, RES, LANES), BF16),
            pltpu.VMEM((HELD, RES, LANES), F32),
            pltpu.SemaphoreType.DMA((27,)),
            pltpu.SemaphoreType.DMA((27,)),
        ] + attend_scratch(HELD, 24, RES, WIDE),
        compiler_params=pltpu.CompilerParams(collective_id=0, has_side_effects=True),
        cost_estimate=pl.CostEstimate(flops=10 ** 10, bytes_accessed=2 ** 22, transcendentals=0),
        name="row_first",
    )(x, z, mask, wb, w, wo)


def row_last_kernel(x_ref, rows_ref, mask_ref, w_ref, wo_ref, out_ref, wide_ref, m_ref, bias_ref, *scratch):
    me = lax.axis_index('dap')
    turn_tokens(x_ref, wide_ref, m_ref)
    bias_ref[...] = rows_ref[...].astype(F32) * LOG2E

    def finish(block, out):
        out_ref[pl.ds(4 * block, 4)] = out.reshape(4, RES, WIDE)

    attend_blocks(8, scratch, lambda at: m_ref[pl.ds(at * 4, 4)].astype(F32).reshape(BLOCK, WIDE),
                  lambda at: lambda sl: w_ref[sl, :], lambda at: wo_ref[...],
                  lambda at: row_keep(mask_ref, 32 * me + 4 * at), bias_ref, finish, lambda: None, lambda i: None)


def turn_tokens(x_ref, wide_ref, m_ref):
    outer, inner = x_ref.shape[:2]
    for part in range(3):
        lanes = pl.ds(LANES * part, LANES)
        wide_ref[part] = x_ref[:, :, lanes].astype(F32).reshape(outer * inner, LANES)

    def one(row, carry):
        for part in range(3):
            m_ref[row, :, pl.ds(LANES * part, LANES)] = wide_ref[part, pl.ds(row, outer, stride=inner), :].astype(BF16)
        return carry

    lax.fori_loop(0, inner, one, 0, unroll=2)


def row_last(x, rows, mask, w, wo):
    return pl.pallas_call(
        row_last_kernel,
        grid=(1,),
        in_specs=[whole(x), whole(rows), whole(mask)] + [of_layer(a, 1) for a in (w, wo)],
        out_specs=VMEM,
        out_shape=jax.ShapeDtypeStruct((32, RES, WIDE), BF16),
        scratch_shapes=[
            pltpu.VMEM((3, 2048, LANES), F32),
            pltpu.VMEM((32, RES, WIDE), BF16),
            pltpu.VMEM((HELD, RES, LANES), F32),
        ] + attend_scratch(HELD, 24, RES, WIDE),
        cost_estimate=pl.CostEstimate(flops=10 ** 10, bytes_accessed=2 ** 22, transcendentals=0),
        name="row_last",
    )(x, rows, mask, w, wo)


def col_kernel(x_ref, mask_ref, w_ref, wo_ref, wp_ref, out_ref, own1_ref, own2_ref, full1_ref, full2_ref,
               wide_ref, m_ref, part_ref, keys_ref, send_sem, recv_sem, *scratch):
    me = lax.axis_index('dap')
    greet(me)
    turn_tokens(x_ref, wide_ref, m_ref.at[0])
    mine = pl.ds(pl.multiple_of(HELD * me, HELD), HELD)
    keys_ref[...] = mask_ref[mine, :].astype(F32).T

    def keep(at):
        return [jnp.broadcast_to(pick_column(keys_ref[...], at % 8 * 2 + blk), (LANES, LANES)) > 0.5 for blk in range(2)]

    def finish(block, out):
        layer, pair = block // 8, block % 8
        m_ref[layer + 1, pl.ds(pair * 2, 2)] = out.reshape(2, LANES, WIDE)
        ac = lax.dot_general(wp_ref[layer], layer_norm(out), NT, preferred_element_type=F32)
        ac = (ac * jnp.concatenate([mask_ref[pl.ds(HELD * me + 2 * pair + blk, 1), :] for blk in range(2)], axis=1).astype(F32)).astype(BF16)
        parts = (ac[:32], ac[32:])
        own1_ref[pair] = jnp.where(layer == 0, parts[0].astype(F32), own1_ref[pair].astype(F32)).astype(BF16)
        own2_ref[pair] = parts[1]
        for blk in range(2):
            lanes = slice(LANES * blk, LANES * blk + LANES)
            part_ref[block, blk] = jnp.where(layer == 0, parts[1][:, lanes].astype(F32), parts[0][:, lanes].astype(F32)).astype(BF16)

    def part_copies(block, full_ref):
        target = full_ref.at[pl.ds(HELD * me + block % 8 * 2, 2)]
        return [pltpu.make_async_remote_copy(
            src_ref=part_ref.at[block], dst_ref=target, send_sem=send_sem.at[3 * block + o - 1],
            recv_sem=recv_sem.at[3 * block + o - 1], device_id={'dap': lax.rem(me + o, 4)},
            device_id_type=pl.DeviceIdType.MESH) for o in range(1, 4)]

    def seq_copies(pair):
        target = out_ref.at[pl.ds(HELD * me + 2 * pair, 2)]
        return [pltpu.make_async_remote_copy(
            src_ref=m_ref.at[2, pl.ds(2 * pair, 2), pl.ds(pl.multiple_of(32 * lax.rem(me + o, 4), 32), 32), :],
            dst_ref=target, send_sem=send_sem.at[48 + 3 * pair + o - 1], recv_sem=recv_sem.at[48 + 3 * pair + o - 1],
            device_id={'dap': lax.rem(me + o, 4)}, device_id_type=pl.DeviceIdType.MESH) for o in range(1, 4)]

    def emit_first(block):
        for copy in part_copies(block, full1_ref):
            copy.start()
        full1_ref[pl.ds(HELD * me + 2 * block, 2)] = part_ref[block]

    def emit_second(block):
        pair = block - 8
        for copy in part_copies(block, full2_ref) + seq_copies(pair):
            copy.start()
        full2_ref[pl.ds(HELD * me + 2 * pair, 2)] = part_ref[block]
        out_ref[pl.ds(HELD * me + 2 * pair, 2)] = m_ref[2, pl.ds(2 * pair, 2), pl.ds(pl.multiple_of(32 * me, 32), 32), :]

    def aside(i):
        @pl.when(jnp.logical_and(i >= 3, i < 11))
        def _():
            emit_first(i - 3)

        @pl.when(i >= 11)
        def _():
            emit_second(i - 3)

    attend_blocks(16, scratch, lambda at: m_ref[at // 8, pl.ds(at % 8 * 2, 2)].astype(F32).reshape(BLOCK, WIDE),
                  lambda at: lambda sl: w_ref[at // 8, sl, :], lambda at: wo_ref[at // 8],
                  keep, None, finish, lambda: None, aside)
    emit_second(14)
    emit_second(15)

    def drain(pair, carry):
        for copy in part_copies(pair, full1_ref) + part_copies(pair + 8, full2_ref) + seq_copies(pair):
            copy.wait()
        return carry

    lax.fori_loop(0, 8, drain, 0)


def column_pair(x, mask, w, wo, wp):
    return pl.pallas_call(
        col_kernel,
        in_specs=[VMEM] * 5,
        out_specs=[VMEM] * 5,
        out_shape=[
            jax.ShapeDtypeStruct((RES, 32, WIDE), BF16),
            jax.ShapeDtypeStruct((8, 32, BLOCK), BF16),
            jax.ShapeDtypeStruct((8, 32, BLOCK), BF16),
            jax.ShapeDtypeStruct((RES, 32, LANES), BF16),
            jax.ShapeDtypeStruct((RES, 32, LANES), BF16),
        ],
        scratch_shapes=[
            pltpu.VMEM((3, 2048, LANES), F32),
            pltpu.VMEM((3, HELD, LANES, WIDE), BF16),
            pltpu.VMEM((HELD, 2, 32, LANES), BF16),
            pltpu.VMEM((LANES, HELD), F32),
            pltpu.SemaphoreType.DMA((72,)),
            pltpu.SemaphoreType.DMA((72,)),
        ] + attend_scratch(HELD, 24, LANES, WIDE),
        compiler_params=pltpu.CompilerParams(collective_id=1, has_side_effects=True),
        cost_estimate=pl.CostEstimate(flops=10 ** 10, bytes_accessed=2 ** 22, transcendentals=0),
        name="col_pair",
    )(x, mask, w, wo, wp)


def greet(me):
    barrier = pltpu.get_barrier_semaphore()
    for o in range(1, 4):
        pl.semaphore_signal(barrier, inc=1, device_id={'dap': lax.rem(me + o, 4)}, device_id_type=pl.DeviceIdType.MESH)
    pl.semaphore_wait(barrier, 3)


def push(me, kind, send_sem, recv_sem, source, target):
    copies = []
    for o in range(1, 4):
        peer = lax.rem(me + o, 4)
        copy = pltpu.make_async_remote_copy(
            src_ref=source(peer), dst_ref=target, send_sem=send_sem.at[3 * kind + o - 1],
            recv_sem=recv_sem.at[3 * kind + o - 1], device_id={'dap': peer}, device_id_type=pl.DeviceIdType.MESH)
        copy.start()
        copies.append(copy)
    return copies


def finish_all(copies):
    for copy in copies:
        copy.wait()


def local_bias_rows(ln_ref, w):
    heads = w.shape[0]
    spread = jnp.concatenate([jnp.broadcast_to(w[head:head + 1], (HELD, LANES)) for head in range(heads)], axis=0)
    index = lax.broadcasted_iota(jnp.int32, spread.shape, 0) % HELD
    total = jnp.zeros(spread.shape, F32)
    for held in range(HELD):
        chosen = spread * (index == held).astype(F32).astype(BF16)
        part = ln_ref[pl.ds(RES * held, RES), :]
        total += lax.dot_general(chosen, jnp.concatenate([part, part], axis=0), NT, preferred_element_type=F32)
    return total.astype(BF16)


def triangle(zf_ref, ln_ref, w_ref, wo_ref, keep, bias_ref, pt_refs, gt_refs, others, ready):
    def project(block, part):
        def job():
            pt_refs[block % 2][pl.ds(LANES * part, LANES), :] = lax.dot_general(
                w_ref[pl.ds(LANES * part, LANES), :], ln_ref[pl.ds(BLOCK * block, BLOCK), :], NT,
                preferred_element_type=F32).astype(BF16)
        return job

    def leave(block):
        def job():
            update = jnp.dot(gt_refs[block % 2][...].T, wo_ref[...], preferred_element_type=F32)
            rows = pl.ds(BLOCK * block, BLOCK)
            zf_ref[rows, :] = (zf_ref[rows, :] + update).astype(BF16).astype(F32)
        return job

    for part in range(4):
        project(0, part)()
    ready()
    for block in range(4):
        work = [leave(block - 1)] if block else []
        if block < 3:
            work += [project(block + 1, part) for part in range(4)]
        attend_units(pt_refs[block % 2], gt_refs[block % 2], *others, 4, 32, [keep, keep], bias_ref, work)
    leave(3)()


def pair_kernel(has_next, own_ref, full_ref, z_ref, mask_ref, res_ref, wm_ref, wba_ref, wa_ref, woa_ref, wbb_ref, wb_ref, wob_ref, *rest):
    if has_next:
        wn_ref, out_ref, next_ref = rest[:3]
        rest = rest[3:]
    else:
        out_ref = rest[0]
        rest = rest[1:]
    (full32_ref, o_ref, wt_ref, zf_ref, zt_ref, ln_ref, bias_ref, la_ref, ra_ref, lb_ref, rb_ref, zs_ref, zr_ref, nl_ref,
     send_sem, recv_sem) = rest[:16]
    att = rest[16:]
    pt_refs, gt_refs, others = att[0:2], att[2:4], att[4:7]
    me = lax.axis_index('dap')
    mine = pl.ds(pl.multiple_of(HELD * me, HELD), HELD)
    greet(me)
    diagonal = lax.broadcasted_iota(jnp.int32, (RES, RES), 0) == lax.broadcasted_iota(jnp.int32, (RES, RES), 1)
    keys = jnp.sum(jnp.where(diagonal, jnp.broadcast_to(res_ref[...], (RES, RES)), 0).astype(F32), axis=1, keepdims=True)
    keep = jnp.broadcast_to(keys, (RES, LANES)) > 0.5
    mask = mask_ref[...].astype(F32).astype(BF16)
    norm = lax.dot_general(mask, mask_ref[mine, :].astype(F32).astype(BF16), NT, preferred_element_type=F32)

    full32_ref[:CELLS] = wm_ref[...].astype(F32).reshape(CELLS, LANES)
    if has_next:
        for q in range(32):
            wt_ref[pl.ds(32 * q, 32), :] = full32_ref[pl.ds(q, 32, stride=32), :].astype(BF16)
    else:
        wt_ref[...] = wm_ref[...].reshape(CELLS, LANES)
    w_turned = wt_ref[...].T
    full32_ref[...] = full_ref[...].astype(F32).reshape(2048, LANES)
    own = own_ref[...].reshape(BLOCK, BLOCK)
    zeros = jnp.zeros((RES, LANES), BF16)

    def one(q, carry):
        c_q = full32_ref[pl.ds(q, RES, stride=32), :].astype(BF16)
        rhs = jnp.concatenate([jnp.concatenate([c_q, zeros], axis=1), jnp.concatenate([zeros, c_q], axis=1)], axis=0)
        o = lax.dot_general(own, rhs, NT, preferred_element_type=F32).astype(BF16)
        for pair in range(8):
            o_ref[pair, pl.ds(pl.multiple_of(q * 32, 32), 32), :] = o[32 * pair:32 * pair + 32]
        return carry

    lax.fori_loop(0, 32, one, 0, unroll=4)
    for pair in range(8):
        update = jnp.dot(w_turned, o_ref[pair], preferred_element_type=F32).T
        z = z_ref[pl.ds(2 * pair, 2)].astype(F32).reshape(LANES, LANES)
        below = jnp.concatenate([pick_column(norm, 2 * pair), pick_column(norm, 2 * pair + 1)], axis=0)
        z = (z + update / (1e-3 + below)).astype(BF16).astype(F32)
        rows = pl.ds(LANES * pair, LANES)
        zf_ref[rows, :] = z
        ln_ref[rows, :] = layer_norm(z)

    la_ref[...] = local_bias_rows(ln_ref, wba_ref[...]).reshape(4, HELD, LANES)
    copies = push(me, 0, send_sem, recv_sem, lambda peer: la_ref, ra_ref.at[:, mine, :])
    ra_ref[:, mine, :] = la_ref[...]

    def queries_ready():
        finish_all(copies)
        bias_by_query(ra_ref, bias_ref)

    triangle(zf_ref, ln_ref, wa_ref, woa_ref, keep, bias_ref, pt_refs, gt_refs, others, queries_ready)

    zs_ref[...] = zf_ref[...].astype(BF16).reshape(HELD, RES, LANES)
    norm_all(zf_ref, ln_ref)
    moved = push(me, 1, send_sem, recv_sem, lambda peer: zs_ref.at[:, pl.ds(pl.multiple_of(HELD * peer, HELD), HELD), :], zr_ref.at[mine])
    zr_ref[mine] = zs_ref[:, mine, :]
    lb_ref[...] = local_bias_rows(ln_ref, wbb_ref[...]).reshape(4, HELD, LANES)
    copies_b = push(me, 2, send_sem, recv_sem, lambda peer: lb_ref, rb_ref.at[:, mine, :])
    rb_ref[:, mine, :] = lb_ref[...]
    finish_all(moved)
    zt_ref[...] = zr_ref[...].astype(F32).reshape(CELLS, LANES)
    for row in range(HELD):
        value = zt_ref[pl.ds(row, RES, stride=HELD), :]
        zf_ref[pl.ds(RES * row, RES), :] = value
        ln_ref[pl.ds(RES * row, RES), :] = layer_norm(value)

    def keys_ready():
        finish_all(copies_b)
        bias_ref[...] = rb_ref[...].astype(F32) * LOG2E

    triangle(zf_ref, ln_ref, wb_ref, wob_ref, keep, bias_ref, pt_refs, gt_refs, others, keys_ready)
    out_ref[...] = zf_ref[...].astype(BF16).reshape(HELD, RES, LANES)
    if has_next:
        norm_all(zf_ref, ln_ref)
        nl_ref[...] = local_bias_rows(ln_ref, wn_ref[...]).reshape(HELD, HELD, LANES)
        copies = push(me, 3, send_sem, recv_sem, lambda peer: nl_ref, next_ref.at[:, mine, :])
        next_ref[:, mine, :] = nl_ref[...]
        finish_all(copies)


def norm_all(zf_ref, ln_ref):
    for block in range(8):
        rows = pl.ds(LANES * block, LANES)
        ln_ref[rows, :] = layer_norm(zf_ref[rows, :])


def pair_block(ident, layer, own, full, z, mask, res_mask, weights, w_next):
    has_next = w_next is not None
    out_shape = [jax.ShapeDtypeStruct(z.shape, BF16)]
    picks = [of_layer(w, layer) for w in weights]
    if has_next:
        weights = weights + (w_next,)
        picks.append(of_layer(w_next, layer + 1))
        out_shape.append(jax.ShapeDtypeStruct((HELD, RES, LANES), BF16))
    args = (own, full, z, mask, res_mask)
    return pl.pallas_call(
        functools.partial(pair_kernel, has_next),
        grid=(1,),
        out_shape=out_shape,
        in_specs=[whole(a) for a in args] + picks,
        out_specs=[VMEM] * len(out_shape),
        scratch_shapes=[
            pltpu.VMEM((2048, LANES), F32),
            pltpu.VMEM((8, CELLS, LANES), BF16),
            pltpu.VMEM((CELLS, LANES), BF16),
            pltpu.VMEM((CELLS, LANES), F32),
            pltpu.VMEM((CELLS, LANES), F32),
            pltpu.VMEM((CELLS, LANES), BF16),
            pltpu.VMEM((4, RES, LANES), F32),
            pltpu.VMEM((4, HELD, LANES), BF16),
            pltpu.VMEM((4, RES, LANES), BF16),
            pltpu.VMEM((4, HELD, LANES), BF16),
            pltpu.VMEM((4, RES, LANES), BF16),
            pltpu.VMEM((HELD, RES, LANES), BF16),
            pltpu.VMEM((RES, HELD, LANES), BF16),
            pltpu.VMEM((HELD, HELD, LANES), BF16),
            pltpu.SemaphoreType.DMA((12,)),
            pltpu.SemaphoreType.DMA((12,)),
        ] + attend_scratch(4, 32, RES, LANES)[1:],
        compiler_params=pltpu.CompilerParams(collective_id=ident, has_side_effects=True),
        cost_estimate=pl.CostEstimate(flops=10 ** 10, bytes_accessed=2 ** 22, transcendentals=0),
        name="pair_block",
    )(*args, *weights)


def solution(mesh):
    def local_step(m, z, mask, res_mask, w_row_bias, w_row_in, w_row_out, w_col_in, w_col_out, w_opm_in, w_opm_out, w_ts_bias, w_ts_in, w_ts_out, w_te_bias, w_te_in, w_te_out):
        flat_in = lambda w: jnp.transpose(w, (0, 2, 3, 4, 1)).reshape(2, -1, w.shape[1])
        flat_out = lambda w: w.reshape(2, -1, w.shape[-1])
        flat_bias = lambda w: jnp.transpose(w, (0, 2, 1))
        w_row_in, w_col_in, w_ts_in, w_te_in = map(flat_in, (w_row_in, w_col_in, w_ts_in, w_te_in))
        w_row_out, w_col_out, w_ts_out, w_te_out = map(flat_out, (w_row_out, w_col_out, w_ts_out, w_te_out))
        w_row_bias, w_ts_bias, w_te_bias = map(flat_bias, (w_row_bias, w_ts_bias, w_te_bias))
        w_opm_in = jnp.transpose(w_opm_in, (0, 2, 3, 1)).reshape(2, RES, WIDE)
        w_opm_out = w_opm_out.reshape(2, CELLS, LANES)
        mask = mask.T
        res_mask = res_mask.reshape(1, RES)

        m = row_first(m, z, mask, w_row_bias, w_row_in, w_row_out)
        m, own1, own2, full1, full2 = column_pair(m, mask, w_col_in, w_col_out, w_opm_in)
        z, row_bias = pair_block(
            2, 0, own1, full1, z, mask, res_mask,
            (w_opm_out, w_ts_bias, w_ts_in, w_ts_out, w_te_bias, w_te_in, w_te_out), w_row_bias)
        z, = pair_block(
            3, 1, own2, full2, z, mask, res_mask,
            (w_opm_out, w_te_bias, w_te_in, w_te_out, w_ts_bias, w_ts_in, w_ts_out), None)
        m = row_last(m, row_bias, mask, w_row_in, w_row_out)
        return m, z

    in_specs = (P(('data', 'dap')), P(('data', 'dap')), P('data'), P('data')) + (P(),) * 13
    out_specs = (P(('data', 'dap')), P(('data', 'dap')))
    return jax.shard_map(local_step, mesh=mesh, in_specs=in_specs, out_specs=out_specs, check_vma=False)
```

```python
import functools

import jax
import jax.numpy as jnp
from jax import lax
from jax.experimental import pallas as pl
from jax.experimental.pallas import tpu as pltpu
from jax.sharding import PartitionSpec as P

LOG2E = 1.4426950408889634
NEG = -1e9 * LOG2E
F32 = jnp.float32
BF16 = jnp.bfloat16
LAG = 2
SLOTS = 4
NT = (((1,), (1,)), ((), ()))
LANES = 128
RES = 64
BLOCK = 256
HELD = 16
WIDE = 384
CELLS = 1024


def layer_norm(values):
    flat = values.astype(F32)
    row_mean = jnp.mean(flat, axis=-1, keepdims=True)
    centered = flat - row_mean
    row_var = jnp.mean(centered * centered, axis=-1, keepdims=True)
    return (centered * lax.rsqrt(row_var + 1e-5)).astype(BF16)


def half_masks(rows, split):
    index = lax.broadcasted_iota(jnp.int32, (rows, LANES), 0)
    upper = (index < split).astype(F32).astype(BF16)
    lower = (index >= split).astype(F32).astype(BF16)
    return upper, lower


def attend_units(pt_ref, gt_ref, kt_ref, lg_ref, pr_ref, heads, dim, keep, bias_ref, work):
    width = heads * dim
    rows = 2 * dim
    pairs = heads // 2
    units = 2 * pairs
    up, low = half_masks(rows, dim)
    scale = dim ** -0.5 * LOG2E
    if bias_ref is not None:
        left = lax.broadcasted_iota(jnp.int32, (RES, LANES), 1) < RES
        left_b = left.astype(F32).astype(BF16)
        right_b = (1.0 - left.astype(F32)).astype(BF16)

    def place(unit):
        return pl.ds(unit // pairs * LANES, LANES), rows * (unit % pairs)

    def turn_keys(unit):
        ln, r = place(unit)
        kt_ref[unit % SLOTS] = pt_ref[pl.ds(width + r, rows), ln].T

    def make_logits(unit):
        ln, r = place(unit)
        q = pt_ref[pl.ds(r, rows), ln]
        rhs = jnp.concatenate([q * up, q * low], axis=1)
        logits2 = jnp.dot(kt_ref[unit % SLOTS], rhs, preferred_element_type=F32)
        for half in range(2):
            lg = logits2[:, LANES * half:LANES * half + LANES]
            if bias_ref is not None:
                lg = jnp.where(left, lg[0:RES], lg[RES:LANES])
            lg_ref[unit % SLOTS, half] = lg

    def soften(unit):
        blk, hp = unit // pairs, unit % pairs
        for half in range(2):
            lg = lg_ref[unit % SLOTS, half] * scale
            if bias_ref is not None:
                lg = lg + bias_ref[2 * hp + half]
            lg = jnp.where(keep[blk], lg, NEG)
            e = jnp.exp2(lg - jnp.max(lg, axis=0, keepdims=True))
            p = (e * (1.0 / jnp.sum(e, axis=0, keepdims=True))).astype(BF16)
            pr_ref[unit % SLOTS, half] = p

    def mix(unit):
        ln, r = place(unit)
        v = pt_ref[pl.ds(2 * width + r, rows), ln]
        g = pt_ref[pl.ds(3 * width + r, rows), ln]
        probs = []
        for half in range(2):
            p = pr_ref[unit % SLOTS, half]
            probs += [p] if bias_ref is None else [p * left_b, p * right_b]
        att = jnp.dot(jnp.concatenate([v * up, v * low], axis=1), jnp.concatenate(probs, axis=0), preferred_element_type=F32)
        gt_ref[pl.ds(r, rows), ln] = (att * jax.nn.sigmoid(g.astype(F32))).astype(BF16)

    stages = ((turn_keys, 0), (make_logits, LAG), (soften, 2 * LAG), (mix, 3 * LAG))
    ticks = units + 3 * LAG
    for tick in range(ticks):
        for stage, lag in stages:
            if 0 <= tick - lag < units:
                stage(tick - lag)
        for job in work[len(work) * tick // ticks:len(work) * (tick + 1) // ticks]:
            job()


def project(ln_ref, pt_ref, w):
    rows = pt_ref.shape[0]
    chunk = BLOCK if rows > CELLS else LANES

    def job(part):
        sl = pl.ds(part * chunk, chunk)
        pt_ref[sl, :] = lax.dot_general(w(sl), ln_ref[...], NT, preferred_element_type=F32).astype(BF16)
    return [functools.partial(job, part) for part in range(rows // chunk)]


def leave(gt_ref, x_old, wo):
    return (x_old + jnp.dot(gt_ref[...].T, wo, preferred_element_type=F32)).astype(BF16)


def attend_blocks(blocks, scratch, read, w_in, w_out, keep, bias_ref, finish, ready, aside):
    ln_ref, pt_refs, gt_refs, others = scratch[0], scratch[1:3], scratch[3:5], scratch[5:8]
    ln_ref[...] = layer_norm(read(0))
    for job in project(ln_ref, pt_refs[0], w_in(0)):
        job()
    ready()

    def body(turn, carry):
        for half in (1, 0):
            i = 2 * turn + 2 - half
            new = jnp.minimum(i, blocks - 1)
            old = jnp.maximum(i - 2, 0)
            aside(i, half)

            def norm():
                ln_ref[...] = layer_norm(read(new))

            def done():
                finish(old, leave(gt_refs[half], read(old), w_out(old)))

            work = [norm, done] + project(ln_ref, pt_refs[half], w_in(new))
            attend_units(pt_refs[1 - half], gt_refs[1 - half], *others, 16, 24, keep(i - 1), bias_ref, work)
        return carry

    lax.fori_loop(0, blocks // 2, body, 0)
    finish(blocks - 1, leave(gt_refs[1], read(blocks - 1), w_out(blocks - 1)))


def attend_scratch(heads, dim, keys, channels):
    inner = heads * dim
    return [
        pltpu.VMEM((BLOCK, channels), BF16),
        pltpu.VMEM((4 * inner, BLOCK), BF16),
        pltpu.VMEM((4 * inner, BLOCK), BF16),
        pltpu.VMEM((inner, BLOCK), BF16),
        pltpu.VMEM((inner, BLOCK), BF16),
        pltpu.VMEM((SLOTS, LANES, 2 * dim), BF16),
        pltpu.VMEM((SLOTS, 2, keys, LANES), F32),
        pltpu.VMEM((SLOTS, 2, keys, LANES), BF16),
    ]


def pick_column(table, col):
    lane = lax.broadcasted_iota(jnp.int32, table.shape, 1)
    return jnp.sum(jnp.where(lane == col, table, 0.0), axis=1, keepdims=True)


def row_keep(mask_ref, seq):
    left = lax.broadcasted_iota(jnp.int32, (RES, LANES), 1) < RES
    table = mask_ref[...].astype(F32)
    column = [pick_column(table, seq + n) for n in range(4)]
    return [jnp.where(left, column[2 * blk], column[2 * blk + 1]) > 0.5 for blk in range(2)]


def row_first_kernel(x_ref, z_ref, mask_ref, wb_ref, w_ref, wo_ref, out_ref, mo_ref, lnz_ref, nl_ref, rows_ref, bias_ref,
                     send_sem, recv_sem, *scratch):
    me = lax.axis_index('dap')
    mine = pl.ds(pl.multiple_of(HELD * me, HELD), HELD)
    for part in range(4):
        lnz_ref[pl.ds(BLOCK * part, BLOCK), :] = layer_norm(z_ref[pl.ds(4 * part, 4)].reshape(BLOCK, LANES))
    nl_ref[...] = local_bias_rows(lnz_ref, wb_ref[...]).reshape(HELD, HELD, LANES)
    greet(me)
    copies = group_copies(me, 8, send_sem, recv_sem, lambda peer: nl_ref, rows_ref.at[:, mine, :])
    start_all(copies)
    rows_ref[:, mine, :] = nl_ref[...]

    def ready():
        finish_all(copies)
        bias_by_query(rows_ref, bias_ref)

    def moves(block):
        return group_copies(
            me, block, send_sem, recv_sem,
            lambda peer: mo_ref.at[pl.ds(4 * block, 4), pl.ds(pl.multiple_of(HELD * peer, HELD), HELD), :],
            out_ref.at[pl.ds(32 * me + 4 * block, 4)])

    def emit(block):
        start_all(moves(block))
        out_ref[pl.ds(32 * me + 4 * block, 4)] = mo_ref[pl.ds(4 * block, 4), mine, :]

    def aside(i, half):
        @pl.when(i >= 3)
        def _():
            emit(i - 3)

    def finish(block, out):
        mo_ref[pl.ds(4 * block, 4)] = out.reshape(4, RES, WIDE)

    attend_blocks(8, scratch, lambda at: x_ref[pl.ds(at * 4, 4)].astype(F32).reshape(BLOCK, WIDE),
                  lambda at: lambda sl: w_ref[sl, :], lambda at: wo_ref[...],
                  lambda at: row_keep(mask_ref, 32 * me + 4 * at), bias_ref, finish, ready, aside)
    emit(6)
    emit(7)

    def drain(block, carry):
        finish_all(moves(block))
        return carry

    lax.fori_loop(0, 8, drain, 0)


def bias_by_query(rows_ref, bias_ref):
    for head in range(rows_ref.shape[0]):
        turned = (rows_ref[head].astype(F32) * LOG2E).T[:RES]
        bias_ref[head] = jnp.concatenate([turned, turned], axis=1)


VMEM = pl.BlockSpec(memory_space=pltpu.VMEM)


def of_layer(array, layer):
    rank = array.ndim - 1
    return pl.BlockSpec((None,) + array.shape[1:], lambda i: (layer,) + (0,) * rank)


def whole(array):
    return pl.BlockSpec(array.shape, lambda i: (0,) * array.ndim)


def row_first(x, z, mask, wb, w, wo):
    return pl.pallas_call(
        row_first_kernel,
        grid=(1,),
        in_specs=[whole(x), whole(z), whole(mask)] + [of_layer(a, 0) for a in (wb, w, wo)],
        out_specs=VMEM,
        out_shape=jax.ShapeDtypeStruct((LANES, HELD, WIDE), BF16),
        scratch_shapes=[
            pltpu.VMEM((32, RES, WIDE), BF16),
            pltpu.VMEM((CELLS, LANES), BF16),
            pltpu.VMEM((HELD, HELD, LANES), BF16),
            pltpu.VMEM((HELD, RES, LANES), BF16),
            pltpu.VMEM((HELD, RES, LANES), F32),
            pltpu.SemaphoreType.DMA((27,)),
            pltpu.SemaphoreType.DMA((27,)),
        ] + attend_scratch(HELD, 24, RES, WIDE),
        compiler_params=pltpu.CompilerParams(collective_id=0, has_side_effects=True),
        cost_estimate=pl.CostEstimate(flops=10 ** 10, bytes_accessed=2 ** 22, transcendentals=0),
        name="row_first",
    )(x, z, mask, wb, w, wo)


def row_last_kernel(x_ref, rows_ref, own_ref, full_ref, z_ref, mask_ref, res_ref, w_ref, wo_ref, wm_ref, wba_ref, wa_ref, woa_ref,
                    wbb_ref, wb_ref, wob_ref, out_ref, z_out_ref, wide_ref, m_ref, bias_ref, send_sem, recv_sem, *scratch):
    me = lax.axis_index('dap')
    greet(me)
    outer, along, across, _ = pair_stages(
        me, 0, False, own_ref, full_ref, z_ref, mask_ref, res_ref, (wm_ref, wba_ref, wa_ref, woa_ref, wbb_ref, wb_ref, wob_ref),
        z_out_ref, None, send_sem, recv_sem, scratch[8:])
    outer()
    turn_tokens(x_ref, wide_ref, m_ref)
    bias_ref[...] = rows_ref[...].astype(F32) * LOG2E

    def finish(block, out):
        out_ref[pl.ds(4 * block, 4)] = out.reshape(4, RES, WIDE)

    def aside(i, half):
        if half:
            pl.when(i == 3)(along)
            pl.when(i == 5)(across)

    attend_blocks(8, scratch[:8], lambda at: m_ref[pl.ds(at * 4, 4)].astype(F32).reshape(BLOCK, WIDE),
                  lambda at: lambda sl: w_ref[sl, :], lambda at: wo_ref[...],
                  lambda at: row_keep(mask_ref, 32 * me + 4 * at), bias_ref, finish, lambda: None, aside)


def turn_tokens(x_ref, wide_ref, m_ref):
    outer, inner = x_ref.shape[:2]
    for part in range(3):
        lanes = pl.ds(LANES * part, LANES)
        wide_ref[part] = x_ref[:, :, lanes].astype(F32).reshape(outer * inner, LANES)

    def one(row, carry):
        for part in range(3):
            m_ref[row, :, pl.ds(LANES * part, LANES)] = wide_ref[part, pl.ds(row, outer, stride=inner), :].astype(BF16)
        return carry

    lax.fori_loop(0, inner, one, 0, unroll=2)


def row_last(args, weights):
    return pl.pallas_call(
        row_last_kernel,
        grid=(1,),
        in_specs=[whole(a) for a in args] + [of_layer(a, 1) for a in weights],
        out_specs=[VMEM] * 2,
        out_shape=[jax.ShapeDtypeStruct((32, RES, WIDE), BF16), jax.ShapeDtypeStruct((HELD, RES, LANES), BF16)],
        scratch_shapes=[
            pltpu.VMEM((3, 2048, LANES), F32),
            pltpu.VMEM((32, RES, WIDE), BF16),
            pltpu.VMEM((HELD, RES, LANES), F32),
            pltpu.SemaphoreType.DMA((12,)),
            pltpu.SemaphoreType.DMA((12,)),
        ] + attend_scratch(HELD, 24, RES, WIDE) + pair_scratch(),
        compiler_params=pltpu.CompilerParams(collective_id=2, has_side_effects=True),
        cost_estimate=pl.CostEstimate(flops=10 ** 10, bytes_accessed=2 ** 22, transcendentals=0),
        name="row_last",
    )(*args, *weights)


def col_kernel(x_ref, mask_ref, w_ref, wo_ref, wp_ref, z_ref, res_ref, wm_ref, wba_ref, wa_ref, woa_ref, wbb_ref, wb_ref, wob_ref, wn_ref,
               out_ref, own2_ref, full2_ref, z_out_ref, next_ref, own1_ref, full1_ref,
               wide_ref, m_ref, part_ref, keys_ref, send_sem, recv_sem, *scratch):
    me = lax.axis_index('dap')
    greet(me)
    turn_tokens(x_ref, wide_ref, m_ref.at[0])
    mine = pl.ds(pl.multiple_of(HELD * me, HELD), HELD)
    keys_ref[...] = mask_ref[mine, :].astype(F32).T

    def keep(at):
        return [jnp.broadcast_to(pick_column(keys_ref[...], at % 8 * 2 + blk), (LANES, LANES)) > 0.5 for blk in range(2)]

    def finish(block, out):
        layer, pair = block // 8, block % 8
        m_ref[layer + 1, pl.ds(pair * 2, 2)] = out.reshape(2, LANES, WIDE)
        ac = lax.dot_general(wp_ref[layer], layer_norm(out), NT, preferred_element_type=F32)
        ac = (ac * jnp.concatenate([mask_ref[pl.ds(HELD * me + 2 * pair + blk, 1), :] for blk in range(2)], axis=1).astype(F32)).astype(BF16)
        parts = (ac[:32], ac[32:])
        own1_ref[pair] = jnp.where(layer == 0, parts[0].astype(F32), own1_ref[pair].astype(F32)).astype(BF16)
        own2_ref[pair] = parts[1]
        for blk in range(2):
            lanes = slice(LANES * blk, LANES * blk + LANES)
            part_ref[block, blk] = jnp.where(layer == 0, parts[1][:, lanes].astype(F32), parts[0][:, lanes].astype(F32)).astype(BF16)

    def part_copies(block, full_ref):
        return group_copies(me, block, send_sem, recv_sem, lambda peer: part_ref.at[block],
                            full_ref.at[pl.ds(HELD * me + block % 8 * 2, 2)])

    def seq_copies(pair):
        return group_copies(
            me, HELD + pair, send_sem, recv_sem,
            lambda peer: m_ref.at[2, pl.ds(2 * pair, 2), pl.ds(pl.multiple_of(32 * peer, 32), 32), :],
            out_ref.at[pl.ds(HELD * me + 2 * pair, 2)])

    outer, along, across, close = pair_stages(
        me, 24, True, own1_ref, full1_ref, z_ref, mask_ref, res_ref, (wm_ref, wba_ref, wa_ref, woa_ref, wbb_ref, wb_ref, wob_ref, wn_ref),
        z_out_ref, next_ref, send_sem, recv_sem, scratch[8:])

    def open_pairs():
        drain_parts(0, full1_ref)
        outer()

    def drain_parts(start, full_ref):
        def one(pair, carry):
            finish_all(part_copies(start + pair, full_ref))
            return carry
        lax.fori_loop(0, 8, one, 0)

    def emit_first(block):
        start_all(part_copies(block, full1_ref))
        full1_ref[pl.ds(HELD * me + 2 * block, 2)] = part_ref[block]

    def emit_second(block):
        pair = block - 8
        start_all(part_copies(block, full2_ref) + seq_copies(pair))
        full2_ref[pl.ds(HELD * me + 2 * pair, 2)] = part_ref[block]
        out_ref[pl.ds(HELD * me + 2 * pair, 2)] = m_ref[2, pl.ds(2 * pair, 2), pl.ds(pl.multiple_of(32 * me, 32), 32), :]

    def aside(i, half):
        @pl.when(jnp.logical_and(i >= 3, i < 11))
        def _():
            emit_first(i - 3)

        @pl.when(i >= 11)
        def _():
            emit_second(i - 3)

        if half:
            pl.when(i == 11)(open_pairs)
            pl.when(i == 13)(along)
            pl.when(i == 15)(across)

    attend_blocks(16, scratch[:8], lambda at: m_ref[at // 8, pl.ds(at % 8 * 2, 2)].astype(F32).reshape(BLOCK, WIDE),
                  lambda at: lambda sl: w_ref[at // 8, sl, :], lambda at: wo_ref[at // 8],
                  keep, None, finish, lambda: None, aside)
    emit_second(14)
    emit_second(15)

    close()
    drain_parts(8, full2_ref)

    def drain(pair, carry):
        finish_all(seq_copies(pair))
        return carry

    lax.fori_loop(0, 8, drain, 0)


def column_pair(args, weights, w_next):
    return pl.pallas_call(
        col_kernel,
        grid=(1,),
        in_specs=[whole(a) for a in args] + [of_layer(a, 0) for a in weights] + [of_layer(w_next, 1)],
        out_specs=[VMEM] * 5,
        out_shape=[
            jax.ShapeDtypeStruct((RES, 32, WIDE), BF16),
            jax.ShapeDtypeStruct((8, 32, BLOCK), BF16),
            jax.ShapeDtypeStruct((RES, 32, LANES), BF16),
            jax.ShapeDtypeStruct((HELD, RES, LANES), BF16),
            jax.ShapeDtypeStruct((HELD, RES, LANES), BF16),
        ],
        scratch_shapes=[
            pltpu.VMEM((8, 32, BLOCK), BF16),
            pltpu.VMEM((RES, 32, LANES), BF16),
            pltpu.VMEM((3, 2048, LANES), F32),
            pltpu.VMEM((3, HELD, LANES, WIDE), BF16),
            pltpu.VMEM((HELD, 2, 32, LANES), BF16),
            pltpu.VMEM((LANES, HELD), F32),
            pltpu.SemaphoreType.DMA((84,)),
            pltpu.SemaphoreType.DMA((84,)),
        ] + attend_scratch(HELD, 24, LANES, WIDE) + pair_scratch(),
        compiler_params=pltpu.CompilerParams(collective_id=1, has_side_effects=True),
        cost_estimate=pl.CostEstimate(flops=10 ** 10, bytes_accessed=2 ** 22, transcendentals=0),
        name="col_pair",
    )(*args, *weights, w_next)


def greet(me):
    barrier = pltpu.get_barrier_semaphore()
    for o in range(1, 4):
        pl.semaphore_signal(barrier, inc=1, device_id={'dap': lax.rem(me + o, 4)}, device_id_type=pl.DeviceIdType.MESH)
    pl.semaphore_wait(barrier, 3)


def group_copies(me, kind, send_sem, recv_sem, source, target):
    copies = []
    for o in range(1, 4):
        peer = lax.rem(me + o, 4)
        copies.append(pltpu.make_async_remote_copy(
            src_ref=source(peer), dst_ref=target, send_sem=send_sem.at[3 * kind + o - 1],
            recv_sem=recv_sem.at[3 * kind + o - 1], device_id={'dap': peer}, device_id_type=pl.DeviceIdType.MESH))
    return copies


def start_all(copies):
    for copy in copies:
        copy.start()


def finish_all(copies):
    for copy in copies:
        copy.wait()


def local_bias_rows(ln_ref, w):
    heads = w.shape[0]
    spread = jnp.concatenate([jnp.broadcast_to(w[head:head + 1], (HELD, LANES)) for head in range(heads)], axis=0)
    index = lax.broadcasted_iota(jnp.int32, spread.shape, 0) % HELD
    total = jnp.zeros(spread.shape, F32)
    for held in range(HELD):
        chosen = spread * (index == held).astype(F32).astype(BF16)
        part = ln_ref[pl.ds(RES * held, RES), :]
        total += lax.dot_general(chosen, jnp.concatenate([part, part], axis=0), NT, preferred_element_type=F32)
    return total.astype(BF16)


def triangle(zf_ref, ln_ref, w_ref, wo_ref, keep, bias_ref, pt_refs, gt_refs, others, ready):
    def project(block, part):
        def job():
            pt_refs[block % 2][pl.ds(LANES * part, LANES), :] = lax.dot_general(
                w_ref[pl.ds(LANES * part, LANES), :], ln_ref[pl.ds(BLOCK * block, BLOCK), :], NT,
                preferred_element_type=F32).astype(BF16)
        return job

    def leave(block):
        def job():
            update = jnp.dot(gt_refs[block % 2][...].T, wo_ref[...], preferred_element_type=F32)
            rows = pl.ds(BLOCK * block, BLOCK)
            zf_ref[rows, :] = (zf_ref[rows, :] + update).astype(BF16).astype(F32)
        return job

    for part in range(4):
        project(0, part)()
    ready()
    for block in range(4):
        work = [leave(block - 1)] if block else []
        if block < 3:
            work += [project(block + 1, part) for part in range(4)]
        attend_units(pt_refs[block % 2], gt_refs[block % 2], *others, 4, 32, [keep, keep], bias_ref, work)
    leave(3)()


def pair_stages(me, first, swap, own_ref, full_ref, z_ref, mask_ref, res_ref, weights, out_ref, next_ref, send_sem, recv_sem, scratch):
    wm_ref, wba_ref, wa_ref, woa_ref, wbb_ref, wb_ref, wob_ref = weights[:7]
    (full32_ref, o_ref, wt_ref, zf_ref, zt_ref, ln_ref, bias_ref, la_ref, ra_ref, lb_ref, rb_ref, zs_ref, zr_ref, nl_ref) = scratch[:14]
    att = scratch[14:]
    pt_refs, gt_refs, others = att[0:2], att[2:4], att[4:7]
    mine = pl.ds(pl.multiple_of(HELD * me, HELD), HELD)

    def keep():
        diagonal = lax.broadcasted_iota(jnp.int32, (RES, RES), 0) == lax.broadcasted_iota(jnp.int32, (RES, RES), 1)
        keys = jnp.sum(jnp.where(diagonal, jnp.broadcast_to(res_ref[...], (RES, RES)), 0).astype(F32), axis=1, keepdims=True)
        return jnp.broadcast_to(keys, (RES, LANES)) > 0.5

    def exchange(kind):
        source, target = (
            (lambda peer: la_ref, ra_ref.at[:, mine, :]),
            (lambda peer: zs_ref.at[:, pl.ds(pl.multiple_of(HELD * peer, HELD), HELD), :], zr_ref.at[mine]),
            (lambda peer: lb_ref, rb_ref.at[:, mine, :]),
            (lambda peer: nl_ref, None if next_ref is None else next_ref.at[:, mine, :]),
        )[kind]
        return group_copies(me, first + kind, send_sem, recv_sem, source, target)

    def outer():
        mask = mask_ref[...].astype(F32).astype(BF16)
        norm = lax.dot_general(mask, mask_ref[mine, :].astype(F32).astype(BF16), NT, preferred_element_type=F32)
        full32_ref[:CELLS] = wm_ref[...].astype(F32).reshape(CELLS, LANES)
        if swap:
            for q in range(32):
                wt_ref[pl.ds(32 * q, 32), :] = full32_ref[pl.ds(q, 32, stride=32), :].astype(BF16)
        else:
            wt_ref[...] = wm_ref[...].reshape(CELLS, LANES)
        w_turned = wt_ref[...].T
        full32_ref[...] = full_ref[...].astype(F32).reshape(2048, LANES)
        own = own_ref[...].reshape(BLOCK, BLOCK)
        zeros = jnp.zeros((RES, LANES), BF16)

        def one(q, carry):
            c_q = full32_ref[pl.ds(q, RES, stride=32), :].astype(BF16)
            rhs = jnp.concatenate([jnp.concatenate([c_q, zeros], axis=1), jnp.concatenate([zeros, c_q], axis=1)], axis=0)
            o = lax.dot_general(own, rhs, NT, preferred_element_type=F32).astype(BF16)
            for pair in range(8):
                o_ref[pair, pl.ds(pl.multiple_of(q * 32, 32), 32), :] = o[32 * pair:32 * pair + 32]
            return carry

        lax.fori_loop(0, 32, one, 0, unroll=4)
        for pair in range(8):
            update = jnp.dot(w_turned, o_ref[pair], preferred_element_type=F32).T
            z = z_ref[pl.ds(2 * pair, 2)].astype(F32).reshape(LANES, LANES)
            below = jnp.concatenate([pick_column(norm, 2 * pair), pick_column(norm, 2 * pair + 1)], axis=0)
            z = (z + update / (1e-3 + below)).astype(BF16).astype(F32)
            rows = pl.ds(LANES * pair, LANES)
            zf_ref[rows, :] = z
            ln_ref[rows, :] = layer_norm(z)
        la_ref[...] = local_bias_rows(ln_ref, wba_ref[...]).reshape(4, HELD, LANES)
        start_all(exchange(0))
        ra_ref[:, mine, :] = la_ref[...]

    def along():
        def ready():
            finish_all(exchange(0))
            bias_by_query(ra_ref, bias_ref)

        triangle(zf_ref, ln_ref, wa_ref, woa_ref, keep(), bias_ref, pt_refs, gt_refs, others, ready)
        zs_ref[...] = zf_ref[...].astype(BF16).reshape(HELD, RES, LANES)
        norm_all(zf_ref, ln_ref)
        start_all(exchange(1))
        zr_ref[mine] = zs_ref[:, mine, :]
        lb_ref[...] = local_bias_rows(ln_ref, wbb_ref[...]).reshape(4, HELD, LANES)
        start_all(exchange(2))
        rb_ref[:, mine, :] = lb_ref[...]

    def across():
        finish_all(exchange(1))
        zt_ref[...] = zr_ref[...].astype(F32).reshape(CELLS, LANES)
        for row in range(HELD):
            value = zt_ref[pl.ds(row, RES, stride=HELD), :]
            zf_ref[pl.ds(RES * row, RES), :] = value
            ln_ref[pl.ds(RES * row, RES), :] = layer_norm(value)

        def ready():
            finish_all(exchange(2))
            bias_ref[...] = rb_ref[...].astype(F32) * LOG2E

        triangle(zf_ref, ln_ref, wb_ref, wob_ref, keep(), bias_ref, pt_refs, gt_refs, others, ready)
        out_ref[...] = zf_ref[...].astype(BF16).reshape(HELD, RES, LANES)
        if next_ref is not None:
            norm_all(zf_ref, ln_ref)
            nl_ref[...] = local_bias_rows(ln_ref, weights[7][...]).reshape(HELD, HELD, LANES)
            start_all(exchange(3))
            next_ref[:, mine, :] = nl_ref[...]

    def close():
        if next_ref is not None:
            finish_all(exchange(3))

    return outer, along, across, close


def pair_scratch():
    return [
        pltpu.VMEM((2048, LANES), F32),
        pltpu.VMEM((8, CELLS, LANES), BF16),
        pltpu.VMEM((CELLS, LANES), BF16),
        pltpu.VMEM((CELLS, LANES), F32),
        pltpu.VMEM((CELLS, LANES), F32),
        pltpu.VMEM((CELLS, LANES), BF16),
        pltpu.VMEM((4, RES, LANES), F32),
        pltpu.VMEM((4, HELD, LANES), BF16),
        pltpu.VMEM((4, RES, LANES), BF16),
        pltpu.VMEM((4, HELD, LANES), BF16),
        pltpu.VMEM((4, RES, LANES), BF16),
        pltpu.VMEM((HELD, RES, LANES), BF16),
        pltpu.VMEM((RES, HELD, LANES), BF16),
        pltpu.VMEM((HELD, HELD, LANES), BF16),
    ] + attend_scratch(4, 32, RES, LANES)[1:]


def norm_all(zf_ref, ln_ref):
    for block in range(8):
        rows = pl.ds(LANES * block, LANES)
        ln_ref[rows, :] = layer_norm(zf_ref[rows, :])


def solution(mesh):
    def local_step(m, z, mask, res_mask, w_row_bias, w_row_in, w_row_out, w_col_in, w_col_out, w_opm_in, w_opm_out, w_ts_bias, w_ts_in, w_ts_out, w_te_bias, w_te_in, w_te_out):
        flat_in = lambda w: jnp.transpose(w, (0, 2, 3, 4, 1)).reshape(2, -1, w.shape[1])
        flat_out = lambda w: w.reshape(2, -1, w.shape[-1])
        flat_bias = lambda w: jnp.transpose(w, (0, 2, 1))
        w_row_in, w_col_in, w_ts_in, w_te_in = map(flat_in, (w_row_in, w_col_in, w_ts_in, w_te_in))
        w_row_out, w_col_out, w_ts_out, w_te_out = map(flat_out, (w_row_out, w_col_out, w_ts_out, w_te_out))
        w_row_bias, w_ts_bias, w_te_bias = map(flat_bias, (w_row_bias, w_ts_bias, w_te_bias))
        w_opm_in = jnp.transpose(w_opm_in, (0, 2, 3, 1)).reshape(2, RES, WIDE)
        w_opm_out = w_opm_out.reshape(2, CELLS, LANES)
        mask = mask.T
        res_mask = res_mask.reshape(1, RES)

        m = row_first(m, z, mask, w_row_bias, w_row_in, w_row_out)
        m, own, full, z, row_bias = column_pair(
            (m, mask, w_col_in, w_col_out, w_opm_in, z, res_mask),
            (w_opm_out, w_ts_bias, w_ts_in, w_ts_out, w_te_bias, w_te_in, w_te_out), w_row_bias)
        m, z = row_last(
            (m, row_bias, own, full, z, mask, res_mask),
            (w_row_in, w_row_out, w_opm_out, w_te_bias, w_te_in, w_te_out, w_ts_bias, w_ts_in, w_ts_out))
        return m, z

    in_specs = (P(('data', 'dap')), P(('data', 'dap')), P('data'), P('data')) + (P(),) * 13
    out_specs = (P(('data', 'dap')), P(('data', 'dap')))
    return jax.shard_map(local_step, mesh=mesh, in_specs=in_specs, out_specs=out_specs, check_vma=False)
```

```python
import functools

import jax
import jax.numpy as jnp
from jax import lax
from jax.experimental import pallas as pl
from jax.experimental.pallas import tpu as pltpu
from jax.sharding import PartitionSpec as P

LOG2E = 1.4426950408889634
NEG = -1e9 * LOG2E
F32 = jnp.float32
BF16 = jnp.bfloat16
LAG = 2
SLOTS = 4
NT = (((1,), (1,)), ((), ()))
LANES = 128
RES = 64
BLOCK = 256
HELD = 16
WIDE = 384
CELLS = 1024


def layer_norm(values):
    flat = values.astype(F32)
    row_mean = jnp.mean(flat, axis=-1, keepdims=True)
    centered = flat - row_mean
    row_var = jnp.mean(centered * centered, axis=-1, keepdims=True)
    return (centered * lax.rsqrt(row_var + 1e-5)).astype(BF16)


def half_masks(rows, split):
    index = lax.broadcasted_iota(jnp.int32, (rows, LANES), 0)
    upper = (index < split).astype(F32).astype(BF16)
    lower = (index >= split).astype(F32).astype(BF16)
    return upper, lower


def attend_stream(blocks, others, heads, dim, bias_ref, jobs):
    kt_ref, lg_ref, pr_ref = others
    width = heads * dim
    rows = 2 * dim
    pairs = heads // 2
    each = 2 * pairs
    units = each * len(blocks)
    up, low = half_masks(rows, dim)
    scale = dim ** -0.5 * LOG2E
    if bias_ref is not None:
        left = lax.broadcasted_iota(jnp.int32, (RES, LANES), 1) < RES
        left_b = left.astype(F32).astype(BF16)
        right_b = (1.0 - left.astype(F32)).astype(BF16)

    def place(unit):
        return blocks[unit // each], pl.ds(unit % each // pairs * LANES, LANES), rows * (unit % pairs)

    def turn_keys(unit):
        (pt_ref, _, _), ln, r = place(unit)
        kt_ref[unit % SLOTS] = pt_ref[pl.ds(width + r, rows), ln].T

    def make_logits(unit):
        (pt_ref, _, _), ln, r = place(unit)
        q = pt_ref[pl.ds(r, rows), ln]
        rhs = jnp.concatenate([q * up, q * low], axis=1)
        logits2 = jnp.dot(kt_ref[unit % SLOTS], rhs, preferred_element_type=F32)
        for half in range(2):
            lg = logits2[:, LANES * half:LANES * half + LANES]
            if bias_ref is not None:
                lg = jnp.where(left, lg[:RES], lg[RES:])
            lg_ref[unit % SLOTS, half] = lg

    def soften(unit):
        (_, _, keep), _, _ = place(unit)
        for half in range(2):
            lg = lg_ref[unit % SLOTS, half] * scale
            if bias_ref is not None:
                lg = lg + bias_ref[2 * (unit % pairs) + half]
            lg = jnp.where(keep[unit % each // pairs], lg, NEG)
            e = jnp.exp2(lg - jnp.max(lg, axis=0, keepdims=True))
            pr_ref[unit % SLOTS, half] = (e * (1.0 / jnp.sum(e, axis=0, keepdims=True))).astype(BF16)

    def mix(unit):
        (pt_ref, gt_ref, _), ln, r = place(unit)
        v = pt_ref[pl.ds(2 * width + r, rows), ln]
        g = pt_ref[pl.ds(3 * width + r, rows), ln]
        probs = []
        for half in range(2):
            p = pr_ref[unit % SLOTS, half]
            probs += [p] if bias_ref is None else [p * left_b, p * right_b]
        att = jnp.dot(jnp.concatenate([v * up, v * low], axis=1), jnp.concatenate(probs, axis=0), preferred_element_type=F32)
        gt_ref[pl.ds(r, rows), ln] = (att * jax.nn.sigmoid(g.astype(F32))).astype(BF16)

    stages = ((turn_keys, 0), (make_logits, LAG), (soften, 2 * LAG), (mix, 3 * LAG))
    for tick in range(units + 3 * LAG):
        for stage, lag in stages:
            if 0 <= tick - lag < units:
                stage(tick - lag)
        for start, end, work in jobs:
            if start <= tick < end:
                for job in work[len(work) * (tick - start) // (end - start):len(work) * (tick - start + 1) // (end - start)]:
                    job()


def project(ln_ref, pt_ref, w, rows=slice(None)):
    size = pt_ref.shape[0]
    chunk = BLOCK if size > CELLS else LANES

    def job(part):
        sl = pl.ds(part * chunk, chunk)
        pt_ref[sl, :] = lax.dot_general(w(sl), ln_ref[rows, :], NT, preferred_element_type=F32).astype(BF16)
    return [functools.partial(job, part) for part in range(size // chunk)]


def leave(gt_ref, x_old, wo):
    return (x_old + jnp.dot(gt_ref[...].T, wo, preferred_element_type=F32)).astype(BF16)


def attend_blocks(blocks, scratch, read, w_in, w_out, keep, bias_ref, finish, ready, aside):
    ln_ref, pt_refs, gt_refs, others = scratch[0], scratch[1:3], scratch[3:5], scratch[5:8]
    ln_ref[...] = layer_norm(read(0))
    for job in project(ln_ref, pt_refs[0], w_in(0)):
        job()
    ready()

    def body(turn, carry):
        aside(turn)

        def jobs(half):
            new = jnp.minimum(2 * turn + 2 - half, blocks - 1)
            old = jnp.maximum(2 * turn - half, 0)

            def norm():
                ln_ref[...] = layer_norm(read(new))

            def done():
                finish(old, leave(gt_refs[half], read(old), w_out(old)))

            return [norm, done] + project(ln_ref, pt_refs[half], w_in(new))

        both = [(pt_refs[half], gt_refs[half], keep(2 * turn + half)) for half in range(2)]
        attend_stream(both, others, HELD, 24, bias_ref, [
            (0, HELD - 2, jobs(1)), (HELD + 3 * LAG, 2 * HELD + 3 * LAG, jobs(0))])
        return carry

    lax.fori_loop(0, blocks // 2, body, 0)
    finish(blocks - 1, leave(gt_refs[1], read(blocks - 1), w_out(blocks - 1)))


def attend_scratch(heads, dim, keys, buffers):
    inner = heads * dim
    return [pltpu.VMEM((4 * inner, BLOCK), BF16)] * buffers + [pltpu.VMEM((inner, BLOCK), BF16)] * buffers + [
        pltpu.VMEM((SLOTS, LANES, 2 * dim), BF16),
        pltpu.VMEM((SLOTS, 2, keys, LANES), F32),
        pltpu.VMEM((SLOTS, 2, keys, LANES), BF16),
    ]


def wide_scratch(keys):
    return [pltpu.VMEM((BLOCK, WIDE), BF16)] + attend_scratch(HELD, 24, keys, 2)


def pick_column(table, col):
    lane = lax.broadcasted_iota(jnp.int32, table.shape, 1)
    return jnp.sum(jnp.where(lane == col, table, 0.0), axis=1, keepdims=True)


def row_keep(mask_ref, seq):
    left = lax.broadcasted_iota(jnp.int32, (RES, LANES), 1) < RES
    table = mask_ref[...].astype(F32)
    column = [pick_column(table, seq + n) for n in range(4)]
    return [jnp.where(left, column[2 * blk], column[2 * blk + 1]) > 0.5 for blk in range(2)]


def row_first_kernel(x_ref, z_ref, mask_ref, wb_ref, w_ref, wo_ref, out_ref, mo_ref, lnz_ref, nl_ref, rows_ref, bias_ref, spread_ref,
                     send_sem, recv_sem, *scratch):
    me = lax.axis_index('dap')
    mine = pl.ds(pl.multiple_of(HELD * me, HELD), HELD)
    greet(me)
    for part in range(4):
        lnz_ref[pl.ds(BLOCK * part, BLOCK), :] = layer_norm(z_ref[pl.ds(4 * part, 4)].reshape(BLOCK, LANES))
    nl_ref[...] = local_bias_rows(lnz_ref, wb_ref, spread_ref)
    meet()
    copies = group_copies(me, 8, send_sem, recv_sem, lambda peer: nl_ref, rows_ref.at[:, mine, :])
    start_all(copies)
    rows_ref[:, mine, :] = nl_ref[...]

    def ready():
        finish_all(copies)
        bias_by_query(rows_ref, bias_ref)

    def moves(block):
        return group_copies(
            me, block, send_sem, recv_sem,
            lambda peer: mo_ref.at[pl.ds(4 * block, 4), pl.ds(pl.multiple_of(HELD * peer, HELD), HELD), :],
            out_ref.at[pl.ds(32 * me + 4 * block, 4)])

    def emit(block):
        start_all(moves(block))
        out_ref[pl.ds(32 * me + 4 * block, 4)] = mo_ref[pl.ds(4 * block, 4), mine, :]

    def aside(turn):
        @pl.when(turn >= 2)
        def _():
            emit(2 * turn - 3)

        @pl.when(turn >= 1)
        def _():
            emit(2 * turn - 2)

    def finish(block, out):
        mo_ref[pl.ds(4 * block, 4)] = out.reshape(4, RES, WIDE)

    attend_blocks(8, scratch, lambda at: x_ref[pl.ds(at * 4, 4)].astype(F32).reshape(BLOCK, WIDE),
                  lambda at: lambda sl: w_ref[sl, :], lambda at: wo_ref[...],
                  lambda at: row_keep(mask_ref, 32 * me + 4 * at), bias_ref, finish, ready, aside)
    emit(5)
    emit(6)
    emit(7)

    def drain(block, carry):
        finish_all(moves(block))
        return carry

    lax.fori_loop(0, 8, drain, 0)


def bias_by_query(rows_ref, bias_ref):
    for head in range(rows_ref.shape[0]):
        turned = (rows_ref[head].astype(F32) * LOG2E).T[:RES]
        bias_ref[head] = jnp.concatenate([turned, turned], axis=1)


VMEM = pl.BlockSpec(memory_space=pltpu.VMEM)


def of_layer(array, layer):
    rank = array.ndim - 1
    return pl.BlockSpec((None,) + array.shape[1:], lambda i: (layer,) + (0,) * rank)


def whole(array):
    return pl.BlockSpec(array.shape, lambda i: (0,) * array.ndim)


def row_first(x, z, mask, wb, w, wo):
    return pl.pallas_call(
        row_first_kernel,
        grid=(1,),
        in_specs=[whole(x), whole(z), whole(mask)] + [of_layer(a, 0) for a in (wb, w, wo)],
        out_specs=VMEM,
        out_shape=jax.ShapeDtypeStruct((LANES, HELD, WIDE), BF16),
        scratch_shapes=[
            pltpu.VMEM((32, RES, WIDE), BF16),
            pltpu.VMEM((CELLS, LANES), BF16),
            pltpu.VMEM((HELD, HELD, LANES), BF16),
            pltpu.VMEM((HELD, RES, LANES), BF16),
            pltpu.VMEM((HELD, RES, LANES), F32),
            pltpu.VMEM((BLOCK, LANES), F32),
            pltpu.SemaphoreType.DMA((27,)),
            pltpu.SemaphoreType.DMA((27,)),
        ] + wide_scratch(RES),
        compiler_params=pltpu.CompilerParams(collective_id=0, has_side_effects=True),
        cost_estimate=pl.CostEstimate(flops=10 ** 10, bytes_accessed=2 ** 22, transcendentals=0),
        name="row_first",
    )(x, z, mask, wb, w, wo)


def row_last_kernel(x_ref, rows_ref, own_ref, full_ref, z_ref, mask_ref, res_ref, w_ref, wo_ref, wm_ref, wba_ref, wa_ref, woa_ref,
                    wbb_ref, wb_ref, wob_ref, out_ref, z_out_ref, wide_ref, m_ref, bias_ref, send_sem, recv_sem, *scratch):
    me = lax.axis_index('dap')
    greet(me)
    meet()
    outer, along, across, _ = pair_stages(
        me, 0, False, own_ref, full_ref, z_ref, mask_ref, res_ref, (wm_ref, wba_ref, wa_ref, woa_ref, wbb_ref, wb_ref, wob_ref),
        z_out_ref, None, send_sem, recv_sem, scratch[8:])
    outer(lambda: None)
    turn_tokens(x_ref, wide_ref, m_ref)
    bias_ref[...] = rows_ref[...].astype(F32) * LOG2E

    def finish(block, out):
        out_ref[pl.ds(4 * block, 4)] = out.reshape(4, RES, WIDE)

    def aside(turn):
        pl.when(turn == 1)(along)
        pl.when(turn == 2)(across)

    attend_blocks(8, scratch[:8], lambda at: m_ref[pl.ds(at * 4, 4)].astype(F32).reshape(BLOCK, WIDE),
                  lambda at: lambda sl: w_ref[sl, :], lambda at: wo_ref[...],
                  lambda at: row_keep(mask_ref, 32 * me + 4 * at), bias_ref, finish, lambda: None, aside)


def turn_tokens(x_ref, wide_ref, m_ref):
    outer, inner = x_ref.shape[:2]
    for part in range(3):
        lanes = pl.ds(LANES * part, LANES)
        wide_ref[part] = x_ref[:, :, lanes].astype(F32).reshape(outer * inner, LANES)

    def one(row, carry):
        for part in range(3):
            m_ref[row, :, pl.ds(LANES * part, LANES)] = wide_ref[part, pl.ds(row, outer, stride=inner), :].astype(BF16)
        return carry

    lax.fori_loop(0, inner, one, 0, unroll=2)


def row_last(args, weights):
    return pl.pallas_call(
        row_last_kernel,
        grid=(1,),
        in_specs=[whole(a) for a in args] + [of_layer(a, 1) for a in weights],
        out_specs=[VMEM] * 2,
        out_shape=[jax.ShapeDtypeStruct((32, RES, WIDE), BF16), jax.ShapeDtypeStruct((HELD, RES, LANES), BF16)],
        scratch_shapes=[
            pltpu.VMEM((3, 2048, LANES), F32),
            pltpu.VMEM((32, RES, WIDE), BF16),
            pltpu.VMEM((HELD, RES, LANES), F32),
            pltpu.SemaphoreType.DMA((12,)),
            pltpu.SemaphoreType.DMA((12,)),
        ] + wide_scratch(RES) + pair_scratch(),
        compiler_params=pltpu.CompilerParams(collective_id=2, has_side_effects=True),
        cost_estimate=pl.CostEstimate(flops=10 ** 10, bytes_accessed=2 ** 22, transcendentals=0),
        name="row_last",
    )(*args, *weights)


def col_kernel(x_ref, mask_ref, w_ref, wo_ref, wp_ref, z_ref, res_ref, wm_ref, wba_ref, wa_ref, woa_ref, wbb_ref, wb_ref, wob_ref, wn_ref,
               out_ref, own2_ref, full2_ref, z_out_ref, next_ref, own1_ref, full1_ref,
               wide_ref, m_ref, part_ref, keys_ref, send_sem, recv_sem, *scratch):
    me = lax.axis_index('dap')
    greet(me)
    turn_tokens(x_ref, wide_ref, m_ref.at[0])
    meet()
    mine = pl.ds(pl.multiple_of(HELD * me, HELD), HELD)
    keys_ref[...] = mask_ref[mine, :].astype(F32).T

    def keep(at):
        return [jnp.broadcast_to(pick_column(keys_ref[...], at % 8 * 2 + blk), (LANES, LANES)) > 0.5 for blk in range(2)]

    def finish(block, out):
        layer, pair = block // 8, block % 8
        m_ref[layer + 1, pl.ds(pair * 2, 2)] = out.reshape(2, LANES, WIDE)
        ac = lax.dot_general(wp_ref[layer], layer_norm(out), NT, preferred_element_type=F32)
        ac = (ac * jnp.concatenate([mask_ref[pl.ds(HELD * me + 2 * pair + blk, 1), :] for blk in range(2)], axis=1).astype(F32)).astype(BF16)
        parts = (ac[:32], ac[32:])
        own1_ref[pair] = jnp.where(layer == 0, parts[0].astype(F32), own1_ref[pair].astype(F32)).astype(BF16)
        own2_ref[pair] = parts[1]
        for blk in range(2):
            lanes = slice(LANES * blk, LANES * blk + LANES)
            part_ref[block, blk] = jnp.where(layer == 0, parts[1][:, lanes].astype(F32), parts[0][:, lanes].astype(F32)).astype(BF16)

    def part_copies(block, full_ref):
        return group_copies(me, block, send_sem, recv_sem, lambda peer: part_ref.at[block],
                            full_ref.at[pl.ds(HELD * me + block % 8 * 2, 2)])

    def seq_copies(pair):
        return group_copies(
            me, HELD + pair, send_sem, recv_sem,
            lambda peer: m_ref.at[2, pl.ds(2 * pair, 2), pl.ds(pl.multiple_of(32 * peer, 32), 32), :],
            out_ref.at[pl.ds(HELD * me + 2 * pair, 2)])

    outer, along, across, close = pair_stages(
        me, 24, True, own1_ref, full1_ref, z_ref, mask_ref, res_ref, (wm_ref, wba_ref, wa_ref, woa_ref, wbb_ref, wb_ref, wob_ref, wn_ref),
        z_out_ref, next_ref, send_sem, recv_sem, scratch[8:])

    def drain_parts(start, full_ref):
        def one(pair, carry):
            finish_all(part_copies(start + pair, full_ref))
            return carry
        lax.fori_loop(0, 8, one, 0)

    def emit_first(block):
        start_all(part_copies(block, full1_ref))
        full1_ref[pl.ds(HELD * me + 2 * block, 2)] = part_ref[block]

    def emit_second(block):
        pair = block - 8
        start_all(part_copies(block, full2_ref) + seq_copies(pair))
        full2_ref[pl.ds(HELD * me + 2 * pair, 2)] = part_ref[block]
        out_ref[pl.ds(HELD * me + 2 * pair, 2)] = m_ref[2, pl.ds(2 * pair, 2), pl.ds(pl.multiple_of(32 * me, 32), 32), :]

    def emit_any(block):
        pl.when(jnp.logical_and(block >= 0, block < 8))(lambda: emit_first(block))
        pl.when(block >= 8)(lambda: emit_second(block))

    def aside(turn):
        emit_any(2 * turn - 3)
        emit_any(2 * turn - 2)
        pl.when(turn == 5)(lambda: outer(lambda: drain_parts(0, full1_ref)))
        pl.when(turn == 6)(along)
        pl.when(turn == 7)(across)

    attend_blocks(16, scratch[:8], lambda at: m_ref[at // 8, pl.ds(at % 8 * 2, 2)].astype(F32).reshape(BLOCK, WIDE),
                  lambda at: lambda sl: w_ref[at // 8, sl, :], lambda at: wo_ref[at // 8],
                  keep, None, finish, lambda: None, aside)
    emit_second(13)
    emit_second(14)
    emit_second(15)

    close()
    drain_parts(8, full2_ref)

    def drain(pair, carry):
        finish_all(seq_copies(pair))
        return carry

    lax.fori_loop(0, 8, drain, 0)


def column_pair(args, weights, w_next):
    return pl.pallas_call(
        col_kernel,
        grid=(1,),
        in_specs=[whole(a) for a in args] + [of_layer(a, 0) for a in weights] + [of_layer(w_next, 1)],
        out_specs=[VMEM] * 5,
        out_shape=[
            jax.ShapeDtypeStruct((RES, 32, WIDE), BF16),
            jax.ShapeDtypeStruct((8, 32, BLOCK), BF16),
            jax.ShapeDtypeStruct((RES, 32, LANES), BF16),
            jax.ShapeDtypeStruct((HELD, RES, LANES), BF16),
            jax.ShapeDtypeStruct((HELD, RES, LANES), BF16),
        ],
        scratch_shapes=[
            pltpu.VMEM((8, 32, BLOCK), BF16),
            pltpu.VMEM((RES, 32, LANES), BF16),
            pltpu.VMEM((3, 2048, LANES), F32),
            pltpu.VMEM((3, HELD, LANES, WIDE), BF16),
            pltpu.VMEM((HELD, 2, 32, LANES), BF16),
            pltpu.VMEM((LANES, HELD), F32),
            pltpu.SemaphoreType.DMA((84,)),
            pltpu.SemaphoreType.DMA((84,)),
        ] + wide_scratch(LANES) + pair_scratch(),
        compiler_params=pltpu.CompilerParams(collective_id=1, has_side_effects=True),
        cost_estimate=pl.CostEstimate(flops=10 ** 10, bytes_accessed=2 ** 22, transcendentals=0),
        name="col_pair",
    )(*args, *weights, w_next)


def greet(me):
    barrier = pltpu.get_barrier_semaphore()
    for o in range(1, 4):
        pl.semaphore_signal(barrier, inc=1, device_id={'dap': lax.rem(me + o, 4)}, device_id_type=pl.DeviceIdType.MESH)


def meet():
    pl.semaphore_wait(pltpu.get_barrier_semaphore(), 3)


def group_copies(me, kind, send_sem, recv_sem, source, target):
    copies = []
    for o in range(1, 4):
        peer = lax.rem(me + o, 4)
        copies.append(pltpu.make_async_remote_copy(
            src_ref=source(peer), dst_ref=target, send_sem=send_sem.at[3 * kind + o - 1],
            recv_sem=recv_sem.at[3 * kind + o - 1], device_id={'dap': peer}, device_id_type=pl.DeviceIdType.MESH))
    return copies


def start_all(copies):
    for copy in copies:
        copy.start()


def finish_all(copies):
    for copy in copies:
        copy.wait()


def local_bias_rows(ln_ref, w_ref, spread_ref):
    heads = w_ref.shape[0]
    w = w_ref[...]
    if heads < 8:
        w = jnp.concatenate([w, jnp.zeros((8 - heads, LANES), BF16)], axis=0)
    values = lax.dot_general(w, ln_ref[...], NT, preferred_element_type=F32)
    left = lax.broadcasted_iota(jnp.int32, (heads, LANES), 1) < RES
    for two in range(8):
        value = values[:heads, LANES * two:LANES * two + LANES]
        turned = pltpu.roll(value, RES, 1)
        spread_ref[pl.ds(2 * two, heads, stride=HELD), :] = jnp.where(left, value, turned)
        spread_ref[pl.ds(2 * two + 1, heads, stride=HELD), :] = jnp.where(left, turned, value)
    return spread_ref[pl.ds(0, HELD * heads), :].astype(BF16).reshape(heads, HELD, LANES)


def triangle(zf_ref, ln_ref, w_ref, wo_ref, keep, bias_ref, pt_refs, gt_refs, others, ready):
    def fill(block):
        return project(ln_ref, pt_refs[block], lambda sl: w_ref[sl, :], pl.ds(BLOCK * block, BLOCK))

    def done(block):
        def job():
            rows = pl.ds(BLOCK * block, BLOCK)
            zf_ref[rows, :] = leave(gt_refs[block], zf_ref[rows, :], wo_ref[...]).astype(F32)
        return job

    for job in fill(0):
        job()
    ready()
    jobs = [(4 * block - 4, 4 * block - 1, fill(block)) for block in range(1, 4)]
    jobs += [(4 * block + 4 + 3 * LAG, 4 * block + 5 + 3 * LAG, [done(block)]) for block in range(3)]
    attend_stream([(pt_refs[block], gt_refs[block], [keep, keep]) for block in range(4)], others, 4, 32, bias_ref, jobs)
    done(3)()


def pair_stages(me, first, swap, own_ref, full_ref, z_ref, mask_ref, res_ref, weights, out_ref, next_ref, send_sem, recv_sem, scratch):
    wm_ref, wba_ref, wa_ref, woa_ref, wbb_ref, wb_ref, wob_ref = weights[:7]
    (full32_ref, o_ref, wt_ref, zf_ref, zt_ref, ln_ref, bias_ref, la_ref, ra_ref, lb_ref, rb_ref, zs_ref, zr_ref, nl_ref) = scratch[:14]
    att = scratch[14:]
    pt_refs, gt_refs, others = att[0:4], att[4:8], att[8:11]
    mine = pl.ds(pl.multiple_of(HELD * me, HELD), HELD)

    def keep():
        diagonal = lax.broadcasted_iota(jnp.int32, (RES, RES), 0) == lax.broadcasted_iota(jnp.int32, (RES, RES), 1)
        keys = jnp.sum(jnp.where(diagonal, jnp.broadcast_to(res_ref[...], (RES, RES)), 0).astype(F32), axis=1, keepdims=True)
        return jnp.broadcast_to(keys, (RES, LANES)) > 0.5

    def exchange(kind):
        source, target = (
            (lambda peer: la_ref, ra_ref.at[:, mine, :]),
            (lambda peer: zs_ref.at[:, pl.ds(pl.multiple_of(HELD * peer, HELD), HELD), :], zr_ref.at[mine]),
            (lambda peer: lb_ref, rb_ref.at[:, mine, :]),
            (lambda peer: nl_ref, None if next_ref is None else next_ref.at[:, mine, :]),
        )[kind]
        return group_copies(me, first + kind, send_sem, recv_sem, source, target)

    def outer(arrive):
        mask = mask_ref[...].astype(F32).astype(BF16)
        norm = lax.dot_general(mask, mask_ref[mine, :].astype(F32).astype(BF16), NT, preferred_element_type=F32)
        full32_ref[:CELLS] = wm_ref[...].astype(F32).reshape(CELLS, LANES)
        if swap:
            for q in range(32):
                wt_ref[pl.ds(32 * q, 32), :] = full32_ref[pl.ds(q, 32, stride=32), :].astype(BF16)
        else:
            wt_ref[...] = wm_ref[...].reshape(CELLS, LANES)
        w_turned = wt_ref[...].T
        arrive()
        full32_ref[...] = full_ref[...].astype(F32).reshape(2048, LANES)
        own = own_ref[...].reshape(BLOCK, BLOCK)
        zeros = jnp.zeros((RES, LANES), BF16)

        def one(q, carry):
            c_q = full32_ref[pl.ds(q, RES, stride=32), :].astype(BF16)
            rhs = jnp.concatenate([jnp.concatenate([c_q, zeros], axis=1), jnp.concatenate([zeros, c_q], axis=1)], axis=0)
            o = lax.dot_general(own, rhs, NT, preferred_element_type=F32).astype(BF16)
            for pair in range(8):
                o_ref[pair, pl.ds(pl.multiple_of(q * 32, 32), 32), :] = o[32 * pair:32 * pair + 32]
            return carry

        lax.fori_loop(0, 32, one, 0, unroll=4)
        for pair in range(8):
            update = jnp.dot(w_turned, o_ref[pair], preferred_element_type=F32).T
            z = z_ref[pl.ds(2 * pair, 2)].astype(F32).reshape(LANES, LANES)
            below = jnp.concatenate([pick_column(norm, 2 * pair), pick_column(norm, 2 * pair + 1)], axis=0)
            z = (z + update / (1e-3 + below)).astype(BF16).astype(F32)
            rows = pl.ds(LANES * pair, LANES)
            zf_ref[rows, :] = z
            ln_ref[rows, :] = layer_norm(z)
        la_ref[...] = local_bias_rows(ln_ref, wba_ref, zt_ref)
        start_all(exchange(0))
        ra_ref[:, mine, :] = la_ref[...]

    def along():
        def ready():
            finish_all(exchange(0))
            bias_by_query(ra_ref, bias_ref)

        triangle(zf_ref, ln_ref, wa_ref, woa_ref, keep(), bias_ref, pt_refs, gt_refs, others, ready)
        zs_ref[...] = zf_ref[...].astype(BF16).reshape(HELD, RES, LANES)
        norm_all(zf_ref, ln_ref)
        start_all(exchange(1))
        zr_ref[mine] = zs_ref[:, mine, :]
        lb_ref[...] = local_bias_rows(ln_ref, wbb_ref, zt_ref)
        start_all(exchange(2))
        rb_ref[:, mine, :] = lb_ref[...]

    def across():
        finish_all(exchange(1))
        zt_ref[...] = zr_ref[...].astype(F32).reshape(CELLS, LANES)
        for row in range(HELD):
            value = zt_ref[pl.ds(row, RES, stride=HELD), :]
            zf_ref[pl.ds(RES * row, RES), :] = value
            ln_ref[pl.ds(RES * row, RES), :] = layer_norm(value)

        def ready():
            finish_all(exchange(2))
            bias_ref[...] = rb_ref[...].astype(F32) * LOG2E

        triangle(zf_ref, ln_ref, wb_ref, wob_ref, keep(), bias_ref, pt_refs, gt_refs, others, ready)
        out_ref[...] = zf_ref[...].astype(BF16).reshape(HELD, RES, LANES)
        if next_ref is not None:
            norm_all(zf_ref, ln_ref)
            nl_ref[...] = local_bias_rows(ln_ref, weights[7], zt_ref)
            start_all(exchange(3))
            next_ref[:, mine, :] = nl_ref[...]

    def close():
        if next_ref is not None:
            finish_all(exchange(3))

    return outer, along, across, close


def pair_scratch():
    return [
        pltpu.VMEM((2048, LANES), F32),
        pltpu.VMEM((8, CELLS, LANES), BF16),
        pltpu.VMEM((CELLS, LANES), BF16),
        pltpu.VMEM((CELLS, LANES), F32),
        pltpu.VMEM((CELLS, LANES), F32),
        pltpu.VMEM((CELLS, LANES), BF16),
        pltpu.VMEM((4, RES, LANES), F32),
        pltpu.VMEM((4, HELD, LANES), BF16),
        pltpu.VMEM((4, RES, LANES), BF16),
        pltpu.VMEM((4, HELD, LANES), BF16),
        pltpu.VMEM((4, RES, LANES), BF16),
        pltpu.VMEM((HELD, RES, LANES), BF16),
        pltpu.VMEM((RES, HELD, LANES), BF16),
        pltpu.VMEM((HELD, HELD, LANES), BF16),
    ] + attend_scratch(4, 32, RES, 4)


def norm_all(zf_ref, ln_ref):
    for block in range(8):
        rows = pl.ds(LANES * block, LANES)
        ln_ref[rows, :] = layer_norm(zf_ref[rows, :])


def solution(mesh):
    def local_step(m, z, mask, res_mask, w_row_bias, w_row_in, w_row_out, w_col_in, w_col_out, w_opm_in, w_opm_out, w_ts_bias, w_ts_in, w_ts_out, w_te_bias, w_te_in, w_te_out):
        flat_in = lambda w: jnp.transpose(w, (0, 2, 3, 4, 1)).reshape(2, -1, w.shape[1])
        flat_out = lambda w: w.reshape(2, -1, w.shape[-1])
        flat_bias = lambda w: jnp.transpose(w, (0, 2, 1))
        w_row_in, w_col_in, w_ts_in, w_te_in = map(flat_in, (w_row_in, w_col_in, w_ts_in, w_te_in))
        w_row_out, w_col_out, w_ts_out, w_te_out = map(flat_out, (w_row_out, w_col_out, w_ts_out, w_te_out))
        w_row_bias, w_ts_bias, w_te_bias = map(flat_bias, (w_row_bias, w_ts_bias, w_te_bias))
        w_opm_in = jnp.transpose(w_opm_in, (0, 2, 3, 1)).reshape(2, RES, WIDE)
        w_opm_out = w_opm_out.reshape(2, CELLS, LANES)
        mask = mask.T
        res_mask = res_mask.reshape(1, RES)

        m = row_first(m, z, mask, w_row_bias, w_row_in, w_row_out)
        m, own, full, z, row_bias = column_pair(
            (m, mask, w_col_in, w_col_out, w_opm_in, z, res_mask),
            (w_opm_out, w_ts_bias, w_ts_in, w_ts_out, w_te_bias, w_te_in, w_te_out), w_row_bias)
        m, z = row_last(
            (m, row_bias, own, full, z, mask, res_mask),
            (w_row_in, w_row_out, w_opm_out, w_te_bias, w_te_in, w_te_out, w_ts_bias, w_ts_in, w_ts_out))
        return m, z

    in_specs = (P(('data', 'dap')), P(('data', 'dap')), P('data'), P('data')) + (P(),) * 13
    out_specs = (P(('data', 'dap')), P(('data', 'dap')))
    return jax.shard_map(local_step, mesh=mesh, in_specs=in_specs, out_specs=out_specs, check_vma=False)
```

```python
import functools

import jax
import jax.numpy as jnp
from jax import lax
from jax.experimental import pallas as pl
from jax.experimental.pallas import tpu as pltpu
from jax.sharding import PartitionSpec as P

LOG2E = 1.4426950408889634
NEG = -1e9 * LOG2E
F32 = jnp.float32
BF16 = jnp.bfloat16
LAG = 2
SLOTS = 4
NT = (((1,), (1,)), ((), ()))
LANES = 128
RES = 64
BLOCK = 256
HELD = 16
WIDE = 384
CELLS = 1024


def layer_norm(values):
    flat = values.astype(F32)
    row_mean = jnp.mean(flat, axis=-1, keepdims=True)
    centered = flat - row_mean
    row_var = jnp.mean(centered * centered, axis=-1, keepdims=True)
    return (centered * lax.rsqrt(row_var + 1e-5)).astype(BF16)


def half_masks(rows, split):
    index = lax.broadcasted_iota(jnp.int32, (rows, LANES), 0)
    upper = (index < split).astype(F32).astype(BF16)
    lower = (index >= split).astype(F32).astype(BF16)
    return upper, lower


def attend_stream(blocks, others, heads, dim, bias_ref, jobs):
    kt_ref, lg_ref, pr_ref = others
    width = heads * dim
    rows = 2 * dim
    pairs = heads // 2
    each = 2 * pairs
    keys = pl.ds(0, LANES if bias_ref is None else RES)
    units = each * len(blocks)
    up, low = half_masks(rows, dim)
    scale = dim ** -0.5 * LOG2E
    if bias_ref is not None:
        left = lax.broadcasted_iota(jnp.int32, (RES, LANES), 1) < RES
        left_b = left.astype(F32).astype(BF16)
        right_b = (1.0 - left.astype(F32)).astype(BF16)

    def place(unit):
        return blocks[unit // each], pl.ds(unit % each // pairs * LANES, LANES), rows * (unit % pairs)

    def turn_keys(unit):
        (pt_ref, _, _), ln, r = place(unit)
        kt_ref[unit % SLOTS] = pt_ref[pl.ds(width + r, rows), ln].T

    def make_logits(unit):
        (pt_ref, _, _), ln, r = place(unit)
        q = pt_ref[pl.ds(r, rows), ln]
        rhs = jnp.concatenate([q * up, q * low], axis=1)
        logits2 = jnp.dot(kt_ref[unit % SLOTS], rhs, preferred_element_type=F32)
        for half in range(2):
            lg = logits2[:, LANES * half:LANES * half + LANES]
            if bias_ref is not None:
                lg = jnp.where(left, lg[:RES], lg[RES:])
            lg_ref[unit % SLOTS, half, pl.ds(0, lg.shape[0])] = lg

    def soften(unit):
        (_, _, keep), _, _ = place(unit)
        for half in range(2):
            lg = lg_ref[unit % SLOTS, half, keys] * scale
            if bias_ref is not None:
                lg = lg + bias_ref[2 * (unit % pairs) + half]
            lg = jnp.where(keep[unit % each // pairs], lg, NEG)
            e = jnp.exp2(lg - jnp.max(lg, axis=0, keepdims=True))
            pr_ref[unit % SLOTS, half, keys] = (e * (1.0 / jnp.sum(e, axis=0, keepdims=True))).astype(BF16)

    def mix(unit):
        (pt_ref, gt_ref, _), ln, r = place(unit)
        v = pt_ref[pl.ds(2 * width + r, rows), ln]
        g = pt_ref[pl.ds(3 * width + r, rows), ln]
        probs = []
        for half in range(2):
            p = pr_ref[unit % SLOTS, half, keys]
            probs += [p] if bias_ref is None else [p * left_b, p * right_b]
        att = jnp.dot(jnp.concatenate([v * up, v * low], axis=1), jnp.concatenate(probs, axis=0), preferred_element_type=F32)
        gt_ref[pl.ds(r, rows), ln] = (att * jax.nn.sigmoid(g.astype(F32))).astype(BF16)

    stages = ((turn_keys, 0), (make_logits, LAG), (soften, 2 * LAG), (mix, 3 * LAG))
    for tick in range(units + 3 * LAG):
        for stage, lag in stages:
            if 0 <= tick - lag < units:
                stage(tick - lag)
        for start, end, work in jobs:
            if start <= tick < end:
                for job in work[len(work) * (tick - start) // (end - start):len(work) * (tick - start + 1) // (end - start)]:
                    job()


def project(ln_ref, pt_ref, w, rows=slice(None)):
    size = pt_ref.shape[0]
    chunk = BLOCK if size > CELLS else LANES

    def job(part):
        sl = pl.ds(part * chunk, chunk)
        pt_ref[sl, :] = lax.dot_general(w(sl), ln_ref[rows, :], NT, preferred_element_type=F32).astype(BF16)
    return [functools.partial(job, part) for part in range(size // chunk)]


def leave(gt_ref, x_old, wo):
    return (x_old + jnp.dot(gt_ref[...].T, wo, preferred_element_type=F32)).astype(BF16)


def attend_blocks(blocks, scratch, read, w_in, w_out, keep, bias_ref, finish, ready, aside):
    ln_ref, pt_refs, gt_refs, others = scratch[0], scratch[1:3], scratch[3:5], scratch[5:8]
    ln_ref[...] = layer_norm(read(0))
    for job in project(ln_ref, pt_refs[0], w_in(0)):
        job()
    ready()

    def body(turn, carry):
        aside(turn)

        def jobs(half):
            new = jnp.minimum(2 * turn + 2 - half, blocks - 1)
            old = jnp.maximum(2 * turn - half, 0)

            def norm():
                ln_ref[...] = layer_norm(read(new))

            def done():
                finish(old, leave(gt_refs[half], read(old), w_out(old)))

            return [norm, done] + project(ln_ref, pt_refs[half], w_in(new))

        both = [(pt_refs[half], gt_refs[half], keep(2 * turn + half)) for half in range(2)]
        attend_stream(both, others, HELD, 24, bias_ref, [
            (0, HELD - 2, jobs(1)), (HELD + 3 * LAG, 2 * HELD + 3 * LAG, jobs(0))])
        return carry

    lax.fori_loop(0, blocks // 2, body, 0)
    finish(blocks - 1, leave(gt_refs[1], read(blocks - 1), w_out(blocks - 1)))


def attend_scratch(heads, dim, keys, buffers):
    inner = heads * dim
    return [pltpu.VMEM((4 * inner, BLOCK), BF16)] * buffers + [pltpu.VMEM((inner, BLOCK), BF16)] * buffers + [
        pltpu.VMEM((SLOTS, LANES, 2 * dim), BF16),
        pltpu.VMEM((SLOTS, 2, keys, LANES), F32),
        pltpu.VMEM((SLOTS, 2, keys, LANES), BF16),
    ]


def wide_scratch(keys):
    return [pltpu.VMEM((BLOCK, WIDE), BF16)] + attend_scratch(HELD, 24, keys, 2)


def pick_column(table, col):
    lane = lax.broadcasted_iota(jnp.int32, table.shape, 1)
    return jnp.sum(jnp.where(lane == col, table, 0.0), axis=1, keepdims=True)


def row_keep(mask_ref, seq):
    left = lax.broadcasted_iota(jnp.int32, (RES, LANES), 1) < RES
    table = mask_ref[...].astype(F32)
    column = [pick_column(table, seq + n) for n in range(4)]
    return [jnp.where(left, column[2 * blk], column[2 * blk + 1]) > 0.5 for blk in range(2)]


def bias_by_query(rows_ref, bias_ref):
    for head in range(rows_ref.shape[0]):
        turned = (rows_ref[head].astype(F32) * LOG2E).T[:RES]
        bias_ref[head] = jnp.concatenate([turned, turned], axis=1)


VMEM = pl.BlockSpec(memory_space=pltpu.VMEM)


def of_layer(array, layer):
    rank = array.ndim - 1
    return pl.BlockSpec((None,) + array.shape[1:], lambda i: (layer,) + (0,) * rank)


def whole(array):
    return pl.BlockSpec(array.shape, lambda i: (0,) * array.ndim)


def turn_tokens(x_ref, wide_ref, put):
    outer, inner = x_ref.shape[:2]
    for part in range(3):
        wide_ref[part] = x_ref[:, :, pl.ds(LANES * part, LANES)].astype(F32).reshape(outer * inner, LANES)

    def one(row, carry):
        for part in range(3):
            put(row, pl.ds(LANES * part, LANES), wide_ref[part, pl.ds(row, outer, stride=inner), :].astype(BF16))
        return carry

    lax.fori_loop(0, inner, one, 0, unroll=4)


def kernel(x_ref, z_ref, mask_ref, res_ref, wrb_ref, wr_ref, wro_ref, wsb_ref, ws_ref, wso_ref, web_ref, we_ref, weo_ref, wnb_ref,
           wc_hbm, wco_hbm, wp_hbm, wm_hbm, wr_hbm, wro_hbm, out_ref, z_out_ref,
           wc_ref, wco_ref, wp_ref, wm_ref, wl_ref, wlo_ref, mo_ref, in_ref, wide_ref, m_ref, back_ref, ml_ref,
           rows_ref, bias_ref, part_ref, keys_ref, own1_ref, own2_ref, full1_ref, full2_ref, zc_ref, next_ref,
           send_sem, recv_sem, load_sem, *scratch):
    me = lax.axis_index('dap')
    greet(me)
    loads = [pltpu.make_async_copy(source, target, load_sem.at[n]) for n, (source, target) in enumerate((
        (wc_hbm, wc_ref), (wco_hbm, wco_ref), (wp_hbm, wp_ref), (wm_hbm, wm_ref), (wr_hbm.at[1], wl_ref), (wro_hbm.at[1], wlo_ref)))]
    start_all(loads)
    mine = pl.ds(pl.multiple_of(HELD * me, HELD), HELD)
    wide, pair = scratch[:8], scratch[8:]
    zf_ref, zt_ref, ln_ref, nl_ref = pair[3], pair[4], pair[5], pair[13]

    for part in range(4):
        ln_ref[pl.ds(BLOCK * part, BLOCK), :] = layer_norm(z_ref[pl.ds(4 * part, 4)].reshape(BLOCK, LANES))
    nl_ref[...] = local_bias_rows(ln_ref, wrb_ref, zt_ref)
    meet()
    copies = group_copies(me, 9, send_sem, recv_sem, lambda peer: nl_ref, rows_ref.at[:, mine, :])
    start_all(copies)
    rows_ref[:, mine, :] = nl_ref[...]

    def row_ready():
        finish_all(copies)
        bias_by_query(rows_ref, bias_ref)

    def moves(block):
        return group_copies(me, block, send_sem, recv_sem, lambda peer: mo_ref.at[2 * peer, pl.ds(4 * block, 4)],
                            in_ref.at[0, pl.ds(32 * me + 4 * block, 4)])

    def later_moves():
        return group_copies(me, 8, send_sem, recv_sem, lambda peer: mo_ref.at[2 * peer + 1], in_ref.at[1, pl.ds(32 * me, 32)])

    def row_aside(turn):
        pl.when(turn >= 2)(lambda: start_all(moves(2 * turn - 3)))
        pl.when(turn >= 1)(lambda: start_all(moves(2 * turn - 2)))

    def row_finish(block, out):
        out = out.astype(F32).reshape(4, 8, 8, WIDE)
        for group in range(8):
            mo_ref[group, pl.ds(4 * block, 4)] = out[:, group].astype(BF16)

    attend_blocks(8, wide, lambda at: x_ref[pl.ds(at * 4, 4)].astype(F32).reshape(BLOCK, WIDE),
                  lambda at: lambda sl: wr_ref[sl, :], lambda at: wro_ref[...],
                  lambda at: row_keep(mask_ref, 32 * me + 4 * at), bias_ref, row_finish, row_ready, row_aside)
    for block in range(5, 8):
        start_all(moves(block))
    start_all(later_moves())
    for half in range(2):
        in_ref[half, pl.ds(32 * me, 32)] = mo_ref[2 * me + half]

    finish_all(loads)
    keys_ref[...] = mask_ref[mine, :].astype(F32).T

    def take(half):
        def put(row, lanes, value):
            m_ref[0, 8 * half + row, :, lanes] = value
        turn_tokens(in_ref.at[half], wide_ref, put)

    def drain(count, copies_of):
        def one(n, carry):
            finish_all(copies_of(n))
            return carry
        lax.fori_loop(0, count, one, 0)

    def col_keep(at):
        return [jnp.broadcast_to(pick_column(keys_ref[...], at % 8 * 2 + blk), (LANES, LANES)) > 0.5 for blk in range(2)]

    def col_finish(block, out):
        layer, two = block // 8, block % 8
        m_ref[layer + 1, pl.ds(two * 2, 2)] = out.reshape(2, LANES, WIDE)
        ac = lax.dot_general(wp_ref[layer], layer_norm(out), NT, preferred_element_type=F32)
        ac = (ac * jnp.concatenate([mask_ref[pl.ds(HELD * me + 2 * two + blk, 1), :] for blk in range(2)], axis=1).astype(F32)).astype(BF16)
        parts = (ac[:32], ac[32:])
        own1_ref[two] = jnp.where(layer == 0, parts[0].astype(F32), own1_ref[two].astype(F32)).astype(BF16)
        own2_ref[two] = parts[1]
        for blk in range(2):
            lanes = slice(LANES * blk, LANES * blk + LANES)
            part_ref[block, blk] = jnp.where(layer == 0, parts[1][:, lanes].astype(F32), parts[0][:, lanes].astype(F32)).astype(BF16)

    def part_copies(block, full_ref):
        return group_copies(me, 10 + block, send_sem, recv_sem, lambda peer: part_ref.at[block],
                            full_ref.at[pl.ds(HELD * me + block % 8 * 2, 2)])

    def seq_copies(two):
        return group_copies(
            me, 26 + two, send_sem, recv_sem,
            lambda peer: m_ref.at[2, pl.ds(2 * two, 2), pl.ds(pl.multiple_of(32 * peer, 32), HELD), :],
            back_ref.at[0, pl.ds(HELD * me + 2 * two, 2)])

    def later_seqs():
        return group_copies(
            me, 34, send_sem, recv_sem, lambda peer: m_ref.at[2, :, pl.ds(pl.multiple_of(32 * peer + HELD, HELD), HELD), :],
            back_ref.at[1, mine])

    def emit(block):
        def first():
            start_all(part_copies(block, full1_ref))
            full1_ref[pl.ds(HELD * me + 2 * block, 2)] = part_ref[block]

        def second():
            start_all(part_copies(block, full2_ref) + seq_copies(block - 8))
            full2_ref[pl.ds(HELD * me + 2 * (block - 8), 2)] = part_ref[block]

        if isinstance(block, int):
            second()
        else:
            pl.when(jnp.logical_and(block >= 0, block < 8))(first)
            pl.when(block >= 8)(second)

    outer, along, across, close = pair_stages(
        me, 35, True, own1_ref, full1_ref, z_ref, mask_ref, res_ref,
        (wm_ref.at[0], wsb_ref.at[0], ws_ref.at[0], wso_ref.at[0], web_ref.at[0], we_ref.at[0], weo_ref.at[0], wnb_ref),
        zc_ref, next_ref, send_sem, recv_sem, pair)

    def second_half():
        finish_all(later_moves())
        take(1)

    def col_aside(turn):
        emit(2 * turn - 3)
        emit(2 * turn - 2)
        pl.when(turn == 1)(second_half)
        pl.when(turn == 6)(lambda: outer(lambda: drain(8, lambda n: part_copies(n, full1_ref))))
        pl.when(turn == 7)(along)

    drain(8, moves)
    take(0)
    attend_blocks(16, wide, lambda at: m_ref[at // 8, pl.ds(at % 8 * 2, 2)].astype(F32).reshape(BLOCK, WIDE),
                  lambda at: lambda sl: wc_ref[at // 8, sl, :], lambda at: wco_ref[at // 8],
                  col_keep, None, col_finish, lambda: None, col_aside)
    for block in range(13, 16):
        emit(block)
    start_all(later_seqs())
    for half in range(2):
        back_ref[half, mine] = m_ref[2, :, pl.ds(pl.multiple_of(32 * me + HELD * half, HELD), HELD), :]
    across()

    outer, along_2, across_2, _ = pair_stages(
        me, 39, False, own2_ref, full2_ref, zc_ref, mask_ref, res_ref,
        (wm_ref.at[1], web_ref.at[1], we_ref.at[1], weo_ref.at[1], wsb_ref.at[1], ws_ref.at[1], wso_ref.at[1]),
        z_out_ref, None, send_sem, recv_sem, pair)
    outer(lambda: drain(8, lambda n: part_copies(n + 8, full2_ref)))

    def take_back(half):
        def put(row, lanes, value):
            ml_ref[HELD * half + row, :, lanes] = value
        turn_tokens(back_ref.at[half], wide_ref, put)

    def last_half():
        finish_all(later_seqs())
        take_back(1)

    def last_aside(turn):
        pl.when(turn == 1)(along_2)
        pl.when(turn == 1)(last_half)
        pl.when(turn == 2)(across_2)

    def last_ready():
        close()
        bias_ref[...] = next_ref[...].astype(F32) * LOG2E

    def last_finish(block, out):
        out_ref[pl.ds(4 * block, 4)] = out.reshape(4, RES, WIDE)

    drain(8, seq_copies)
    take_back(0)
    attend_blocks(8, wide, lambda at: ml_ref[pl.ds(at * 4, 4)].astype(F32).reshape(BLOCK, WIDE),
                  lambda at: lambda sl: wl_ref[sl, :], lambda at: wlo_ref[...],
                  lambda at: row_keep(mask_ref, 32 * me + 4 * at), bias_ref, last_finish, last_ready, last_aside)


def run_all(m, z, mask, res_mask, row, tri, streamed):
    w_row_bias, w_row_in, w_row_out = row
    args = (m, z, mask, res_mask) + row + tri + (w_row_bias,) + streamed
    specs = [whole(a) for a in args[:4]] + [of_layer(a, 0) for a in row] + [whole(a) for a in tri] + [of_layer(w_row_bias, 1)]
    specs += [pl.BlockSpec(memory_space=pl.ANY)] * len(streamed)
    vmem = lambda *shape: pltpu.VMEM(shape, BF16)
    return pl.pallas_call(
        kernel,
        grid=(1,),
        in_specs=specs,
        out_specs=[VMEM] * 2,
        out_shape=[jax.ShapeDtypeStruct(m.shape, BF16), jax.ShapeDtypeStruct(z.shape, BF16)],
        scratch_shapes=[
            vmem(2, 4 * WIDE, WIDE),
            vmem(2, WIDE, WIDE),
            vmem(2, RES, WIDE),
            vmem(2, CELLS, LANES),
            vmem(4 * WIDE, WIDE),
            vmem(WIDE, WIDE),
            vmem(8, 32, 8, WIDE),
            vmem(2, LANES, 8, WIDE),
            pltpu.VMEM((3, CELLS, LANES), F32),
            vmem(3, HELD, LANES, WIDE),
            vmem(2, RES, HELD, WIDE),
            vmem(32, RES, WIDE),
            vmem(HELD, RES, LANES),
            pltpu.VMEM((HELD, RES, LANES), F32),
            vmem(HELD, 2, 32, LANES),
            pltpu.VMEM((LANES, HELD), F32),
            vmem(8, 32, BLOCK),
            vmem(8, 32, BLOCK),
            vmem(RES, 32, LANES),
            vmem(RES, 32, LANES),
            vmem(HELD, RES, LANES),
            vmem(HELD, RES, LANES),
            pltpu.SemaphoreType.DMA((126,)),
            pltpu.SemaphoreType.DMA((126,)),
            pltpu.SemaphoreType.DMA((6,)),
        ] + wide_scratch(LANES) + pair_scratch(),
        compiler_params=pltpu.CompilerParams(collective_id=0, has_side_effects=True),
        cost_estimate=pl.CostEstimate(flops=10 ** 10, bytes_accessed=2 ** 22, transcendentals=0),
        name="evoformer",
    )(*args)


def greet(me):
    barrier = pltpu.get_barrier_semaphore()
    for o in range(1, 4):
        pl.semaphore_signal(barrier, inc=1, device_id={'dap': lax.rem(me + o, 4)}, device_id_type=pl.DeviceIdType.MESH)


def meet():
    pl.semaphore_wait(pltpu.get_barrier_semaphore(), 3)


def group_copies(me, kind, send_sem, recv_sem, source, target):
    copies = []
    for o in range(1, 4):
        peer = lax.rem(me + o, 4)
        copies.append(pltpu.make_async_remote_copy(
            src_ref=source(peer), dst_ref=target, send_sem=send_sem.at[3 * kind + o - 1],
            recv_sem=recv_sem.at[3 * kind + o - 1], device_id={'dap': peer}, device_id_type=pl.DeviceIdType.MESH))
    return copies


def start_all(copies):
    for copy in copies:
        copy.start()


def finish_all(copies):
    for copy in copies:
        copy.wait()


def local_bias_rows(ln_ref, w_ref, spread_ref):
    heads = w_ref.shape[0]
    w = w_ref[...]
    if heads < 8:
        w = jnp.concatenate([w, jnp.zeros((8 - heads, LANES), BF16)], axis=0)
    values = lax.dot_general(w, ln_ref[...], NT, preferred_element_type=F32)
    left = lax.broadcasted_iota(jnp.int32, (heads, LANES), 1) < RES
    for two in range(8):
        value = values[:heads, LANES * two:LANES * two + LANES]
        turned = pltpu.roll(value, RES, 1)
        spread_ref[pl.ds(2 * two, heads, stride=HELD), :] = jnp.where(left, value, turned)
        spread_ref[pl.ds(2 * two + 1, heads, stride=HELD), :] = jnp.where(left, turned, value)
    return spread_ref[pl.ds(0, HELD * heads), :].astype(BF16).reshape(heads, HELD, LANES)


def triangle(zf_ref, ln_ref, w_ref, wo_ref, keep, bias_ref, pt_refs, gt_refs, others, ready):
    def fill(block):
        return project(ln_ref, pt_refs[block], lambda sl: w_ref[sl, :], pl.ds(BLOCK * block, BLOCK))

    def done(block):
        def job():
            rows = pl.ds(BLOCK * block, BLOCK)
            zf_ref[rows, :] = leave(gt_refs[block], zf_ref[rows, :], wo_ref[...]).astype(F32)
        return job

    for job in fill(0):
        job()
    ready()
    jobs = [(4 * block - 4, 4 * block - 1, fill(block)) for block in range(1, 4)]
    jobs += [(4 * block + 4 + 3 * LAG, 4 * block + 5 + 3 * LAG, [done(block)]) for block in range(3)]
    attend_stream([(pt_refs[block], gt_refs[block], [keep, keep]) for block in range(4)], others, 4, 32, bias_ref, jobs)
    done(3)()


def pair_stages(me, first, swap, own_ref, full_ref, z_ref, mask_ref, res_ref, weights, out_ref, next_ref, send_sem, recv_sem, scratch):
    wm_ref, wba_ref, wa_ref, woa_ref, wbb_ref, wb_ref, wob_ref = weights[:7]
    (full32_ref, o_ref, wt_ref, zf_ref, zt_ref, ln_ref, bias_ref, la_ref, ra_ref, lb_ref, rb_ref, zs_ref, zr_ref, nl_ref) = scratch[:14]
    att = scratch[14:]
    pt_refs, gt_refs, others = att[0:4], att[4:8], att[8:11]
    mine = pl.ds(pl.multiple_of(HELD * me, HELD), HELD)

    def keep():
        diagonal = lax.broadcasted_iota(jnp.int32, (RES, RES), 0) == lax.broadcasted_iota(jnp.int32, (RES, RES), 1)
        keys = jnp.sum(jnp.where(diagonal, jnp.broadcast_to(res_ref[...], (RES, RES)), 0).astype(F32), axis=1, keepdims=True)
        return jnp.broadcast_to(keys, (RES, LANES)) > 0.5

    def exchange(kind):
        source, target = (
            (lambda peer: la_ref, ra_ref.at[:, mine, :]),
            (lambda peer: zs_ref.at[:, pl.ds(pl.multiple_of(HELD * peer, HELD), HELD), :], zr_ref.at[mine]),
            (lambda peer: lb_ref, rb_ref.at[:, mine, :]),
            (lambda peer: nl_ref, None if next_ref is None else next_ref.at[:, mine, :]),
        )[kind]
        return group_copies(me, first + kind, send_sem, recv_sem, source, target)

    def outer(arrive):
        mask = mask_ref[...].astype(F32).astype(BF16)
        norm = lax.dot_general(mask, mask_ref[mine, :].astype(F32).astype(BF16), NT, preferred_element_type=F32)
        full32_ref[:CELLS] = wm_ref[...].astype(F32).reshape(CELLS, LANES)
        if swap:
            for q in range(32):
                wt_ref[pl.ds(32 * q, 32), :] = full32_ref[pl.ds(q, 32, stride=32), :].astype(BF16)
        else:
            wt_ref[...] = wm_ref[...].reshape(CELLS, LANES)
        w_turned = wt_ref[...].T
        arrive()
        full32_ref[...] = full_ref[...].astype(F32).reshape(2048, LANES)
        own = own_ref[...].reshape(BLOCK, BLOCK)
        zeros = jnp.zeros((RES, LANES), BF16)

        def one(q, carry):
            c_q = full32_ref[pl.ds(q, RES, stride=32), :].astype(BF16)
            rhs = jnp.concatenate([jnp.concatenate([c_q, zeros], axis=1), jnp.concatenate([zeros, c_q], axis=1)], axis=0)
            o = lax.dot_general(own, rhs, NT, preferred_element_type=F32).astype(BF16)
            for pair in range(8):
                o_ref[pair, pl.ds(pl.multiple_of(q * 32, 32), 32), :] = o[32 * pair:32 * pair + 32]
            return carry

        lax.fori_loop(0, 32, one, 0, unroll=4)
        for pair in range(8):
            update = jnp.dot(w_turned, o_ref[pair], preferred_element_type=F32).T
            z = z_ref[pl.ds(2 * pair, 2)].astype(F32).reshape(LANES, LANES)
            below = jnp.concatenate([pick_column(norm, 2 * pair), pick_column(norm, 2 * pair + 1)], axis=0)
            z = (z + update / (1e-3 + below)).astype(BF16).astype(F32)
            rows = pl.ds(LANES * pair, LANES)
            zf_ref[rows, :] = z
            ln_ref[rows, :] = layer_norm(z)
        la_ref[...] = local_bias_rows(ln_ref, wba_ref, zt_ref)
        start_all(exchange(0))
        ra_ref[:, mine, :] = la_ref[...]

    def along():
        def ready():
            finish_all(exchange(0))
            bias_by_query(ra_ref, bias_ref)

        triangle(zf_ref, ln_ref, wa_ref, woa_ref, keep(), bias_ref, pt_refs, gt_refs, others, ready)
        zs_ref[...] = zf_ref[...].astype(BF16).reshape(HELD, RES, LANES)
        norm_all(zf_ref, ln_ref)
        start_all(exchange(1))
        zr_ref[mine] = zs_ref[:, mine, :]
        lb_ref[...] = local_bias_rows(ln_ref, wbb_ref, zt_ref)
        start_all(exchange(2))
        rb_ref[:, mine, :] = lb_ref[...]

    def across():
        finish_all(exchange(1))
        zt_ref[...] = zr_ref[...].astype(F32).reshape(CELLS, LANES)
        for row in range(HELD):
            value = zt_ref[pl.ds(row, RES, stride=HELD), :]
            zf_ref[pl.ds(RES * row, RES), :] = value
            ln_ref[pl.ds(RES * row, RES), :] = layer_norm(value)

        def ready():
            finish_all(exchange(2))
            bias_ref[...] = rb_ref[...].astype(F32) * LOG2E

        triangle(zf_ref, ln_ref, wb_ref, wob_ref, keep(), bias_ref, pt_refs, gt_refs, others, ready)
        out_ref[...] = zf_ref[...].astype(BF16).reshape(HELD, RES, LANES)
        if next_ref is not None:
            norm_all(zf_ref, ln_ref)
            nl_ref[...] = local_bias_rows(ln_ref, weights[7], zt_ref)
            start_all(exchange(3))
            next_ref[:, mine, :] = nl_ref[...]

    def close():
        if next_ref is not None:
            finish_all(exchange(3))

    return outer, along, across, close


def pair_scratch():
    return [
        pltpu.VMEM((2048, LANES), F32),
        pltpu.VMEM((8, CELLS, LANES), BF16),
        pltpu.VMEM((CELLS, LANES), BF16),
        pltpu.VMEM((CELLS, LANES), F32),
        pltpu.VMEM((CELLS, LANES), F32),
        pltpu.VMEM((CELLS, LANES), BF16),
        pltpu.VMEM((4, RES, LANES), F32),
        pltpu.VMEM((4, HELD, LANES), BF16),
        pltpu.VMEM((4, RES, LANES), BF16),
        pltpu.VMEM((4, HELD, LANES), BF16),
        pltpu.VMEM((4, RES, LANES), BF16),
        pltpu.VMEM((HELD, RES, LANES), BF16),
        pltpu.VMEM((RES, HELD, LANES), BF16),
        pltpu.VMEM((HELD, HELD, LANES), BF16),
    ] + attend_scratch(4, 32, RES, 4)


def norm_all(zf_ref, ln_ref):
    for block in range(8):
        rows = pl.ds(LANES * block, LANES)
        ln_ref[rows, :] = layer_norm(zf_ref[rows, :])


def solution(mesh):
    def local_step(m, z, mask, res_mask, w_row_bias, w_row_in, w_row_out, w_col_in, w_col_out, w_opm_in, w_opm_out, w_ts_bias, w_ts_in, w_ts_out, w_te_bias, w_te_in, w_te_out):
        flat_in = lambda w: jnp.transpose(w, (0, 2, 3, 4, 1)).reshape(2, -1, w.shape[1])
        flat_out = lambda w: w.reshape(2, -1, w.shape[-1])
        flat_bias = lambda w: jnp.transpose(w, (0, 2, 1))
        w_row_in, w_col_in, w_ts_in, w_te_in = map(flat_in, (w_row_in, w_col_in, w_ts_in, w_te_in))
        w_row_out, w_col_out, w_ts_out, w_te_out = map(flat_out, (w_row_out, w_col_out, w_ts_out, w_te_out))
        w_row_bias, w_ts_bias, w_te_bias = map(flat_bias, (w_row_bias, w_ts_bias, w_te_bias))
        w_opm_in = jnp.transpose(w_opm_in, (0, 2, 3, 1)).reshape(2, RES, WIDE)
        w_opm_out = w_opm_out.reshape(2, CELLS, LANES)
        mask = mask.T
        res_mask = res_mask.reshape(1, RES)

        m, z = run_all(
            m, z, mask, res_mask, (w_row_bias, w_row_in, w_row_out),
            (w_ts_bias, w_ts_in, w_ts_out, w_te_bias, w_te_in, w_te_out),
            (w_col_in, w_col_out, w_opm_in, w_opm_out, w_row_in, w_row_out))
        return m, z

    in_specs = (P(('data', 'dap')), P(('data', 'dap')), P('data'), P('data')) + (P(),) * 13
    out_specs = (P(('data', 'dap')), P(('data', 'dap')))
    return jax.shard_map(local_step, mesh=mesh, in_specs=in_specs, out_specs=out_specs, check_vma=False)
```

```python
import functools

import jax
import jax.numpy as jnp
from jax import lax
from jax.experimental import pallas as pl
from jax.experimental.pallas import tpu as pltpu
from jax.sharding import PartitionSpec as P

LOG2E = 1.4426950408889634
NEG = -1e9 * LOG2E
F32 = jnp.float32
BF16 = jnp.bfloat16
LAG = 2
SLOTS = 4
NT = (((1,), (1,)), ((), ()))
SEQS = 32
LANES = 128
RES = 64
BLOCK = 256
HELD = 16
WIDE = 384
CELLS = 1024


def layer_norm(values):
    flat = values.astype(F32)
    row_mean = jnp.mean(flat, axis=-1, keepdims=True)
    centered = flat - row_mean
    row_var = jnp.mean(centered * centered, axis=-1, keepdims=True)
    return (centered * lax.rsqrt(row_var + 1e-5)).astype(BF16)


def half_masks(rows, split):
    index = lax.broadcasted_iota(jnp.int32, (rows, LANES), 0)
    upper = (index < split).astype(F32).astype(BF16)
    lower = (index >= split).astype(F32).astype(BF16)
    return upper, lower


def attend_stream(blocks, others, heads, dim, bias_ref, jobs):
    kt_ref, lg_ref, pr_ref = others
    width = heads * dim
    rows = 2 * dim
    pairs = heads // 2
    each = 2 * pairs
    keys = pl.ds(0, LANES if bias_ref is None else RES)
    units = each * len(blocks)
    up, low = half_masks(rows, dim)
    scale = dim ** -0.5 * LOG2E
    if bias_ref is not None:
        left = lax.broadcasted_iota(jnp.int32, (RES, LANES), 1) < RES
        left_b = left.astype(F32).astype(BF16)
        right_b = (1.0 - left.astype(F32)).astype(BF16)

    def place(unit):
        return blocks[unit // each], pl.ds(unit % each // pairs * LANES, LANES), rows * (unit % pairs)

    def turn_keys(unit):
        (pt_ref, _, _), ln, r = place(unit)
        kt_ref[unit % SLOTS] = pt_ref[pl.ds(width + r, rows), ln].T

    def make_logits(unit):
        (pt_ref, _, _), ln, r = place(unit)
        q = pt_ref[pl.ds(r, rows), ln]
        rhs = jnp.concatenate([q * up, q * low], axis=1)
        logits2 = jnp.dot(kt_ref[unit % SLOTS], rhs, preferred_element_type=F32)
        for half in range(2):
            lg = logits2[:, LANES * half:LANES * half + LANES]
            if bias_ref is not None:
                lg = jnp.where(left, lg[:RES], lg[RES:])
            lg_ref[unit % SLOTS, half, pl.ds(0, lg.shape[0])] = lg

    def soften(unit):
        (_, _, keep), _, _ = place(unit)
        for half in range(2):
            lg = lg_ref[unit % SLOTS, half, keys] * scale
            if bias_ref is not None:
                lg = lg + bias_ref[2 * (unit % pairs) + half]
            lg = jnp.where(keep[unit % each // pairs], lg, NEG)
            e = jnp.exp2(lg - jnp.max(lg, axis=0, keepdims=True))
            pr_ref[unit % SLOTS, half, keys] = (e * (1.0 / jnp.sum(e, axis=0, keepdims=True))).astype(BF16)

    def mix(unit):
        (pt_ref, gt_ref, _), ln, r = place(unit)
        v = pt_ref[pl.ds(2 * width + r, rows), ln]
        g = pt_ref[pl.ds(3 * width + r, rows), ln]
        probs = []
        for half in range(2):
            p = pr_ref[unit % SLOTS, half, keys]
            probs += [p] if bias_ref is None else [p * left_b, p * right_b]
        att = jnp.dot(jnp.concatenate([v * up, v * low], axis=1), jnp.concatenate(probs, axis=0), preferred_element_type=F32)
        gt_ref[pl.ds(r, rows), ln] = (att * jax.nn.sigmoid(g.astype(F32))).astype(BF16)

    stages = ((turn_keys, 0), (make_logits, LAG), (soften, 2 * LAG), (mix, 3 * LAG))
    for tick in range(units + 3 * LAG):
        for stage, lag in stages:
            if 0 <= tick - lag < units:
                stage(tick - lag)
        for start, end, work in jobs:
            if start <= tick < end:
                for job in work[len(work) * (tick - start) // (end - start):len(work) * (tick - start + 1) // (end - start)]:
                    job()


def project(ln_ref, pt_ref, w, rows=slice(None)):
    size = pt_ref.shape[0]
    chunk = BLOCK if size > CELLS else LANES

    def job(part):
        sl = pl.ds(part * chunk, chunk)
        pt_ref[sl, :] = lax.dot_general(w(sl), ln_ref[rows, :], NT, preferred_element_type=F32).astype(BF16)
    return [functools.partial(job, part) for part in range(size // chunk)]


def leave(gt_ref, x_old, wo):
    return (x_old + jnp.dot(gt_ref[...].T, wo, preferred_element_type=F32)).astype(BF16)


def attend_blocks(blocks, scratch, read, w_in, w_out, keep, bias_ref, finish, ready, aside):
    ln_ref, pt_refs, gt_refs, others = scratch[0], scratch[1:3], scratch[3:5], scratch[5:8]
    ln_ref[...] = layer_norm(read(0))
    for job in project(ln_ref, pt_refs[0], w_in(0)):
        job()
    ready()

    def body(turn, carry):
        aside(turn)

        def jobs(half):
            new = jnp.minimum(2 * turn + 2 - half, blocks - 1)
            old = jnp.maximum(2 * turn - half, 0)

            def norm():
                ln_ref[...] = layer_norm(read(new))

            def done():
                finish(old, leave(gt_refs[half], read(old), w_out(old)))

            return [norm, done] + project(ln_ref, pt_refs[half], w_in(new))

        both = [(pt_refs[half], gt_refs[half], keep(2 * turn + half)) for half in range(2)]
        attend_stream(both, others, HELD, 24, bias_ref, [
            (0, HELD - 2, jobs(1)), (HELD + 3 * LAG, 2 * HELD + 3 * LAG, jobs(0))])
        return carry

    lax.fori_loop(0, blocks // 2, body, 0)
    finish(blocks - 1, leave(gt_refs[1], read(blocks - 1), w_out(blocks - 1)))


def attend_scratch(heads, dim, keys, buffers):
    inner = heads * dim
    return [pltpu.VMEM((4 * inner, BLOCK), BF16)] * buffers + [pltpu.VMEM((inner, BLOCK), BF16)] * buffers + [
        pltpu.VMEM((SLOTS, LANES, 2 * dim), BF16),
        pltpu.VMEM((SLOTS, 2, keys, LANES), F32),
        pltpu.VMEM((SLOTS, 2, keys, LANES), BF16),
    ]


def wide_scratch(keys):
    return [pltpu.VMEM((BLOCK, WIDE), BF16)] + attend_scratch(HELD, 24, keys, 2)


def pick_column(table, col):
    lane = lax.broadcasted_iota(jnp.int32, table.shape, 1)
    return jnp.sum(jnp.where(lane == col, table, 0.0), axis=1, keepdims=True)


def row_keep(mask_ref, seq):
    left = lax.broadcasted_iota(jnp.int32, (RES, LANES), 1) < RES
    table = mask_ref[...].astype(F32)
    column = [pick_column(table, seq + n) for n in range(4)]
    return [jnp.where(left, column[2 * blk], column[2 * blk + 1]) > 0.5 for blk in range(2)]


VMEM = pl.BlockSpec(memory_space=pltpu.VMEM)


def of_layer(array, layer):
    rank = array.ndim - 1
    return pl.BlockSpec((None,) + array.shape[1:], lambda i: (layer,) + (0,) * rank)


def whole(array):
    return pl.BlockSpec(array.shape, lambda i: (0,) * array.ndim)


def turn_tokens(x_ref, wide_ref, put):
    outer, inner = x_ref.shape[:2]
    for part in range(3):
        wide_ref[part] = x_ref[:, :, pl.ds(LANES * part, LANES)].astype(F32).reshape(outer * inner, LANES)

    def one(row, carry):
        for part in range(3):
            put(row, pl.ds(LANES * part, LANES), wide_ref[part, pl.ds(row, outer, stride=inner), :].astype(BF16))
        return carry

    lax.fori_loop(0, inner, one, 0, unroll=4)


def kernel(x_ref, z_ref, mask_ref, res_ref, wrb_ref, wr_ref, wro_ref, wsb_ref, ws_ref, wso_ref, web_ref, we_ref, weo_ref, wnb_ref,
           wc_hbm, wco_hbm, wp_hbm, wm_hbm, wr_hbm, wro_hbm, out_ref, z_out_ref,
           wc_ref, wco_ref, wp_ref, wm_ref, wl_ref, wlo_ref, mo_ref, in_ref, wide_ref, m_ref, back_ref, ml_ref,
           rows_ref, bias_ref, part_ref, keys_ref, own1_ref, own2_ref, full1_ref, full2_ref, zc_ref, next_ref,
           send_sem, recv_sem, load_sem, *scratch):
    me = lax.axis_index('dap')
    greet(me)
    loads = [pltpu.make_async_copy(source, target, load_sem.at[n]) for n, (source, target) in enumerate((
        (wc_hbm, wc_ref), (wco_hbm, wco_ref), (wp_hbm, wp_ref), (wm_hbm, wm_ref), (wr_hbm.at[1], wl_ref), (wro_hbm.at[1], wlo_ref)))]
    start_all(loads)
    mine = pl.ds(pl.multiple_of(HELD * me, HELD), HELD)
    wide, pair = scratch[:8], scratch[8:]
    zf_ref, zt_ref, ln_ref, nl_ref = pair[3], pair[4], pair[5], pair[13]

    for part in range(4):
        ln_ref[pl.ds(BLOCK * part, BLOCK), :] = layer_norm(z_ref[pl.ds(4 * part, 4)].reshape(BLOCK, LANES))
    nl_ref[...] = local_bias_rows(ln_ref, wrb_ref, zt_ref)
    meet()
    copies = group_copies(me, 9, send_sem, recv_sem, lambda peer: nl_ref, rows_ref.at[:, mine, :])
    start_all(copies)
    rows_ref[:, mine, :] = nl_ref[...]

    def row_ready():
        finish_all(copies)
        bias_by_query(rows_ref, bias_ref)

    def moves(block):
        return group_copies(me, block, send_sem, recv_sem, lambda peer: mo_ref.at[2 * peer, pl.ds(4 * block, 4)],
                            in_ref.at[0, pl.ds(SEQS * me + 4 * block, 4)])

    def later_moves(part):
        start, count, kind = ((0, 4, 8), (4, 4, 42), (8, 24, 43))[part]
        return group_copies(me, kind, send_sem, recv_sem, lambda peer: mo_ref.at[2 * peer + 1, pl.ds(start, count)],
                            in_ref.at[1, pl.ds(SEQS * me + start, count)])

    def row_aside(turn):
        pl.when(turn >= 2)(lambda: start_all(moves(2 * turn - 3)))
        pl.when(turn >= 1)(lambda: start_all(moves(2 * turn - 2)))
        pl.when(turn == 2)(lambda: start_all(later_moves(0)))
        pl.when(turn == 3)(lambda: start_all(later_moves(1)))

    def row_finish(block, out):
        out = out.astype(F32).reshape(4, 8, 8, WIDE)
        for group in range(8):
            mo_ref[group, pl.ds(4 * block, 4)] = out[:, group].astype(BF16)

    attend_blocks(8, wide, lambda at: x_ref[pl.ds(at * 4, 4)].astype(F32).reshape(BLOCK, WIDE),
                  lambda at: lambda sl: wr_ref[sl, :], lambda at: wro_ref[...],
                  lambda at: row_keep(mask_ref, SEQS * me + 4 * at), bias_ref, row_finish, row_ready, row_aside)
    for block in range(5, 8):
        start_all(moves(block))
    start_all(later_moves(2))
    for half in range(2):
        in_ref[half, pl.ds(SEQS * me, SEQS)] = mo_ref[2 * me + half]

    finish_all(loads)
    keys_ref[...] = mask_ref[mine, :].astype(F32).T

    def take(half):
        def put(row, lanes, value):
            m_ref[0, 8 * half + row, :, lanes] = value
        turn_tokens(in_ref.at[half], wide_ref, put)

    def drain(count, copies_of):
        def one(n, carry):
            finish_all(copies_of(n))
            return carry
        lax.fori_loop(0, count, one, 0)

    def col_keep(at):
        return [jnp.broadcast_to(pick_column(keys_ref[...], at % 8 * 2 + blk), (LANES, LANES)) > 0.5 for blk in range(2)]

    def col_finish(block, out):
        layer, two = block // 8, block % 8
        m_ref[layer + 1, pl.ds(two * 2, 2)] = out.reshape(2, LANES, WIDE)
        ac = lax.dot_general(wp_ref[layer], layer_norm(out), NT, preferred_element_type=F32)
        ac = (ac * jnp.concatenate([mask_ref[pl.ds(HELD * me + 2 * two + blk, 1), :] for blk in range(2)], axis=1).astype(F32)).astype(BF16)
        parts = (ac[:SEQS], ac[SEQS:])
        own1_ref[two] = jnp.where(layer == 0, parts[0].astype(F32), own1_ref[two].astype(F32)).astype(BF16)
        own2_ref[two] = parts[1]
        for blk in range(2):
            lanes = slice(LANES * blk, LANES * blk + LANES)
            part_ref[block, blk] = jnp.where(layer == 0, parts[1][:, lanes].astype(F32), parts[0][:, lanes].astype(F32)).astype(BF16)

    def part_copies(block, full_ref):
        return group_copies(me, 10 + block, send_sem, recv_sem, lambda peer: part_ref.at[block],
                            full_ref.at[pl.ds(HELD * me + block % 8 * 2, 2)])

    def seq_copies(two):
        return group_copies(
            me, 26 + two, send_sem, recv_sem,
            lambda peer: m_ref.at[2, pl.ds(2 * two, 2), pl.ds(pl.multiple_of(SEQS * peer, SEQS), HELD), :],
            back_ref.at[0, pl.ds(HELD * me + 2 * two, 2)])

    def later_seqs(two):
        kind = jnp.where(two == 0, 34, 43 + two)
        return group_copies(
            me, kind, send_sem, recv_sem,
            lambda peer: m_ref.at[2, pl.ds(2 * two, 2), pl.ds(pl.multiple_of(SEQS * peer + HELD, HELD), HELD), :],
            back_ref.at[1, pl.ds(HELD * me + 2 * two, 2)])

    def emit(block):
        def first():
            start_all(part_copies(block, full1_ref))
            full1_ref[pl.ds(HELD * me + 2 * block, 2)] = part_ref[block]

        def second():
            start_all(part_copies(block, full2_ref) + seq_copies(block - 8) + later_seqs(block - 8))
            full2_ref[pl.ds(HELD * me + 2 * (block - 8), 2)] = part_ref[block]

        pl.when(jnp.logical_and(block >= 0, block < 8))(first)
        pl.when(block >= 8)(second)

    outer, along, across, close = pair_stages(
        me, 35, True, own1_ref, full1_ref, z_ref, mask_ref, res_ref,
        (wm_ref.at[0], wsb_ref.at[0], ws_ref.at[0], wso_ref.at[0], web_ref.at[0], we_ref.at[0], weo_ref.at[0], wnb_ref),
        zc_ref, next_ref, send_sem, recv_sem, pair)

    def second_half():
        for part in range(3):
            finish_all(later_moves(part))
        take(1)

    def col_aside(turn):
        emit(2 * turn - 3)
        emit(2 * turn - 2)
        pl.when(turn == 1)(second_half)
        pl.when(turn == 6)(lambda: outer(lambda: drain(8, lambda n: part_copies(n, full1_ref))))
        pl.when(turn == 7)(along)

    drain(8, moves)
    take(0)
    attend_blocks(16, wide, lambda at: m_ref[at // 8, pl.ds(at % 8 * 2, 2)].astype(F32).reshape(BLOCK, WIDE),
                  lambda at: lambda sl: wc_ref[at // 8, sl, :], lambda at: wco_ref[at // 8],
                  col_keep, None, col_finish, lambda: None, col_aside)
    last = range(13, 16)
    for block in last:
        start_all(part_copies(block, full2_ref))
        full2_ref[pl.ds(HELD * me + 2 * (block - 8), 2)] = part_ref[block]
    for block in last:
        start_all(seq_copies(block - 8))
    for half in range(2):
        back_ref[half, mine] = m_ref[2, :, pl.ds(pl.multiple_of(SEQS * me + HELD * half, HELD), HELD), :]
    across()
    for block in last:
        start_all(later_seqs(block - 8))

    outer, along_2, across_2, _ = pair_stages(
        me, 39, False, own2_ref, full2_ref, zc_ref, mask_ref, res_ref,
        (wm_ref.at[1], web_ref.at[1], we_ref.at[1], weo_ref.at[1], wsb_ref.at[1], ws_ref.at[1], wso_ref.at[1]),
        z_out_ref, None, send_sem, recv_sem, pair)
    outer(lambda: drain(8, lambda n: part_copies(n + 8, full2_ref)))

    def take_back(half):
        def put(row, lanes, value):
            ml_ref[HELD * half + row, :, lanes] = value
        turn_tokens(back_ref.at[half], wide_ref, put)

    def last_half():
        drain(8, later_seqs)
        take_back(1)

    def last_aside(turn):
        pl.when(turn == 1)(along_2)
        pl.when(turn == 1)(last_half)
        pl.when(turn == 2)(across_2)

    def last_ready():
        close()
        bias_by_key(next_ref, bias_ref)

    def last_finish(block, out):
        out_ref[pl.ds(4 * block, 4)] = out.reshape(4, RES, WIDE)

    drain(8, seq_copies)
    take_back(0)
    attend_blocks(8, wide, lambda at: ml_ref[pl.ds(at * 4, 4)].astype(F32).reshape(BLOCK, WIDE),
                  lambda at: lambda sl: wl_ref[sl, :], lambda at: wlo_ref[...],
                  lambda at: row_keep(mask_ref, SEQS * me + 4 * at), bias_ref, last_finish, last_ready, last_aside)


def run_all(m, z, mask, res_mask, row, tri, streamed):
    w_row_bias, w_row_in, w_row_out = row
    args = (m, z, mask, res_mask) + row + tri + (w_row_bias,) + streamed
    specs = [whole(a) for a in args[:4]] + [of_layer(a, 0) for a in row] + [whole(a) for a in tri] + [of_layer(w_row_bias, 1)]
    specs += [pl.BlockSpec(memory_space=pl.ANY)] * len(streamed)
    vmem = lambda *shape: pltpu.VMEM(shape, BF16)
    return pl.pallas_call(
        kernel,
        grid=(1,),
        in_specs=specs,
        out_specs=[VMEM] * 2,
        out_shape=[pltpu.VMEM(m.shape, BF16), pltpu.VMEM(z.shape, BF16)],
        scratch_shapes=[
            vmem(2, 4 * WIDE, WIDE),
            vmem(2, WIDE, WIDE),
            vmem(2, RES, WIDE),
            vmem(2, CELLS, LANES),
            vmem(4 * WIDE, WIDE),
            vmem(WIDE, WIDE),
            vmem(8, SEQS, 8, WIDE),
            vmem(2, LANES, 8, WIDE),
            pltpu.VMEM((3, CELLS, LANES), F32),
            vmem(3, HELD, LANES, WIDE),
            vmem(2, RES, HELD, WIDE),
            vmem(SEQS, RES, WIDE),
            vmem(8, RES, LANES),
            pltpu.VMEM((HELD, RES, LANES), F32),
            vmem(HELD, 2, SEQS, LANES),
            pltpu.VMEM((LANES, HELD), F32),
            vmem(8, SEQS, BLOCK),
            vmem(8, SEQS, BLOCK),
            vmem(RES, SEQS, LANES),
            vmem(RES, SEQS, LANES),
            vmem(HELD, RES, LANES),
            vmem(8, RES, LANES),
            pltpu.SemaphoreType.DMA((LANES + 25,)),
            pltpu.SemaphoreType.DMA((LANES + 25,)),
            pltpu.SemaphoreType.DMA((6,)),
        ] + wide_scratch(LANES) + pair_scratch(),
        compiler_params=pltpu.CompilerParams(collective_id=0, has_side_effects=True),
        cost_estimate=pl.CostEstimate(flops=10 ** 10, bytes_accessed=2 ** 22, transcendentals=0),
        name="evoformer",
    )(*args)


def greet(me):
    barrier = pltpu.get_barrier_semaphore()
    for o in range(1, 4):
        pl.semaphore_signal(barrier, inc=1, device_id={'dap': lax.rem(me + o, 4)}, device_id_type=pl.DeviceIdType.MESH)


def meet():
    pl.semaphore_wait(pltpu.get_barrier_semaphore(), 3)


def group_copies(me, kind, send_sem, recv_sem, source, target):
    copies = []
    for o in range(1, 4):
        peer = lax.rem(me + o, 4)
        copies.append(pltpu.make_async_remote_copy(
            src_ref=source(peer), dst_ref=target, send_sem=send_sem.at[3 * kind + o - 1],
            recv_sem=recv_sem.at[3 * kind + o - 1], device_id={'dap': peer}, device_id_type=pl.DeviceIdType.MESH))
    return copies


def start_all(copies):
    for copy in copies:
        copy.start()


def finish_all(copies):
    for copy in copies:
        copy.wait()


def local_bias_rows(ln_ref, w_ref, spread_ref):
    heads = w_ref.shape[0]
    w = w_ref[...]
    if heads < 8:
        w = jnp.concatenate([w, jnp.zeros((8 - heads, LANES), BF16)], axis=0)
    values = lax.dot_general(w, ln_ref[...], NT, preferred_element_type=F32)
    left = lax.broadcasted_iota(jnp.int32, (HELD, LANES), 1) < RES
    for two in range(8):
        value = values[:heads, LANES * two:LANES * two + LANES]
        turned = pltpu.roll(value, RES, 1)
        low = left[:heads]
        spread_ref[pl.ds(2 * two, heads, stride=HELD), :] = jnp.where(low, value, turned)
        spread_ref[pl.ds(2 * two + 1, heads, stride=HELD), :] = jnp.where(low, turned, value)
    both = [jnp.where(left, spread_ref[pl.ds(2 * HELD * n, HELD), :], spread_ref[pl.ds(2 * HELD * n + HELD, HELD), :])
            for n in range(heads // 2)]
    return jnp.concatenate(both, axis=0).astype(BF16).reshape(heads // 2, HELD, LANES)


def bias_by_query(rows_ref, bias_ref):
    for n in range(rows_ref.shape[0]):
        turned = (rows_ref[n].astype(F32) * LOG2E).T
        for half in range(2):
            one = turned[RES * half:RES * half + RES]
            bias_ref[2 * n + half] = jnp.concatenate([one, one], axis=1)


def bias_by_key(rows_ref, bias_ref):
    left = lax.broadcasted_iota(jnp.int32, (RES, LANES), 1) < RES
    for n in range(rows_ref.shape[0]):
        value = rows_ref[n].astype(F32) * LOG2E
        turned = pltpu.roll(value, RES, 1)
        bias_ref[2 * n] = jnp.where(left, value, turned)
        bias_ref[2 * n + 1] = jnp.where(left, turned, value)


def triangle(zf_ref, ln_ref, w_ref, wo_ref, keep, bias_ref, pt_refs, gt_refs, others, ready):
    def fill(block):
        return project(ln_ref, pt_refs[block], lambda sl: w_ref[sl, :], pl.ds(BLOCK * block, BLOCK))

    def done(block):
        def job():
            rows = pl.ds(BLOCK * block, BLOCK)
            zf_ref[rows, :] = leave(gt_refs[block], zf_ref[rows, :], wo_ref[...]).astype(F32)
        return job

    for job in fill(0):
        job()
    ready()
    jobs = [(4 * block - 4, 4 * block - 1, fill(block)) for block in range(1, 4)]
    jobs += [(4 * block + 4 + 3 * LAG, 4 * block + 5 + 3 * LAG, [done(block)]) for block in range(3)]
    attend_stream([(pt_refs[block], gt_refs[block], [keep, keep]) for block in range(4)], others, 4, SEQS, bias_ref, jobs)
    done(3)()


def pair_stages(me, first, swap, own_ref, full_ref, z_ref, mask_ref, res_ref, weights, out_ref, next_ref, send_sem, recv_sem, scratch):
    wm_ref, wba_ref, wa_ref, woa_ref, wbb_ref, wb_ref, wob_ref = weights[:7]
    (full32_ref, o_ref, wt_ref, zf_ref, zt_ref, ln_ref, bias_ref, la_ref, ra_ref, lb_ref, rb_ref, zs_ref, zr_ref, nl_ref) = scratch[:14]
    att = scratch[14:]
    pt_refs, gt_refs, others = att[0:4], att[4:8], att[8:11]
    mine = pl.ds(pl.multiple_of(HELD * me, HELD), HELD)

    def keep():
        diagonal = lax.broadcasted_iota(jnp.int32, (RES, RES), 0) == lax.broadcasted_iota(jnp.int32, (RES, RES), 1)
        keys = jnp.sum(jnp.where(diagonal, jnp.broadcast_to(res_ref[...], (RES, RES)), 0).astype(F32), axis=1, keepdims=True)
        return jnp.broadcast_to(keys, (RES, LANES)) > 0.5

    def exchange(kind):
        source, target = (
            (lambda peer: la_ref, ra_ref.at[:, mine, :]),
            (lambda peer: zs_ref.at[:, pl.ds(pl.multiple_of(HELD * peer, HELD), HELD), :], zr_ref.at[mine]),
            (lambda peer: lb_ref, rb_ref.at[:, mine, :]),
            (lambda peer: nl_ref, None if next_ref is None else next_ref.at[:, mine, :]),
        )[kind]
        return group_copies(me, first + kind, send_sem, recv_sem, source, target)

    def outer(arrive):
        mask = mask_ref[...].astype(F32).astype(BF16)
        norm = lax.dot_general(mask, mask_ref[mine, :].astype(F32).astype(BF16), NT, preferred_element_type=F32)
        full32_ref[:CELLS] = wm_ref[...].astype(F32).reshape(CELLS, LANES)
        if swap:
            for q in range(SEQS):
                wt_ref[pl.ds(SEQS * q, SEQS), :] = full32_ref[pl.ds(q, SEQS, stride=SEQS), :].astype(BF16)
        else:
            wt_ref[...] = wm_ref[...].reshape(CELLS, LANES)
        w_turned = wt_ref[...].T
        arrive()
        full32_ref[...] = full_ref[...].astype(F32).reshape(2048, LANES)
        own = own_ref[...].reshape(BLOCK, BLOCK)
        zeros = jnp.zeros((RES, LANES), BF16)

        def one(q, carry):
            c_q = full32_ref[pl.ds(q, RES, stride=SEQS), :].astype(BF16)
            rhs = jnp.concatenate([jnp.concatenate([c_q, zeros], axis=1), jnp.concatenate([zeros, c_q], axis=1)], axis=0)
            o = lax.dot_general(own, rhs, NT, preferred_element_type=F32).astype(BF16)
            for pair in range(8):
                o_ref[pair, pl.ds(pl.multiple_of(q * SEQS, SEQS), SEQS), :] = o[SEQS * pair:SEQS * pair + SEQS]
            return carry

        lax.fori_loop(0, SEQS, one, 0, unroll=4)
        for pair in range(8):
            update = jnp.dot(w_turned, o_ref[pair], preferred_element_type=F32).T
            z = z_ref[pl.ds(2 * pair, 2)].astype(F32).reshape(LANES, LANES)
            below = jnp.concatenate([pick_column(norm, 2 * pair), pick_column(norm, 2 * pair + 1)], axis=0)
            z = (z + update / (1e-3 + below)).astype(BF16).astype(F32)
            rows = pl.ds(LANES * pair, LANES)
            zf_ref[rows, :] = z
            ln_ref[rows, :] = layer_norm(z)
        la_ref[...] = local_bias_rows(ln_ref, wba_ref, zt_ref)
        start_all(exchange(0))
        ra_ref[:, mine, :] = la_ref[...]

    def along():
        def ready():
            finish_all(exchange(0))
            bias_by_query(ra_ref, bias_ref)

        triangle(zf_ref, ln_ref, wa_ref, woa_ref, keep(), bias_ref, pt_refs, gt_refs, others, ready)
        zs_ref[...] = zf_ref[...].astype(BF16).reshape(HELD, RES, LANES)
        norm_all(zf_ref, ln_ref)
        start_all(exchange(1))
        zr_ref[mine] = zs_ref[:, mine, :]
        lb_ref[...] = local_bias_rows(ln_ref, wbb_ref, zt_ref)
        start_all(exchange(2))
        rb_ref[:, mine, :] = lb_ref[...]

    def across():
        finish_all(exchange(1))
        zt_ref[...] = zr_ref[...].astype(F32).reshape(CELLS, LANES)
        for row in range(HELD):
            value = zt_ref[pl.ds(row, RES, stride=HELD), :]
            zf_ref[pl.ds(RES * row, RES), :] = value
            ln_ref[pl.ds(RES * row, RES), :] = layer_norm(value)

        def ready():
            finish_all(exchange(2))
            bias_by_key(rb_ref, bias_ref)

        triangle(zf_ref, ln_ref, wb_ref, wob_ref, keep(), bias_ref, pt_refs, gt_refs, others, ready)
        out_ref[...] = zf_ref[...].astype(BF16).reshape(HELD, RES, LANES)
        if next_ref is not None:
            norm_all(zf_ref, ln_ref)
            nl_ref[...] = local_bias_rows(ln_ref, weights[7], zt_ref)
            start_all(exchange(3))
            next_ref[:, mine, :] = nl_ref[...]

    def close():
        if next_ref is not None:
            finish_all(exchange(3))

    return outer, along, across, close


def pair_scratch():
    return [
        pltpu.VMEM((2048, LANES), F32),
        pltpu.VMEM((8, CELLS, LANES), BF16),
        pltpu.VMEM((CELLS, LANES), BF16),
        pltpu.VMEM((CELLS, LANES), F32),
        pltpu.VMEM((CELLS, LANES), F32),
        pltpu.VMEM((CELLS, LANES), BF16),
        pltpu.VMEM((4, RES, LANES), F32),
        pltpu.VMEM((2, HELD, LANES), BF16),
        pltpu.VMEM((2, RES, LANES), BF16),
        pltpu.VMEM((2, HELD, LANES), BF16),
        pltpu.VMEM((2, RES, LANES), BF16),
        pltpu.VMEM((HELD, RES, LANES), BF16),
        pltpu.VMEM((RES, HELD, LANES), BF16),
        pltpu.VMEM((8, HELD, LANES), BF16),
    ] + attend_scratch(4, SEQS, RES, 4)


def norm_all(zf_ref, ln_ref):
    for block in range(8):
        rows = pl.ds(LANES * block, LANES)
        ln_ref[rows, :] = layer_norm(zf_ref[rows, :])


def solution(mesh):
    def local_step(m, z, mask, res_mask, w_row_bias, w_row_in, w_row_out, w_col_in, w_col_out, w_opm_in, w_opm_out, w_ts_bias, w_ts_in, w_ts_out, w_te_bias, w_te_in, w_te_out):
        flat_in = lambda w: jnp.transpose(w, (0, 2, 3, 4, 1)).reshape(2, -1, w.shape[1])
        flat_out = lambda w: w.reshape(2, -1, w.shape[-1])
        flat_bias = lambda w: jnp.transpose(w, (0, 2, 1))
        w_row_in, w_col_in, w_ts_in, w_te_in = map(flat_in, (w_row_in, w_col_in, w_ts_in, w_te_in))
        w_row_out, w_col_out, w_ts_out, w_te_out = map(flat_out, (w_row_out, w_col_out, w_ts_out, w_te_out))
        w_row_bias, w_ts_bias, w_te_bias = map(flat_bias, (w_row_bias, w_ts_bias, w_te_bias))
        w_opm_in = jnp.transpose(w_opm_in, (0, 2, 3, 1)).reshape(2, RES, WIDE)
        w_opm_out = w_opm_out.reshape(2, CELLS, LANES)
        mask = mask.T
        res_mask = res_mask.reshape(1, RES)

        m, z = run_all(
            m, z, mask, res_mask, (w_row_bias, w_row_in, w_row_out),
            (w_ts_bias, w_ts_in, w_ts_out, w_te_bias, w_te_in, w_te_out),
            (w_col_in, w_col_out, w_opm_in, w_opm_out, w_row_in, w_row_out))
        return m, z

    in_specs = (P(('data', 'dap')), P(('data', 'dap')), P('data'), P('data')) + (P(),) * 13
    out_specs = (P(('data', 'dap')), P(('data', 'dap')))
    return jax.shard_map(local_step, mesh=mesh, in_specs=in_specs, out_specs=out_specs, check_vma=False)
```
